256 devices in a mesh: gx: 8 (over z), gy: 4 (over y), gz: 8 (over x, core).
Axes of the slice: x: 4, y: 4, z: 8, core: 2. Of those that a mesh axis runs over, the one named last changes fastest.
Arguments:
- chi_field: float32 [64, 128, 1024], P('gx', 'gy', 'gz'), may hold values from 0.5 to 2.5, as said below
- metric: float32 [6, 64, 128, 1024], P(None, 'gx', 'gy', 'gz'), may hold values from -0.3 to 1.5, as said below
- curvature: float32 [6, 64, 128, 1024], P(None, 'gx', 'gy', 'gz'), may hold values from -1.6 to 1.6
- trace_curvature: float32 [64, 128, 1024], P('gx', 'gy', 'gz'), may hold values from -3 to 3
- gamma_field: float32 [3, 64, 128, 1024], P(None, 'gx', 'gy', 'gz'), may hold values from -1.6 to 1.6
Outputs:
- hamiltonian: float32 [64, 128, 1024], P('gx', 'gy', 'gz')
- momentum: float32 [3, 64, 128, 1024], P(None, 'gx', 'gy', 'gz')
- constraint_norms: float32 [2], replicated
The draws below stay inside these ranges and needn't reach their ends.
Inputs may be any that keep to these rules, and one draw needn't show every extreme that they name: `chi_field`: positive. `metric`: at every cell the symmetric 3x3 matrix built from the six components is positive definite with a dominant diagonal.
All inputs are finite; a program needn't handle non-finite values.
Results may differ from the reference program's by a relative error of at most 0.0003.
Values sent between devices are 32-bit elements; how exact they have to be, the bound alone decides.
A program may use at most 128 MiB of HBM per device.

```python
import math
import jax
import jax.numpy as jnp
from jax import lax

CX = 8
NX = 64
NY = 128
NZ = 1024
N_GX = 8


def ramp_level():
    xs = jnp.arange(NX, dtype=jnp.float32) / NX
    ys = jnp.arange(NY, dtype=jnp.float32) / NY
    zs = jnp.arange(NZ, dtype=jnp.float32) / NZ
    level = (xs[:, None, None] + ys[None, :, None] + zs[None, None, :]) / 3.0
    return jnp.exp(math.log(3.0) * level)


def draw_chi_field(key, part):
    noise = jax.random.uniform(key, (NX, NY, NZ), jnp.float32, -1.0, 1.0)
    value = 0.12 * ramp_level() * noise
    return jnp.exp(value)


def draw_metric(key, part):
    noise = jax.random.uniform(key, (6, NX, NY, NZ), jnp.float32, -1.0, 1.0)
    identity = jnp.array([1.0, 0.0, 0.0, 1.0, 0.0, 1.0], dtype=jnp.float32)[:, None, None, None]
    value = 0.05 * ramp_level()[None] * noise
    return identity + value


def draw_curvature(key, part):
    noise = jax.random.uniform(key, (6, NX, NY, NZ), jnp.float32, -1.0, 1.0)
    return 0.3 * ramp_level()[None] * noise


def draw_trace_curvature(key, part):
    noise = jax.random.uniform(key, (NX, NY, NZ), jnp.float32, -1.0, 1.0)
    value = 0.5 * ramp_level() * noise
    return value


def draw_gamma_field(key, part):
    noise = jax.random.uniform(key, (3, NX, NY, NZ), jnp.float32, -1.0, 1.0)
    return 0.3 * ramp_level()[None] * noise


def setup_inputs(seed: int = 0) -> dict:
    keys = jax.random.split(jax.random.key(seed), 6)
    return {
        "chi_field": draw_chi_field(jax.random.fold_in(keys[5], 71), 0),
        "metric": draw_metric(jax.random.fold_in(keys[5], 71), 0),
        "curvature": draw_curvature(jax.random.fold_in(keys[5], 71), 0),
        "trace_curvature": draw_trace_curvature(jax.random.fold_in(keys[5], 71), 0),
        "gamma_field": draw_gamma_field(jax.random.fold_in(keys[5], 71), 0),
    }


pair_index = ((0, 1, 2), (1, 3, 4), (2, 4, 5))
first_taps = ((-2, 1.0 / 12.0), (-1, -8.0 / 12.0), (1, 8.0 / 12.0), (2, -1.0 / 12.0))
second_taps = ((-2, -1.0 / 12.0), (-1, 16.0 / 12.0), (0, -30.0 / 12.0), (1, 16.0 / 12.0), (2, -1.0 / 12.0))

def window(padded, offsets):
    sx = padded.shape[-3] - 4
    sy = padded.shape[-2] - 4
    sz = padded.shape[-1] - 4
    return padded[..., 2 + offsets[0]:2 + offsets[0] + sx, 2 + offsets[1]:2 + offsets[1] + sy, 2 + offsets[2]:2 + offsets[2] + sz]

def shifted(pairs):
    places = [0, 0, 0]
    for axis_num, step in pairs:
        places[axis_num] = places[axis_num] + step
    return tuple(places)

def first_diff(padded, axis_num):
    summed = None
    for step, weight in first_taps:
        term = weight * window(padded, shifted(((axis_num, step),)))
        summed = term if summed is None else summed + term
    return summed

def second_diff(padded, a, b):
    summed = None
    if a == b:
        for step, weight in second_taps:
            term = weight * window(padded, shifted(((a, step),)))
            summed = term if summed is None else summed + term
        return summed
    for step_a, weight_a in first_taps:
        for step_b, weight_b in first_taps:
            term = weight_a * weight_b * window(padded, shifted(((a, step_a), (b, step_b))))
            summed = term if summed is None else summed + term
    return summed

def constraints(geo_pad, rest_pad):
    centre = window(geo_pad, (0, 0, 0))
    remainder = window(rest_pad, (0, 0, 0))
    conformal = centre[0]
    trace_curv = remainder[6]
    geo_first = [first_diff(geo_pad, a) for a in range(3)]
    rest_first = [first_diff(rest_pad, a) for a in range(3)]
    geo_second = {}
    for a in range(3):
        for b in range(a, 3):
            geo_second[a, b] = second_diff(geo_pad, a, b)

    def metric_at(i, j):
        return centre[1 + pair_index[i][j]]

    def curv_at(i, j):
        return remainder[pair_index[i][j]]

    def metric_grad(i, j, a):
        return geo_first[a][1 + pair_index[i][j]]

    def metric_hess(i, j, a, b):
        return geo_second[min(a, b), max(a, b)][1 + pair_index[i][j]]

    def chi_hess(a, b):
        return geo_second[min(a, b), max(a, b)][0]

    def curv_grad(i, j, a):
        return rest_first[a][pair_index[i][j]]
    chi_grad = [geo_first[a][0] for a in range(3)]
    trace_grad = [rest_first[a][6] for a in range(3)]
    g00, g01, g02 = (metric_at(0, 0), metric_at(0, 1), metric_at(0, 2))
    g11, g12, g22 = (metric_at(1, 1), metric_at(1, 2), metric_at(2, 2))
    minor00 = g11 * g22 - g12 * g12
    minor01 = g02 * g12 - g01 * g22
    minor02 = g01 * g12 - g02 * g11
    minor11 = g00 * g22 - g02 * g02
    minor12 = g01 * g02 - g00 * g12
    minor22 = g00 * g11 - g01 * g01
    determinant = g00 * minor00 + g01 * minor01 + g02 * minor02
    scale = 1.0 / determinant
    inverse_list = [minor00 * scale, minor01 * scale, minor02 * scale, minor11 * scale, minor12 * scale, minor22 * scale]

    def inv_at(i, j):
        return inverse_list[pair_index[i][j]]
    christ_low = [[[None] * 3 for i in range(3)] for k in range(3)]
    for k in range(3):
        for i in range(3):
            for j in range(i, 3):
                value = 0.5 * (metric_grad(k, j, i) + metric_grad(k, i, j) - metric_grad(i, j, k))
                christ_low[k][i][j] = value
                christ_low[k][j][i] = value
    christ_up = [[[None] * 3 for i in range(3)] for k in range(3)]
    for k in range(3):
        for i in range(3):
            for j in range(i, 3):
                value = inv_at(k, 0) * christ_low[0][i][j] + inv_at(k, 1) * christ_low[1][i][j] + inv_at(k, 2) * christ_low[2][i][j]
                christ_up[k][i][j] = value
                christ_up[k][j][i] = value
    gamma_calc = []
    for k in range(3):
        summed = None
        for i in range(3):
            for j in range(3):
                term = inv_at(i, j) * christ_up[k][i][j]
                summed = term if summed is None else summed + term
        gamma_calc.append(summed)
    cov_hess = [[None] * 3 for i in range(3)]
    for i in range(3):
        for j in range(i, 3):
            value = chi_hess(i, j) - (christ_up[0][i][j] * chi_grad[0] + christ_up[1][i][j] * chi_grad[1] + christ_up[2][i][j] * chi_grad[2])
            cov_hess[i][j] = value
            cov_hess[j][i] = value
    laplace = None
    grad_sq = None
    for l in range(3):
        for m in range(3):
            term = inv_at(l, m) * cov_hess[l][m]
            laplace = term if laplace is None else laplace + term
            term = inv_at(l, m) * chi_grad[l] * chi_grad[m]
            grad_sq = term if grad_sq is None else grad_sq + term
    scalar_sum = None
    for i in range(3):
        for j in range(i, 3):
            ricci = None
            for l in range(3):
                for m in range(3):
                    term = -0.5 * inv_at(l, m) * metric_hess(i, j, l, m)
                    ricci = term if ricci is None else ricci + term
            for k in range(3):
                ricci = ricci + 0.5 * (metric_at(k, i) * rest_first[j][7 + k] + metric_at(k, j) * rest_first[i][7 + k])
                ricci = ricci + 0.5 * gamma_calc[k] * (christ_low[i][j][k] + christ_low[j][i][k])
            for l in range(3):
                for m in range(3):
                    inner = None
                    for k in range(3):
                        term = christ_up[k][l][i] * christ_low[j][k][m] + christ_up[k][l][j] * christ_low[i][k][m] + christ_up[k][i][m] * christ_low[k][l][j]
                        inner = term if inner is None else inner + term
                    ricci = ricci + inv_at(l, m) * inner
            conf_part = (cov_hess[i][j] + metric_at(i, j) * laplace) / (2.0 * conformal) - (chi_grad[i] * chi_grad[j] + 3.0 * metric_at(i, j) * grad_sq) / (4.0 * conformal * conformal)
            weight = 1.0 if i == j else 2.0
            term = weight * inv_at(i, j) * (ricci + conf_part)
            scalar_sum = term if scalar_sum is None else scalar_sum + term
    mixed = [[None] * 3 for i in range(3)]
    for i in range(3):
        for j in range(3):
            mixed[i][j] = curv_at(i, 0) * inv_at(0, j) + curv_at(i, 1) * inv_at(1, j) + curv_at(i, 2) * inv_at(2, j)
    square_sum = None
    for i in range(3):
        for j in range(3):
            term = mixed[i][j] * mixed[j][i]
            square_sum = term if square_sum is None else square_sum + term
    hamilton = conformal * scalar_sum + 2.0 / 3.0 * trace_curv * trace_curv - square_sum
    momentum_list = []
    for i in range(3):
        summed = None
        for j in range(3):
            for k in range(3):
                term = inv_at(j, k) * curv_grad(k, i, j)
                summed = term if summed is None else summed + term
        for l in range(3):
            summed = summed - gamma_calc[l] * curv_at(l, i)
            for j in range(3):
                summed = summed - christ_up[l][j][i] * mixed[l][j]
        along = mixed[i][0] * chi_grad[0] + mixed[i][1] * chi_grad[1] + mixed[i][2] * chi_grad[2]
        summed = summed - 2.0 / 3.0 * trace_grad[i] - 1.5 * along / conformal
        momentum_list.append(summed)
    return (hamilton, jnp.stack(momentum_list))

def reference(chi_field, metric, curvature, trace_curvature, gamma_field):
    geometry = jnp.concatenate([chi_field[None], metric], 0)
    remainder = jnp.concatenate([curvature, trace_curvature[None], gamma_field], 0)
    geo_pad = jnp.pad(geometry, ((0, 0), (2, 2), (2, 2), (2, 2)), mode='wrap')
    rest_pad = jnp.pad(remainder, ((0, 0), (2, 2), (2, 2), (2, 2)), mode='wrap')

    def one_slab(index):
        start = (index * CX).astype(jnp.int32)
        geo_slab = lax.dynamic_slice_in_dim(geo_pad, start, CX + 4, 1)
        rest_slab = lax.dynamic_slice_in_dim(rest_pad, start, CX + 4, 1)
        hamilton, momentum = constraints(geo_slab, rest_slab)
        ham_sq = lax.optimization_barrier(jnp.sum(lax.optimization_barrier(jnp.sum(lax.optimization_barrier(jnp.sum(hamilton * hamilton, axis=2)), axis=1)), axis=0))
        mom_sq = lax.optimization_barrier(jnp.sum(lax.optimization_barrier(jnp.sum(lax.optimization_barrier(jnp.sum(lax.optimization_barrier(jnp.sum(momentum * momentum, axis=3)), axis=2)), axis=1)), axis=0))
        return (hamilton, momentum, ham_sq, mom_sq)
    hamilton, momentum, ham_sq, mom_sq = lax.map(one_slab, jnp.arange(N_GX, dtype=jnp.int32))
    hamilton = hamilton.reshape(chi_field.shape)
    momentum = jnp.moveaxis(momentum, 1, 0).reshape(gamma_field.shape)
    cell_count = chi_field.size
    sums = jnp.stack([jnp.sum(ham_sq), jnp.sum(mom_sq)])
    norms = jnp.sqrt(sums / jnp.array([cell_count, 3 * cell_count], dtype=jnp.float32))
    return (hamilton, momentum, norms)
```

```python
import functools

import jax
import jax.numpy as jnp
from jax import lax
from jax.experimental import pallas as pl
from jax.experimental.pallas import tpu as pltpu
from jax.sharding import PartitionSpec as P

MESH = pl.DeviceIdType.MESH
PAIR = ((0, 1, 2), (1, 3, 4), (2, 4, 5))

CX, CY, CZ = 8, 32, 128
LX, ROWS, OWN = CX + 4, 48, 8
BLOCKS = CY // 8
PAIRS = CX // 2
GEO, REST = 7, 10
Y_REST = (0, 1, 2, 3, 4, 5, 6, 8)
Z_REST = (0, 1, 2, 3, 4, 5, 6, 9)
X_REST = 8

S_GEO_X, S_EDGE_XY, S_EDGE_YZ, S_EDGE_XZ = 0, 8, 12, 16
S_GEO_Y, S_GEO_Z, S_REST_Y, S_REST_Z, S_TERM = 20, 22, 24, 26, 28
S_SUM_A, S_SUM_B, S_COUNT = 36, 68, 76


def lane_ids():
    return lax.broadcasted_iota(jnp.int32, (8, CZ), 1)


def inverse_of(g):
    g00, g01, g02, g11, g12, g22 = g
    m00 = g11 * g22 - g12 * g12
    m01 = g02 * g12 - g01 * g22
    m02 = g01 * g12 - g02 * g11
    m11 = g00 * g22 - g02 * g02
    m12 = g01 * g02 - g00 * g12
    m22 = g00 * g11 - g01 * g01
    scale = 1.0 / (g00 * m00 + g01 * m01 + g02 * m02)
    return [m00 * scale, m01 * scale, m02 * scale, m11 * scale, m12 * scale, m22 * scale]


def first(lo2, lo1, hi1, hi2):
    return (lo2 - hi2) + 8.0 * (hi1 - lo1)


def second(lo2, lo1, mid, hi1, hi2):
    return 16.0 * (lo1 + hi1) - (lo2 + hi2) - 30.0 * mid


def kernel(
    sizes,
    chi_in, met_in, cur_in, trk_in, gam_in,
    ham_out, mom_out, norm_out,
    F, R, DZ, DZZ, DX, DXX, OUT, ACC,
    YSG, YSR, YRG, YRR, XYR,
    ZSG, ZSR, ZRG, ZRR,
    CS, CR, MINE, SUM_A, SUM_B,
    load_sem, out_sem, send_sem, recv_sem,
):
    n_gx, n_gy, n_gz = sizes
    ix, iy, iz = lax.axis_index("gx"), lax.axis_index("gy"), lax.axis_index("gz")

    def at(dx, dy, dz):
        return (
            lax.rem(ix + dx + n_gx, n_gx),
            lax.rem(iy + dy + n_gy, n_gy),
            lax.rem(iz + dz + n_gz, n_gz),
        )

    def remote(src, dst, place, device):
        return pltpu.make_async_remote_copy(
            src_ref=src, dst_ref=dst, send_sem=send_sem.at[place], recv_sem=recv_sem.at[place],
            device_id=device, device_id_type=MESH,
        )

    loads = [
        (chi_in, F.at[0, 2 : 2 + CX, OWN : OWN + CY]),
        (met_in, F.at[1:7, 2 : 2 + CX, OWN : OWN + CY]),
        (cur_in, R.at[0:6, 2 : 2 + CX, OWN : OWN + CY]),
        (trk_in, R.at[6, 2 : 2 + CX, OWN : OWN + CY]),
        (gam_in, R.at[7:10, 2 : 2 + CX, OWN : OWN + CY]),
    ]
    loads = [pltpu.make_async_copy(s, d, load_sem.at[i]) for i, (s, d) in enumerate(loads)]
    for copy in loads:
        copy.start()

    barrier = pltpu.get_barrier_semaphore()
    n_plane = n_gy * n_gz
    rank_a = iy * n_gz + iz

    def plane_peer(j):
        rank = lax.rem(rank_a + j, n_plane)
        return rank, (ix, rank // n_gz, lax.rem(rank, n_gz))

    def greet_plane(j, _):
        pl.semaphore_signal(barrier, inc=1, device_id=plane_peer(j)[1], device_id_type=MESH)
        return 0

    corners = [(a, b, 0) for a in (-1, 1) for b in (-1, 1)] + [(a, 0, b) for a in (-1, 1) for b in (-1, 1)]
    for step in corners + [(j, 0, 0) for j in range(1, n_gx)]:
        pl.semaphore_signal(barrier, inc=1, device_id=at(*step), device_id_type=MESH)
    lax.fori_loop(1, n_plane, greet_plane, 0)

    lane2 = lane_ids() // 2
    zero = jnp.zeros((8, CZ), jnp.float32)

    def clear(c, _):
        for layer in (0, 1, LX - 2, LX - 1):
            for b in range(BLOCKS):
                R[c, layer, pl.ds(OWN + 8 * b, 8), :] = zero
        return 0

    lax.fori_loop(0, X_REST, clear, 0)
    ACC[...] = jnp.zeros_like(ACC)

    def pack_z(source, channels, to):
        def body(p, _):
            low, high = zero, zero
            for n, c in enumerate(channels):
                for xi in range(2):
                    for b in range(BLOCKS):
                        t = (n * 2 + xi) * BLOCKS + b
                        tile = source[c, 2 + 2 * p + xi, pl.ds(OWN + 8 * b, 8), :]
                        here = lane2 == t
                        low = jnp.where(here, pltpu.roll(tile, 2 * t, 1) if t else tile, low)
                        up = (2 * t + 2) % CZ
                        high = jnp.where(here, pltpu.roll(tile, up, 1) if up else tile, high)
            to[0, p] = low
            to[1, p] = high
            return 0

        lax.fori_loop(0, PAIRS, body, 0)

    loads[0].wait()
    loads[1].wait()
    pack_z(F, range(GEO), ZSG)

    def pack_y_geo(p, _):
        for c in range(GEO):
            for xi in range(2):
                rows = slice(c * 4 + xi * 2, c * 4 + xi * 2 + 2)
                YSG[0, p, rows, :] = F[c, 2 + 2 * p + xi, OWN : OWN + 2, :]
                YSG[1, p, rows, :] = F[c, 2 + 2 * p + xi, OWN + CY - 2 : OWN + CY, :]
        return 0

    for s in range(2):
        for p in range(PAIRS):
            YSG[s, p, 24:32, :] = zero
    lax.fori_loop(0, PAIRS, pack_y_geo, 0)

    pl.semaphore_wait(barrier, n_plane - 1 + n_gx - 1 + len(corners))

    def geo_x(d, b):
        rows = pl.ds(OWN + 8 * b, 8)
        src = F.at[0:GEO, pl.ds(2 if d == 0 else CX, 2), rows]
        dst = F.at[0:GEO, pl.ds(CX + 2 if d == 0 else 0, 2), rows]
        return remote(src, dst, S_GEO_X + 4 * d + b, at(2 * d - 1, 0, 0))

    geo_xs = [[geo_x(d, b) for b in range(BLOCKS)] for d in range(2)]
    geo_ys = [remote(YSG.at[d], YRG.at[1 - d], S_GEO_Y + d, at(0, 2 * d - 1, 0)) for d in range(2)]
    geo_zs = [
        remote(ZSG.at[d], ZRG.at[1 - d, 0, 1 : 1 + PAIRS], S_GEO_Z + d, at(0, 0, 2 * d - 1)) for d in range(2)
    ]
    combos = [(a, b) for a in range(2) for b in range(2)]
    edge_xy = [
        remote(
            YSG.at[dy, PAIRS - 1 if dx else 0], XYR.at[1 - dx, 1 - dy], S_EDGE_XY + 2 * dx + dy,
            at(2 * dx - 1, 2 * dy - 1, 0),
        )
        for dx, dy in combos
    ]
    edge_yz = [
        remote(
            ZSG.at[dz], ZRG.at[1 - dz, 1 if dy else 2, 1 : 1 + PAIRS], S_EDGE_YZ + 2 * dy + dz,
            at(0, 2 * dy - 1, 2 * dz - 1),
        )
        for dy, dz in combos
    ]
    edge_xz = [
        remote(
            ZSG.at[dz, pl.ds(PAIRS - 1 if dx else 0, 1)], ZRG.at[1 - dz, 0, pl.ds(0 if dx else PAIRS + 1, 1)],
            S_EDGE_XZ + 2 * dx + dz, at(2 * dx - 1, 0, 2 * dz - 1),
        )
        for dx, dz in combos
    ]
    for b in range(BLOCKS):
        for d in range(2):
            geo_xs[d][b].start()
        if b == 0:
            for copy in geo_zs + geo_ys + edge_yz:
                copy.start()
        if b == 1:
            for copy in edge_xy + edge_xz:
                copy.start()

    for copy in loads[2:]:
        copy.wait()
    pack_z(R, Z_REST, ZSR)

    def pack_y_rest(x, _):
        rows = pl.ds(2 * x, 2)
        for n, c in enumerate(Y_REST):
            YSR[0, n, rows, :] = R[c, 2 + x, OWN : OWN + 2, :]
            YSR[1, n, rows, :] = R[c, 2 + x, OWN + CY - 2 : OWN + CY, :]
        return 0

    lax.fori_loop(0, CX, pack_y_rest, 0)
    rest_zs = [remote(ZSR.at[d], ZRR.at[1 - d], S_REST_Z + d, at(0, 0, 2 * d - 1)) for d in range(2)]
    rest_ys = [remote(YSR.at[d], YRR.at[1 - d], S_REST_Y + d, at(0, 2 * d - 1, 0)) for d in range(2)]

    lane = lane_ids()

    def z_taps(tile, left, right, t):
        from_left = pltpu.roll(left, CZ - 2 - 2 * t, 1)
        from_right = pltpu.roll(right, lax.rem(CZ - 2 * t, CZ), 1)
        return (
            pltpu.roll(jnp.where(lane >= CZ - 2, from_left, tile), 2, 1),
            pltpu.roll(jnp.where(lane >= CZ - 1, from_left, tile), 1, 1),
            pltpu.roll(jnp.where(lane < 1, from_right, tile), CZ - 1, 1),
            pltpu.roll(jnp.where(lane < 2, from_right, tile), CZ - 2, 1),
        )

    def z_geo(layer, pair, xi, rows, variant, b, out):
        left, right = ZRG[0, variant, pair], ZRG[1, variant, pair]
        for c in range(GEO):
            tile = F[c, layer, rows, :]
            taps = z_taps(tile, left, right, (c * 2 + xi) * BLOCKS + b)
            DZ[c, layer, rows, :] = first(*taps)
            if out is not None:
                DZZ[c, out[0], out[1], :] = second(taps[0], taps[1], tile, taps[2], taps[3])

    for copy in geo_zs:
        copy.wait_recv()

    def z_own(i, _):
        x, b = i // BLOCKS, lax.rem(i, BLOCKS)
        z_geo(
            x + 2, x // 2 + 1, lax.rem(x, 2), pl.ds(pl.multiple_of(OWN + 8 * b, 8), 8), 0, b,
            (x, pl.ds(pl.multiple_of(8 * b, 8), 8)),
        )
        return 0

    lax.fori_loop(0, CX * BLOCKS, z_own, 0)
    for copy in rest_zs + rest_ys:
        copy.start()

    for copy in geo_ys + edge_yz:
        copy.wait_recv()

    def open_y_geo(p, _):
        for c in range(GEO):
            for xi in range(2):
                rows = slice(c * 4 + xi * 2, c * 4 + xi * 2 + 2)
                F[c, 2 + 2 * p + xi, OWN - 2 : OWN, :] = YRG[0, p, rows, :]
                F[c, 2 + 2 * p + xi, OWN + CY : OWN + CY + 2, :] = YRG[1, p, rows, :]
        return 0

    lax.fori_loop(0, PAIRS, open_y_geo, 0)

    def z_rows(x, _):
        z_geo(x + 2, x // 2 + 1, lax.rem(x, 2), slice(0, 8), 1, BLOCKS - 1, None)
        z_geo(x + 2, x // 2 + 1, lax.rem(x, 2), slice(OWN + CY, OWN + CY + 8), 2, 0, None)
        return 0

    lax.fori_loop(0, CX, z_rows, 0)

    for copy in rest_zs + rest_ys:
        copy.wait_recv()

    def open_y_rest(x, _):
        rows = pl.ds(2 * x, 2)
        for n, c in enumerate(Y_REST):
            R[c, 2 + x, OWN - 2 : OWN, :] = YRR[0, n, rows, :]
            R[c, 2 + x, OWN + CY : OWN + CY + 2, :] = YRR[1, n, rows, :]
        return 0

    lax.fori_loop(0, CX, open_y_rest, 0)

    def x_layer(x):
        def body(b, _):
            rows = pl.ds(pl.multiple_of(8 * b, 8), 8)
            for c in range(GEO):
                taps = [F[c, x + k, rows, :] for k in range(5)]
                DX[c, x, rows, :] = first(taps[0], taps[1], taps[3], taps[4])
                DXX[c, x, rows, :] = second(*taps)
            return 0

        lax.fori_loop(0, ROWS // 8, body, 0)

    def cell(x, b):
        r0 = OWN + 8 * b
        mid = pl.ds(pl.multiple_of(r0, 8), 8)
        own = pl.ds(pl.multiple_of(8 * b, 8), 8)

        def y_of(ref, c, layer):
            return [ref[c, layer, pl.ds(r0 + k, 8), :] for k in (-2, -1, 1, 2)]

        def x_of(ref, c):
            return [ref[c, x + 2 + k, mid, :] for k in (-2, -1, 1, 2)]

        g = [F[1 + n, x + 2, mid, :] for n in range(6)]
        chi = F[0, x + 2, mid, :]
        gu = inverse_of(g)
        wide = [gu[0], 2.0 * gu[1], 2.0 * gu[2], gu[3], 2.0 * gu[4], gu[5]]
        same = [12.0 * gu[0], 12.0 * gu[3], 12.0 * gu[5]]

        grads, bend = [[], [], []], []
        for c in range(GEO):
            f = F[c, x + 2, mid, :]
            ys = y_of(F, c, x + 2)
            grads[0].append(DX[c, x, mid, :])
            grads[1].append(first(*ys))
            grads[2].append(DZ[c, x + 2, mid, :])
            bend.append(
                same[0] * DXX[c, x, mid, :]
                + same[1] * second(ys[0], ys[1], f, ys[2], ys[3])
                + same[2] * DZZ[c, x, own, :]
                + wide[1] * first(*y_of(DX, c, x))
                + wide[2] * first(*x_of(DZ, c))
                + wide[4] * first(*y_of(DZ, c, x + 2))
            )
        dchi = [grads[a][0] for a in range(3)]
        bend_g = sum(wide[n] * bend[1 + n] for n in range(1, 6)) + wide[0] * bend[1]

        def d(a, i, j):
            return grads[a][1 + PAIR[i][j]]

        def inv(i, j):
            return gu[PAIR[i][j]]

        trace, low = [], []
        for a in range(3):
            t = wide[0] * grads[a][1]
            for n in range(1, 6):
                t = t + wide[n] * grads[a][1 + n]
            trace.append(t)
            e = gu[0] * d(0, 0, a) + gu[3] * d(1, 1, a) + gu[5] * d(2, 2, a)
            e = e + gu[1] * (d(0, 1, a) + d(1, 0, a)) + gu[2] * (d(0, 2, a) + d(2, 0, a))
            e = e + gu[4] * (d(1, 2, a) + d(2, 1, a))
            low.append(e - 0.5 * t)
        gd = [inv(k, 0) * low[0] + inv(k, 1) * low[1] + inv(k, 2) * low[2] for k in range(3)]

        cyc = {
            (0, 0, 0): 3.0 * d(0, 0, 0), (1, 1, 1): 3.0 * d(1, 1, 1), (2, 2, 2): 3.0 * d(2, 2, 2),
            (0, 0, 1): 2.0 * d(0, 0, 1) + d(1, 0, 0), (0, 0, 2): 2.0 * d(0, 0, 2) + d(2, 0, 0),
            (0, 1, 1): 2.0 * d(1, 0, 1) + d(0, 1, 1), (1, 1, 2): 2.0 * d(1, 1, 2) + d(2, 1, 1),
            (0, 2, 2): 2.0 * d(2, 0, 2) + d(0, 2, 2), (1, 2, 2): 2.0 * d(2, 1, 2) + d(1, 2, 2),
            (0, 1, 2): d(0, 1, 2) + d(1, 0, 2) + d(2, 0, 1),
        }

        def s(*idx):
            return cyc[tuple(sorted(idx))]

        up = [[[None] * 3 for _ in range(3)] for _ in range(3)]
        for i in range(3):
            for l in range(3):
                for j in range(l, 3):
                    value = inv(i, 0) * s(0, l, j) + inv(i, 1) * s(1, l, j) + inv(i, 2) * s(2, l, j)
                    up[l][i][j] = value
                    up[j][i][l] = value
        squares = None
        for l in range(3):
            for m in range(l, 3):
                if l == m:
                    diag = up[l][0][0] * up[l][0][0] + up[l][1][1] * up[l][1][1] + up[l][2][2] * up[l][2][2]
                    off = up[l][0][1] * up[l][1][0] + up[l][0][2] * up[l][2][0] + up[l][1][2] * up[l][2][1]
                    trc = diag + 2.0 * off
                else:
                    trc = sum(up[l][i][j] * up[m][j][i] for i in range(3) for j in range(3) if i + j) + (
                        up[l][0][0] * up[m][0][0]
                    )
                term = wide[PAIR[l][m]] * trc
                squares = term if squares is None else squares + term

        t0 = lax.rem(x, 2) * BLOCKS + b
        left, right = ZRR[0, x // 2], ZRR[1, x // 2]
        rest_grad = [[], [], []]
        for n in range(7):
            tile = R[n, x + 2, mid, :]
            rest_grad[0].append(first(*x_of(R, n)))
            rest_grad[1].append(first(*y_of(R, n, x + 2)))
            rest_grad[2].append(first(*z_taps(tile, left, right, 2 * n * BLOCKS + t0)))
        div = first(*x_of(R, 7)) + first(*y_of(R, 8, x + 2))
        div = div + first(*z_taps(R[9, x + 2, mid, :], left, right, 14 * BLOCKS + t0))
        A = [R[n, x + 2, mid, :] for n in range(6)]
        K = R[6, x + 2, mid, :]

        mixed = [
            [A[PAIR[i][0]] * inv(0, j) + A[PAIR[i][1]] * inv(1, j) + A[PAIR[i][2]] * inv(2, j) for j in range(3)]
            for i in range(3)
        ]
        raised = [
            inv(i, 0) * mixed[0][j] + inv(i, 1) * mixed[1][j] + inv(i, 2) * mixed[2][j]
            for i, j in ((0, 0), (0, 1), (0, 2), (1, 1), (1, 2), (2, 2))
        ]
        a_sq = mixed[0][0] * mixed[0][0] + mixed[1][1] * mixed[1][1] + mixed[2][2] * mixed[2][2]
        a_sq = a_sq + 2.0 * (
            mixed[0][1] * mixed[1][0] + mixed[0][2] * mixed[2][0] + mixed[1][2] * mixed[2][1]
        )
        chi_inv = 1.0 / chi
        dchi_up = [inv(k, 0) * dchi[0] + inv(k, 1) * dchi[1] + inv(k, 2) * dchi[2] for k in range(3)]
        grad_sq = dchi_up[0] * dchi[0] + dchi_up[1] * dchi[1] + dchi_up[2] * dchi[2]
        gd_trace = gd[0] * trace[0] + gd[1] * trace[1] + gd[2] * trace[2]
        gd_chi = gd[0] * dchi[0] + gd[1] * dchi[1] + gd[2] * dchi[2]
        ricci = 0.5 * (gd_trace - bend_g) + squares * (1.0 / 12.0) + 12.0 * div
        ham = (chi * ricci + 2.0 * (bend[0] - gd_chi) - 2.5 * grad_sq * chi_inv) * (1.0 / 144.0)
        OUT[0, x, own, :] = ham + (2.0 / 3.0) * (K * K) - a_sq

        weight = 1.5 * chi_inv
        vec = [gd[l] + weight * dchi_up[l] for l in range(3)]
        twice = [0.5 * raised[0], raised[1], raised[2], 0.5 * raised[3], raised[4], 0.5 * raised[5]]
        for i in range(3):
            total = (-2.0 / 3.0) * rest_grad[i][6]
            for j in range(3):
                for k in range(3):
                    total = total + inv(j, k) * rest_grad[j][PAIR[k][i]]
            for l in range(3):
                total = total - vec[l] * A[PAIR[l][i]]
            for n in range(6):
                total = total - twice[n] * grads[i][1 + n]
            OUT[1 + i, x, own, :] = total * (1.0 / 12.0)

    def tally(x, b):
        own = pl.ds(pl.multiple_of(8 * b, 8), 8)
        ham, m0, m1, m2 = [OUT[n, x, own, :] for n in range(4)]
        ACC[0] += ham * ham
        ACC[1] += m0 * m0 + m1 * m1 + m2 * m2

    def term(d, b):
        rows = pl.ds(8 * b, 8)
        return remote(CS.at[d, :, :, rows], CR.at[1 - d, :, :, rows], S_TERM + 4 * d + b, at(2 * d - 1, 0, 0))

    terms = [[term(d, b) for b in range(BLOCKS)] for d in range(2)]

    def send_terms(b):
        mid = pl.ds(OWN + 8 * b, 8)
        for d in range(2):
            geo_xs[d][b].wait_recv()
        for d in range(2):
            halo = CX + 2 if d else 0
            for k in range(2):
                gu = inverse_of([F[1 + n, halo + k, mid, :] for n in range(6)])
                chi = F[0, halo + k, mid, :]

                def part(n):
                    if d == 0:
                        f0 = R[n, 2, mid, :]
                        return -f0 if k == 0 else 8.0 * f0 - R[n, 3, mid, :]
                    f7 = R[n, CX + 1, mid, :]
                    return R[n, CX, mid, :] - 8.0 * f7 if k == 0 else f7

                a = [part(n) for n in range(8)]
                own = pl.ds(8 * b, 8)
                CS[d, 0, k, own, :] = chi * a[7] * (1.0 / 12.0)
                for i in range(3):
                    value = gu[0] * a[PAIR[0][i]] + gu[1] * a[PAIR[1][i]] + gu[2] * a[PAIR[2][i]]
                    if i == 0:
                        value = value - (2.0 / 3.0) * a[6]
                    CS[d, 1 + i, k, own, :] = value * (1.0 / 12.0)
        for d in range(2):
            terms[d][b].start()

    def inner(x):
        x_layer(x)

        def body(b, _):
            cell(x, b)
            tally(x, b)
            return 0

        lax.fori_loop(0, BLOCKS, body, 0)

    def inner_layer(x, _):
        inner(x)
        return 0

    for b in range(BLOCKS):
        send_terms(b)
        lax.fori_loop(2 + b, 3 + b, inner_layer, 0)

    for copy in edge_xy + edge_xz:
        copy.wait_recv()
    for xs in range(2):
        for ys in range(2):
            for c in range(GEO):
                for k in range(2):
                    layer = (CX + 2 if xs else 0) + k
                    row = OWN + CY if ys else OWN - 2
                    F[c, layer, row : row + 2, :] = XYR[xs, ys, c * 4 + k * 2 : c * 4 + k * 2 + 2, :]

    def z_edge(i, _):
        k, b = i // BLOCKS, lax.rem(i, BLOCKS)
        side, xi = k // 2, lax.rem(k, 2)
        z_geo(
            side * (CX + 2) + xi, side * (PAIRS + 1), xi, pl.ds(pl.multiple_of(OWN + 8 * b, 8), 8), 0, b, None
        )
        return 0

    lax.fori_loop(0, 4 * BLOCKS, z_edge, 0)

    def edge_layer(k, _):
        x = k + (k // 2) * (CX - 4)
        x_layer(x)

        def body(b, _):
            cell(x, b)
            return 0

        lax.fori_loop(0, BLOCKS, body, 0)
        return 0

    lax.fori_loop(0, 4, edge_layer, 0)

    for d in range(2):
        for b in range(BLOCKS):
            terms[d][b].wait_recv()

    def finish(k, _):
        side, sub = k // 2, lax.rem(k, 2)
        x = k + side * (CX - 4)
        for n in range(4):
            OUT[n, x] = OUT[n, x] + CR[side, n, sub]
        for b in range(BLOCKS):
            tally(x, b)
        return 0

    lax.fori_loop(0, 4, finish, 0)
    stores = [
        pltpu.make_async_copy(OUT.at[0], ham_out, out_sem.at[0]),
        pltpu.make_async_copy(OUT.at[1:4], mom_out, out_sem.at[1]),
    ]
    for copy in stores:
        copy.start()

    MINE[0, 0:1, :] = jnp.sum(ACC[0], axis=0, keepdims=True)
    MINE[0, 1:2, :] = jnp.sum(ACC[1], axis=0, keepdims=True)
    SUM_A[rank_a] = MINE[0]

    def plane_copy(j):
        rank, peer = plane_peer(j)
        return pltpu.make_async_remote_copy(
            src_ref=MINE.at[0], dst_ref=SUM_A.at[rank_a], send_sem=send_sem.at[S_SUM_A + rank],
            recv_sem=recv_sem.at[S_SUM_A + rank_a], device_id=peer, device_id_type=MESH,
        )

    def plane_start(j, _):
        plane_copy(j).start()
        return 0

    def plane_wait(j, _):
        rank, peer = plane_peer(j)
        pltpu.make_async_remote_copy(
            src_ref=MINE.at[0], dst_ref=SUM_A.at[rank], send_sem=send_sem.at[S_SUM_A + rank],
            recv_sem=recv_sem.at[S_SUM_A + rank], device_id=peer, device_id_type=MESH,
        ).wait()
        return 0

    lax.fori_loop(1, n_plane, plane_start, 0)
    lax.fori_loop(1, n_plane, plane_wait, 0)
    MINE[1] = lax.fori_loop(1, n_plane, lambda j, acc: acc + SUM_A[j], SUM_A[0])
    SUM_B[ix] = MINE[1]

    def line_copy(j, receiving):
        rank = lax.rem(ix + j, n_gx)
        slot = rank if receiving else ix
        return pltpu.make_async_remote_copy(
            src_ref=MINE.at[1], dst_ref=SUM_B.at[slot], send_sem=send_sem.at[S_SUM_B + rank],
            recv_sem=recv_sem.at[S_SUM_B + slot], device_id=(rank, iy, iz), device_id_type=MESH,
        )

    for j in range(1, n_gx):
        line_copy(j, False).start()
    for j in range(1, n_gx):
        line_copy(j, True).wait()
    total = SUM_B[0]
    for j in range(1, n_gx):
        total = total + SUM_B[j]
    sums = jnp.sum(total, axis=1, keepdims=True)
    cells = float(CX * CY * CZ * n_gx * n_gy * n_gz)
    column = lax.broadcasted_iota(jnp.int32, (1, 2), 1)
    ham_sum = jnp.broadcast_to(sums[0:1], (1, 2))
    mom_sum = jnp.broadcast_to(sums[1:2], (1, 2))
    norm_out[...] = jnp.sqrt(jnp.where(column == 0, ham_sum / cells, mom_sum / (3.0 * cells)))

    for copy in [c for row in geo_xs + terms for c in row] + geo_ys + geo_zs + edge_xy + edge_yz + edge_xz:
        copy.wait_send()
    for copy in rest_ys + rest_zs:
        copy.wait_send()
    for copy in stores:
        copy.wait()


def solution(mesh):
    sizes = (mesh.shape["gx"], mesh.shape["gy"], mesh.shape["gz"])
    n_plane = sizes[1] * sizes[2]
    f32 = jnp.float32

    def step(chi, met, cur, trk, gam):
        vm = lambda *shape: pltpu.VMEM(shape, f32)
        ham, mom, norm = pl.pallas_call(
            functools.partial(kernel, sizes),
            out_shape=(
                jax.ShapeDtypeStruct((CX, CY, CZ), f32),
                jax.ShapeDtypeStruct((3, CX, CY, CZ), f32),
                jax.ShapeDtypeStruct((1, 2), f32),
            ),
            in_specs=[pl.BlockSpec(memory_space=pl.ANY)] * 5,
            out_specs=(
                pl.BlockSpec(memory_space=pl.ANY),
                pl.BlockSpec(memory_space=pl.ANY),
                pl.BlockSpec(memory_space=pltpu.VMEM),
            ),
            scratch_shapes=[
                vm(GEO, LX, ROWS, CZ), vm(REST, LX, ROWS, CZ),
                vm(GEO, LX, ROWS, CZ), vm(GEO, CX, CY, CZ),
                vm(GEO, CX, ROWS, CZ), vm(GEO, CX, ROWS, CZ),
                vm(4, CX, CY, CZ), vm(2, 8, CZ),
                vm(2, PAIRS, 32, CZ), vm(2, 8, 2 * CX, CZ),
                vm(2, PAIRS, 32, CZ), vm(2, 8, 2 * CX, CZ),
                vm(2, 2, 32, CZ),
                vm(2, PAIRS, 8, CZ), vm(2, PAIRS, 8, CZ),
                vm(2, 3, PAIRS + 2, 8, CZ), vm(2, PAIRS, 8, CZ),
                vm(2, 4, 2, CY, CZ), vm(2, 4, 2, CY, CZ),
                vm(2, 2, CZ), vm(n_plane, 2, CZ), vm(sizes[0], 2, CZ),
                pltpu.SemaphoreType.DMA((5,)),
                pltpu.SemaphoreType.DMA((2,)),
                pltpu.SemaphoreType.DMA((S_COUNT,)),
                pltpu.SemaphoreType.DMA((S_COUNT,)),
            ],
            compiler_params=pltpu.CompilerParams(collective_id=0, has_side_effects=True),
        )(chi, met, cur, trk, gam)
        return ham, mom, norm.reshape(2)

    return jax.shard_map(
        step,
        mesh=mesh,
        in_specs=(
            P("gx", "gy", "gz"),
            P(None, "gx", "gy", "gz"),
            P(None, "gx", "gy", "gz"),
            P("gx", "gy", "gz"),
            P(None, "gx", "gy", "gz"),
        ),
        out_specs=(P("gx", "gy", "gz"), P(None, "gx", "gy", "gz"), P()),
        check_vma=False,
    )
```

```python
import functools

import jax
import jax.numpy as jnp
from jax import lax
from jax.experimental import pallas as pl
from jax.experimental.pallas import tpu as pltpu
from jax.sharding import PartitionSpec as P

MESH = pl.DeviceIdType.MESH
PAIR = ((0, 1, 2), (1, 3, 4), (2, 4, 5))

CX, CY, CZ = 8, 32, 128
LX, ROWS, OWN = CX + 4, 48, 8
BLOCKS = CY // 8
PAIRS = CX // 2
GEO, REST = 7, 10
Y_REST = (0, 1, 2, 3, 4, 5, 6, 8)
Z_REST = (0, 1, 2, 3, 4, 5, 6, 9)
X_REST = 8

S_GEO_X, S_EDGE_XY, S_EDGE_YZ, S_EDGE_XZ = 0, 8, 12, 16
S_GEO_Y, S_GEO_Z, S_REST_Y, S_REST_Z, S_TERM, S_ENDS_X = 20, 22, 24, 26, 28, 36
S_SUM_A, S_SUM_B, S_COUNT = 38, 39, 40


def lane_ids():
    return lax.broadcasted_iota(jnp.int32, (8, CZ), 1)


def inverse_of(g):
    g00, g01, g02, g11, g12, g22 = g
    m00 = g11 * g22 - g12 * g12
    m01 = g02 * g12 - g01 * g22
    m02 = g01 * g12 - g02 * g11
    m11 = g00 * g22 - g02 * g02
    m12 = g01 * g02 - g00 * g12
    m22 = g00 * g11 - g01 * g01
    scale = 1.0 / (g00 * m00 + g01 * m01 + g02 * m02)
    return [m00 * scale, m01 * scale, m02 * scale, m11 * scale, m12 * scale, m22 * scale]


def first(lo2, lo1, hi1, hi2):
    return (lo2 - hi2) + 8.0 * (hi1 - lo1)


def second(lo2, lo1, mid, hi1, hi2):
    return 16.0 * (lo1 + hi1) - (lo2 + hi2) - 30.0 * mid


def kernel(
    sizes,
    chi_in, met_in, cur_in, trk_in, gam_in,
    ham_out, mom_out, norm_out,
    F, R, DZ, DZZ, DZR, DX, DXX, ACC,
    YSG, YSR, YRG, YRR, YDZ, YZR, XYR,
    ZP, ZPR, C1, C2, XE, XER, CXE,
    CS, CR, MINE, SUM_A, SUM_B,
    load_sem, send_sem, recv_sem, near_sem, far_sem,
):
    n_gx, n_gy, n_gz = sizes
    ix, iy, iz = lax.axis_index("gx"), lax.axis_index("gy"), lax.axis_index("gz")
    xs = {k: lax.rem(ix + k + n_gx, n_gx) for k in range(-2, n_gx)}
    ys = {k: lax.rem(iy + k + n_gy, n_gy) for k in range(-1, n_gy)}
    zs = {k: lax.rem(iz + k + n_gz, n_gz) for k in range(-2, n_gz)}

    def at(dx, dy, dz):
        return xs[dx], ys[dy], zs[dz]

    def remote(src, dst, place, device):
        return pltpu.make_async_remote_copy(
            src_ref=src, dst_ref=dst, send_sem=send_sem.at[place], recv_sem=recv_sem.at[place],
            device_id=device, device_id_type=MESH,
        )

    loads = [
        (chi_in, F.at[0, 2 : 2 + CX, OWN : OWN + CY]),
        (met_in, F.at[1:7, 2 : 2 + CX, OWN : OWN + CY]),
        (cur_in, R.at[0:6, 2 : 2 + CX, OWN : OWN + CY]),
        (trk_in, R.at[6, 2 : 2 + CX, OWN : OWN + CY]),
        (gam_in, R.at[7:10, 2 : 2 + CX, OWN : OWN + CY]),
    ]
    loads = [pltpu.make_async_copy(s, d, load_sem.at[i]) for i, (s, d) in enumerate(loads)]
    for copy in loads:
        copy.start()

    barrier = pltpu.get_barrier_semaphore()
    faces = [(-1, 0, 0), (1, 0, 0), (0, -1, 0), (0, 1, 0), (0, 0, -1), (0, 0, 1)]
    for step in faces:
        pl.semaphore_signal(barrier, inc=1, device_id=at(*step), device_id_type=MESH)

    lane = lane_ids()
    lane4, place = lane // 4, lax.rem(lane, 4)
    ends = (lane < 2) | (lane >= CZ - 2)
    zero = jnp.zeros((8, CZ), jnp.float32)

    def clear(c, _):
        for layer in (0, 1, LX - 2, LX - 1):
            for b in range(BLOCKS):
                R[c, layer, pl.ds(OWN + 8 * b, 8), :] = zero
        return 0

    lax.fori_loop(0, X_REST, clear, 0)
    ACC[...] = jnp.zeros_like(ACC)

    def packed(tiles):
        out = zero
        for t, tile in enumerate(tiles):
            turn = (4 * t + 2) % CZ
            out = jnp.where(lane4 == t, pltpu.roll(tile, turn, 1) if turn else tile, out)
        return out

    def pack_geo(c, _):
        ZP[c] = packed([F[c, 2 + x, pl.ds(OWN + 8 * b, 8), :] for x in range(CX) for b in range(BLOCKS)])
        return 0

    def pack_rest(n, _):
        c = n + (n // 7) * 2
        ZP[GEO + n] = packed([R[c, 2 + x, pl.ds(OWN + 8 * b, 8), :] for x in range(CX) for b in range(BLOCKS)])
        return 0

    def pack_y_geo(p, _):
        for c in range(GEO):
            for xi in range(2):
                rows = pl.ds(32 * p + c * 4 + xi * 2, 2)
                YSG[0, rows, :] = F[c, 2 + 2 * p + xi, OWN : OWN + 2, :]
                YSG[1, rows, :] = F[c, 2 + 2 * p + xi, OWN + CY - 2 : OWN + CY, :]
        return 0

    def pack_y_rest(x, _):
        rows = pl.ds(2 * x, 2)
        for n, c in enumerate(Y_REST):
            YSR[0, n, rows, :] = R[c, 2 + x, OWN : OWN + 2, :]
            YSR[1, n, rows, :] = R[c, 2 + x, OWN + CY - 2 : OWN + CY, :]
        return 0

    for s in range(2):
        for p in range(PAIRS):
            YSG[s, 32 * p + 24 : 32 * p + 32, :] = zero
    loads[0].wait()
    loads[1].wait()
    lax.fori_loop(0, PAIRS, pack_y_geo, 0)
    lax.fori_loop(0, GEO, pack_geo, 0)
    for s in range(2):
        YSG[s, 128:136, :] = packed([YSG[s, 8 * k : 8 * k + 8, :] for k in range(16)])
        for v in range(2):
            out = zero
            for c in range(4 * v, min(4 * v + 4, GEO)):
                turn = (32 * (c % 4) - 96 * s) % CZ
                out = jnp.where(lane // 32 == c % 4, pltpu.roll(ZP[c], turn, 1) if turn else ZP[c], out)
            XE[s, v] = out
    for copy in loads[2:]:
        copy.wait()
    lax.fori_loop(0, CX, pack_y_rest, 0)
    lax.fori_loop(0, 8, pack_rest, 0)

    def geo_x(d, b):
        rows = pl.ds(OWN + 8 * b, 8)
        src = F.at[0:GEO, pl.ds(CX if d else 2, 2), rows]
        dst = F.at[0:GEO, pl.ds(0 if d else CX + 2, 2), rows]
        return remote(src, dst, S_GEO_X + 4 * d + b, at(2 * d - 1, 0, 0))

    geo_xs = [[geo_x(d, b) for b in range(BLOCKS)] for d in range(2)]
    ends_x = [remote(XE.at[d], XER.at[1 - d, 0], S_ENDS_X + d, at(2 * d - 1, 0, 0)) for d in range(2)]
    geo_ys = [remote(YSG.at[d], YRG.at[1 - d], S_GEO_Y + d, at(0, 2 * d - 1, 0)) for d in range(2)]
    geo_zs = [remote(ZP.at[0:GEO], ZPR.at[1 - d, 0:GEO], S_GEO_Z + d, at(0, 0, 2 * d - 1)) for d in range(2)]
    rest_ys = [remote(YSR.at[d], YRR.at[1 - d], S_REST_Y + d, at(0, 2 * d - 1, 0)) for d in range(2)]
    rest_zs = [
        remote(ZP.at[GEO : GEO + 8], ZPR.at[1 - d, GEO : GEO + 8], S_REST_Z + d, at(0, 0, 2 * d - 1)) for d in range(2)
    ]
    combos = [(a, b) for a in range(2) for b in range(2)]
    edge_xy = [
        remote(
            YSG.at[dy, pl.ds(96 if dx else 0, 32)], XYR.at[1 - dx, 1 - dy], S_EDGE_XY + 2 * dx + dy,
            at(2 * dx - 1, 2 * dy - 1, 0),
        )
        for dx, dy in combos
    ]
    edge_yz = [
        remote(
            YSG.at[dy, 128:136], YZR.at[1 - dz, 1 - dy], S_EDGE_YZ + 2 * dy + dz, at(0, 2 * dy - 1, 2 * dz - 1)
        )
        for dy, dz in combos
    ]
    edge_xz = [
        remote(XE.at[dx], XER.at[1 - dx, 2 - dz], S_EDGE_XZ + 2 * dx + dz, at(2 * dx - 1, 0, 2 * dz - 1))
        for dx, dz in combos
    ]

    pl.semaphore_wait(barrier, len(faces))
    for copy in geo_xs[0][:1] + geo_xs[1][:1] + geo_zs + geo_ys + rest_zs + rest_ys:
        copy.start()
    for b in range(1, BLOCKS):
        for d in range(2):
            geo_xs[d][b].start()
    for copy in ends_x:
        copy.start()

    def wrapped(tile):
        return (
            pltpu.roll(tile, 2, 1), pltpu.roll(tile, 1, 1), pltpu.roll(tile, CZ - 1, 1), pltpu.roll(tile, CZ - 2, 1)
        )

    def z_geo(x, _):
        for c in range(GEO):
            for b in range(BLOCKS):
                rows = pl.ds(OWN + 8 * b, 8)
                tile = F[c, x + 2, rows, :]
                taps = wrapped(tile)
                DZ[c, x + 2, rows, :] = first(*taps)
                DZZ[c, x, pl.ds(8 * b, 8), :] = second(taps[0], taps[1], tile, taps[2], taps[3])
        return 0

    def z_rest(x, _):
        for n, c in enumerate(Z_REST):
            for b in range(BLOCKS):
                DZR[n, x, pl.ds(8 * b, 8), :] = first(*wrapped(R[c, x + 2, pl.ds(OWN + 8 * b, 8), :]))
        return 0

    def x_rows(layers, tiles):
        def body(i, _):
            x, b = layers(i // len(tiles)), lax.rem(i, len(tiles))
            b = tiles[0] + b * (tiles[1] - tiles[0])
            rows = pl.ds(pl.multiple_of(8 * b, 8), 8)
            for c in range(GEO):
                taps = [F[c, x + k, rows, :] for k in range(5)]
                DX[c, x, rows, :] = first(taps[0], taps[1], taps[3], taps[4])
                DXX[c, x, rows, :] = second(*taps)
            return 0

        lax.fori_loop(0, 4 * len(tiles), body, 0)

    lax.fori_loop(0, CX, z_geo, 0)
    for copy in geo_zs:
        copy.wait_recv()
    for copy in edge_yz + edge_xz:
        copy.start()

    def change(own, left, right):
        e = jnp.where(place < 2, left, right) - own
        hi2, hi1, lo1, lo2 = (pltpu.roll(e, k, 1) for k in (CZ - 2, CZ - 1, 1, 2))
        hi1 = jnp.where(place == 1, hi1, 0.0)
        lo1 = jnp.where(place == 2, lo1, 0.0)
        return (
            jnp.where(place < 2, 8.0 * hi1 - hi2, lo2 - 8.0 * lo1),
            16.0 * (hi1 + lo1) - jnp.where(place < 2, hi2, lo2),
        )

    def at_ends(change, turn):
        return jnp.where(ends, pltpu.roll(change, turn, 1), 0.0)

    for c in range(GEO):
        C1[c], C2[c] = change(ZP[c], ZPR[0, c], ZPR[1, c])

    def z_ends(x, _):
        for c in range(GEO):
            changed = C1[c]
            for b in range(BLOCKS):
                rows = pl.ds(OWN + 8 * b, 8)
                DZ[c, x + 2, rows, :] += at_ends(changed, CZ - 2 - 4 * (BLOCKS * x + b))
        return 0

    lax.fori_loop(0, CX, z_ends, 0)
    x_rows(lambda k: k + 2, (1, 2, 3, 4))
    lax.fori_loop(0, CX, z_rest, 0)
    for copy in rest_zs + rest_ys:
        copy.wait_recv()
    for n in range(8):
        C1[GEO + n] = change(ZP[GEO + n], ZPR[0, GEO + n], ZPR[1, GEO + n])[0]

    def open_y_rest(x, _):
        rows = pl.ds(2 * x, 2)
        for n, c in enumerate(Y_REST):
            R[c, 2 + x, OWN - 2 : OWN, :] = YRR[0, n, rows, :]
            R[c, 2 + x, OWN + CY : OWN + CY + 2, :] = YRR[1, n, rows, :]
        return 0

    lax.fori_loop(0, CX, open_y_rest, 0)
    for copy in geo_ys:
        copy.wait_recv()
    for copy in edge_xy:
        copy.start()

    def open_y_geo(p, _):
        for c in range(GEO):
            for xi in range(2):
                rows = pl.ds(32 * p + c * 4 + xi * 2, 2)
                F[c, 2 + 2 * p + xi, OWN - 2 : OWN, :] = YRG[0, rows, :]
                F[c, 2 + 2 * p + xi, OWN + CY : OWN + CY + 2, :] = YRG[1, rows, :]
        return 0

    lax.fori_loop(0, PAIRS, open_y_geo, 0)
    x_rows(lambda k: k + 2, (0, 5))

    def y_ends(s, _):
        changed = change(YRG[s, 128:136, :], YZR[0, s], YZR[1, s])[0]
        for k in range(16):
            rows = slice(8 * k, 8 * k + 8)
            YDZ[s, rows, :] = first(*wrapped(YRG[s, rows, :])) + at_ends(changed, CZ - 2 - 4 * k)
        return 0

    def open_y_dz(p, _):
        for c in range(GEO):
            for xi in range(2):
                rows = pl.ds(32 * p + c * 4 + xi * 2, 2)
                DZ[c, 2 + 2 * p + xi, OWN - 2 : OWN, :] = YDZ[0, rows, :]
                DZ[c, 2 + 2 * p + xi, OWN + CY : OWN + CY + 2, :] = YDZ[1, rows, :]
        return 0

    def cell(x, b):
        r0 = OWN + 8 * b
        mid = pl.ds(pl.multiple_of(r0, 8), 8)
        own = pl.ds(pl.multiple_of(8 * b, 8), 8)
        turn = CZ - 2 - 4 * (BLOCKS * x + b)

        def y_of(ref, c, layer):
            return [ref[c, layer, pl.ds(r0 + k, 8), :] for k in (-2, -1, 1, 2)]

        def x_of(ref, c):
            return [ref[c, x + 2 + k, mid, :] for k in (-2, -1, 1, 2)]

        g = [F[1 + n, x + 2, mid, :] for n in range(6)]
        chi = F[0, x + 2, mid, :]
        gu = inverse_of(g)
        wide = [gu[0], 2.0 * gu[1], 2.0 * gu[2], gu[3], 2.0 * gu[4], gu[5]]
        same = [12.0 * gu[0], 12.0 * gu[3], 12.0 * gu[5]]

        grads, bend = [[], [], []], []
        for c in range(GEO):
            f = F[c, x + 2, mid, :]
            ys = y_of(F, c, x + 2)
            grads[0].append(DX[c, x, mid, :])
            grads[1].append(first(*ys))
            grads[2].append(DZ[c, x + 2, mid, :])
            bend.append(
                same[0] * DXX[c, x, mid, :]
                + same[1] * second(ys[0], ys[1], f, ys[2], ys[3])
                + same[2] * (DZZ[c, x, own, :] + at_ends(C2[c], turn))
                + wide[1] * first(*y_of(DX, c, x))
                + wide[2] * first(*x_of(DZ, c))
                + wide[4] * first(*y_of(DZ, c, x + 2))
            )
        dchi = [grads[a][0] for a in range(3)]
        bend_g = sum(wide[n] * bend[1 + n] for n in range(1, 6)) + wide[0] * bend[1]

        def d(a, i, j):
            return grads[a][1 + PAIR[i][j]]

        def inv(i, j):
            return gu[PAIR[i][j]]

        trace, low = [], []
        for a in range(3):
            t = wide[0] * grads[a][1]
            for n in range(1, 6):
                t = t + wide[n] * grads[a][1 + n]
            trace.append(t)
            e = gu[0] * d(0, 0, a) + gu[3] * d(1, 1, a) + gu[5] * d(2, 2, a)
            e = e + gu[1] * (d(0, 1, a) + d(1, 0, a)) + gu[2] * (d(0, 2, a) + d(2, 0, a))
            e = e + gu[4] * (d(1, 2, a) + d(2, 1, a))
            low.append(e - 0.5 * t)
        gd = [inv(k, 0) * low[0] + inv(k, 1) * low[1] + inv(k, 2) * low[2] for k in range(3)]

        cyc = {
            (0, 0, 0): 3.0 * d(0, 0, 0), (1, 1, 1): 3.0 * d(1, 1, 1), (2, 2, 2): 3.0 * d(2, 2, 2),
            (0, 0, 1): 2.0 * d(0, 0, 1) + d(1, 0, 0), (0, 0, 2): 2.0 * d(0, 0, 2) + d(2, 0, 0),
            (0, 1, 1): 2.0 * d(1, 0, 1) + d(0, 1, 1), (1, 1, 2): 2.0 * d(1, 1, 2) + d(2, 1, 1),
            (0, 2, 2): 2.0 * d(2, 0, 2) + d(0, 2, 2), (1, 2, 2): 2.0 * d(2, 1, 2) + d(1, 2, 2),
            (0, 1, 2): d(0, 1, 2) + d(1, 0, 2) + d(2, 0, 1),
        }

        def s(*idx):
            return cyc[tuple(sorted(idx))]

        up = [[[None] * 3 for _ in range(3)] for _ in range(3)]
        for i in range(3):
            for l in range(3):
                for j in range(l, 3):
                    value = inv(i, 0) * s(0, l, j) + inv(i, 1) * s(1, l, j) + inv(i, 2) * s(2, l, j)
                    up[l][i][j] = value
                    up[j][i][l] = value
        squares = None
        for l in range(3):
            for m in range(l, 3):
                if l == m:
                    diag = up[l][0][0] * up[l][0][0] + up[l][1][1] * up[l][1][1] + up[l][2][2] * up[l][2][2]
                    off = up[l][0][1] * up[l][1][0] + up[l][0][2] * up[l][2][0] + up[l][1][2] * up[l][2][1]
                    trc = diag + 2.0 * off
                else:
                    trc = sum(up[l][i][j] * up[m][j][i] for i in range(3) for j in range(3) if i + j) + (
                        up[l][0][0] * up[m][0][0]
                    )
                term = wide[PAIR[l][m]] * trc
                squares = term if squares is None else squares + term

        def z_of(n):
            return DZR[n, x, own, :] + at_ends(C1[GEO + n], turn)

        rest_grad = [[], [], []]
        for n in range(7):
            rest_grad[0].append(first(*x_of(R, n)))
            rest_grad[1].append(first(*y_of(R, n, x + 2)))
            rest_grad[2].append(z_of(n))
        div = first(*x_of(R, 7)) + first(*y_of(R, 8, x + 2)) + z_of(7)
        A = [R[n, x + 2, mid, :] for n in range(6)]
        K = R[6, x + 2, mid, :]

        mixed = [
            [A[PAIR[i][0]] * inv(0, j) + A[PAIR[i][1]] * inv(1, j) + A[PAIR[i][2]] * inv(2, j) for j in range(3)]
            for i in range(3)
        ]
        raised = [
            inv(i, 0) * mixed[0][j] + inv(i, 1) * mixed[1][j] + inv(i, 2) * mixed[2][j]
            for i, j in ((0, 0), (0, 1), (0, 2), (1, 1), (1, 2), (2, 2))
        ]
        a_sq = mixed[0][0] * mixed[0][0] + mixed[1][1] * mixed[1][1] + mixed[2][2] * mixed[2][2]
        a_sq = a_sq + 2.0 * (
            mixed[0][1] * mixed[1][0] + mixed[0][2] * mixed[2][0] + mixed[1][2] * mixed[2][1]
        )
        chi_inv = 1.0 / chi
        dchi_up = [inv(k, 0) * dchi[0] + inv(k, 1) * dchi[1] + inv(k, 2) * dchi[2] for k in range(3)]
        grad_sq = dchi_up[0] * dchi[0] + dchi_up[1] * dchi[1] + dchi_up[2] * dchi[2]
        gd_trace = gd[0] * trace[0] + gd[1] * trace[1] + gd[2] * trace[2]
        gd_chi = gd[0] * dchi[0] + gd[1] * dchi[1] + gd[2] * dchi[2]
        ricci = 0.5 * (gd_trace - bend_g) + squares * (1.0 / 12.0) + 12.0 * div
        ham = (chi * ricci + 2.0 * (bend[0] - gd_chi) - 2.5 * grad_sq * chi_inv) * (1.0 / 144.0)
        ham_out[x, own, :] = ham + (2.0 / 3.0) * (K * K) - a_sq

        weight = 1.5 * chi_inv
        vec = [gd[l] + weight * dchi_up[l] for l in range(3)]
        twice = [0.5 * raised[0], raised[1], raised[2], 0.5 * raised[3], raised[4], 0.5 * raised[5]]
        for i in range(3):
            total = (-2.0 / 3.0) * rest_grad[i][6]
            for j in range(3):
                for k in range(3):
                    total = total + inv(j, k) * rest_grad[j][PAIR[k][i]]
            for l in range(3):
                total = total - vec[l] * A[PAIR[l][i]]
            for n in range(6):
                total = total - twice[n] * grads[i][1 + n]
            mom_out[i, x, own, :] = total * (1.0 / 12.0)

    def tally(x, b):
        own = pl.ds(pl.multiple_of(8 * b, 8), 8)
        ham = ham_out[x, own, :]
        m0, m1, m2 = [mom_out[n, x, own, :] for n in range(3)]
        ACC[0] += ham * ham
        ACC[1] += m0 * m0 + m1 * m1 + m2 * m2

    def term(d, b):
        rows = pl.ds(8 * b, 8)
        return remote(CS.at[d, :, :, rows], CR.at[1 - d, :, :, rows], S_TERM + 4 * d + b, at(2 * d - 1, 0, 0))

    terms = [[term(d, b) for b in range(BLOCKS)] for d in range(2)]

    def send_terms(b):
        mid = pl.ds(OWN + 8 * b, 8)
        for d in range(2):
            geo_xs[d][b].wait_recv()
        for d in range(2):
            halo = CX + 2 if d else 0
            for k in range(2):
                gu = inverse_of([F[1 + n, halo + k, mid, :] for n in range(6)])
                chi = F[0, halo + k, mid, :]

                def part(n):
                    if d == 0:
                        f0 = R[n, 2, mid, :]
                        return -f0 if k == 0 else 8.0 * f0 - R[n, 3, mid, :]
                    f7 = R[n, CX + 1, mid, :]
                    return R[n, CX, mid, :] - 8.0 * f7 if k == 0 else f7

                a = [part(n) for n in range(8)]
                own = pl.ds(8 * b, 8)
                CS[d, 0, k, own, :] = chi * a[7] * (1.0 / 12.0)
                for i in range(3):
                    value = gu[0] * a[PAIR[0][i]] + gu[1] * a[PAIR[1][i]] + gu[2] * a[PAIR[2][i]]
                    if i == 0:
                        value = value - (2.0 / 3.0) * a[6]
                    CS[d, 1 + i, k, own, :] = value * (1.0 / 12.0)
        for d in range(2):
            terms[d][b].start()

    def inner(lo, hi):
        def body(i, _):
            k = lax.rem(i, 8)
            x, odd, last = 2 + k // 2, lax.rem(k, 2), i // 8
            b = (1 - last) * (1 + odd) + last * 3 * odd
            cell(x, b)
            tally(x, b)
            return 0

        lax.fori_loop(lo, hi, body, 0)

    inner(0, 8)
    for copy in edge_yz:
        copy.wait_recv()
    lax.fori_loop(0, 2, y_ends, 0)
    lax.fori_loop(0, PAIRS, open_y_dz, 0)
    send_terms(0)
    for step in [(-2, 0, 0), (2, 0, 0), (0, 0, -2), (0, 0, 2)]:
        pl.semaphore_signal(near_sem, inc=1, device_id=at(*step), device_id_type=MESH)
    send_terms(1)
    inner(8, 12)
    send_terms(2)
    inner(12, 16)
    send_terms(3)
    pl.semaphore_wait(near_sem, 4)
    for k in range(1, n_gy):
        pl.semaphore_signal(far_sem, inc=1, device_id=at(0, k, 0), device_id_type=MESH)

    for copy in edge_xy + edge_xz + ends_x:
        copy.wait_recv()
    for sx in range(2):
        for sy in range(2):
            for c in range(GEO):
                for k in range(2):
                    layer = (CX + 2 if sx else 0) + k
                    row = OWN + CY if sy else OWN - 2
                    F[c, layer, row : row + 2, :] = XYR[sx, sy, c * 4 + k * 2 : c * 4 + k * 2 + 2, :]
        for v in range(2):
            CXE[sx, v] = change(XER[sx, 0, v], XER[sx, 1, v], XER[sx, 2, v])[0]

    def x_ends(k, _):
        side, xi = k // 2, lax.rem(k, 2)
        layer = side * (CX + 2) + xi
        for c in range(GEO):
            changed = CXE[side, c // 4]
            for b in range(BLOCKS):
                rows = pl.ds(OWN + 8 * b, 8)
                turn = CZ - 2 - 32 * (c % 4) - 4 * (BLOCKS * xi + b)
                DZ[c, layer, rows, :] = first(*wrapped(F[c, layer, rows, :])) + at_ends(changed, turn)
        return 0

    lax.fori_loop(0, 4, x_ends, 0)
    x_rows(lambda k: k + (k // 2) * (CX - 4), (0, 1, 2, 3, 4, 5))

    def edge_cell(i, _):
        k = i // BLOCKS
        cell(k + (k // 2) * (CX - 4), lax.rem(i, BLOCKS))
        return 0

    lax.fori_loop(0, 4 * BLOCKS, edge_cell, 0)

    for d in range(2):
        for b in range(BLOCKS):
            terms[d][b].wait_recv()

    def finish(k, _):
        side, sub = k // 2, lax.rem(k, 2)
        x = k + side * (CX - 4)
        ham_out[x] = ham_out[x] + CR[side, 0, sub]
        for n in range(3):
            mom_out[n, x] = mom_out[n, x] + CR[side, 1 + n, sub]
        for b in range(BLOCKS):
            tally(x, b)
        return 0

    lax.fori_loop(0, 4, finish, 0)
    MINE[0, 0:1, :] = jnp.sum(ACC[0], axis=0, keepdims=True)
    MINE[0, 1:2, :] = jnp.sum(ACC[1], axis=0, keepdims=True)
    rank_a = iy * n_gz + iz
    n_plane = n_gy * n_gz
    SUM_A[rank_a] = MINE[0]
    pl.semaphore_wait(far_sem, n_gy - 1)
    for dy in range(n_gy):
        for dz in range(n_gz):
            if dy or dz:
                remote(MINE.at[0], SUM_A.at[rank_a], S_SUM_A, at(0, dy, dz)).start()
    others = remote(SUM_A.at[pl.ds(0, n_plane - 1)], SUM_A.at[pl.ds(0, n_plane - 1)], S_SUM_A, at(0, 1, 0))
    others.wait_recv()
    total = SUM_A[0]
    for k in range(1, n_plane):
        total = total + SUM_A[k]
    MINE[1] = total
    SUM_B[ix] = total
    for dx in range(1, n_gx):
        remote(MINE.at[1], SUM_B.at[ix], S_SUM_B, at(dx, 0, 0)).start()
    along = remote(SUM_B.at[pl.ds(0, n_gx - 1)], SUM_B.at[pl.ds(0, n_gx - 1)], S_SUM_B, at(1, 0, 0))
    along.wait_recv()
    total = SUM_B[0]
    for j in range(1, n_gx):
        total = total + SUM_B[j]
    sums = jnp.sum(total, axis=1, keepdims=True)
    cells = float(CX * CY * CZ * n_gx * n_gy * n_gz)
    column = lax.broadcasted_iota(jnp.int32, (1, 2), 1)
    ham_sum = jnp.broadcast_to(sums[0:1], (1, 2))
    mom_sum = jnp.broadcast_to(sums[1:2], (1, 2))
    norm_out[...] = jnp.sqrt(jnp.where(column == 0, ham_sum / cells, mom_sum / (3.0 * cells)))

    sent = geo_ys + geo_zs + rest_ys + rest_zs + edge_xy + edge_yz + edge_xz + ends_x + [others, along]
    for copy in [c for row in geo_xs + terms for c in row] + sent:
        copy.wait_send()


def solution(mesh):
    sizes = (mesh.shape["gx"], mesh.shape["gy"], mesh.shape["gz"])
    n_plane = sizes[1] * sizes[2]
    f32 = jnp.float32

    def step(chi, met, cur, trk, gam):
        vm = lambda *shape: pltpu.VMEM(shape, f32)
        ham, mom, norm = pl.pallas_call(
            functools.partial(kernel, sizes),
            out_shape=(
                pltpu.VMEM((CX, CY, CZ), f32),
                pltpu.VMEM((3, CX, CY, CZ), f32),
                jax.ShapeDtypeStruct((1, 2), f32),
            ),
            in_specs=[pl.BlockSpec(memory_space=pl.ANY)] * 5,
            out_specs=(
                pl.BlockSpec(memory_space=pltpu.VMEM),
                pl.BlockSpec(memory_space=pltpu.VMEM),
                pl.BlockSpec(memory_space=pltpu.VMEM),
            ),
            scratch_shapes=[
                vm(GEO, LX, ROWS, CZ), vm(REST, LX, ROWS, CZ),
                vm(GEO, LX, ROWS, CZ), vm(GEO, CX, CY, CZ), vm(8, CX, CY, CZ),
                vm(GEO, CX, ROWS, CZ), vm(GEO, CX, ROWS, CZ), vm(2, 8, CZ),
                vm(2, 136, CZ), vm(2, 8, 2 * CX, CZ), vm(2, 136, CZ), vm(2, 8, 2 * CX, CZ),
                vm(2, 128, CZ), vm(2, 2, 8, CZ), vm(2, 2, 32, CZ),
                vm(15, 8, CZ), vm(2, 15, 8, CZ), vm(15, 8, CZ), vm(GEO, 8, CZ),
                vm(2, 2, 8, CZ), vm(2, 3, 2, 8, CZ), vm(2, 2, 8, CZ),
                vm(2, 4, 2, CY, CZ), vm(2, 4, 2, CY, CZ),
                vm(2, 2, CZ), vm(n_plane, 2, CZ), vm(sizes[0], 2, CZ),
                pltpu.SemaphoreType.DMA((5,)),
                pltpu.SemaphoreType.DMA((S_COUNT,)),
                pltpu.SemaphoreType.DMA((S_COUNT,)),
                pltpu.SemaphoreType.REGULAR,
                pltpu.SemaphoreType.REGULAR,
            ],
            compiler_params=pltpu.CompilerParams(collective_id=0, has_side_effects=True),
        )(chi, met, cur, trk, gam)
        return ham, mom, norm.reshape(2)

    return jax.shard_map(
        step,
        mesh=mesh,
        in_specs=(
            P("gx", "gy", "gz"),
            P(None, "gx", "gy", "gz"),
            P(None, "gx", "gy", "gz"),
            P("gx", "gy", "gz"),
            P(None, "gx", "gy", "gz"),
        ),
        out_specs=(P("gx", "gy", "gz"), P(None, "gx", "gy", "gz"), P()),
        check_vma=False,
    )
```

```python
import functools

import jax
import jax.numpy as jnp
from jax import lax
from jax.experimental import pallas as pl
from jax.experimental.pallas import tpu as pltpu
from jax.sharding import PartitionSpec as P

MESH = pl.DeviceIdType.MESH
PAIR = ((0, 1, 2), (1, 3, 4), (2, 4, 5))

CX, CY, CZ = 8, 32, 128
LX, ROWS, OWN = CX + 4, 48, 8
BLOCKS = CY // 8
PAIRS = CX // 2
GEO, REST = 7, 10
Y_REST = (0, 1, 2, 3, 4, 5, 6, 8)
Z_REST = (0, 1, 2, 3, 4, 5, 6, 9)
X_REST = 8

S_GEO_X, S_EDGE_XY, S_EDGE_YZ, S_EDGE_XZ = 0, 8, 12, 16
S_GEO_Y, S_GEO_Z, S_REST_Y, S_REST_Z, S_TERM, S_ENDS_X = 20, 22, 24, 26, 28, 36
S_SUM_A, S_SUM_B, S_COUNT = 38, 39, 40


def lane_ids():
    return lax.broadcasted_iota(jnp.int32, (8, CZ), 1)


def inverse_of(g):
    g00, g01, g02, g11, g12, g22 = g
    m00 = g11 * g22 - g12 * g12
    m01 = g02 * g12 - g01 * g22
    m02 = g01 * g12 - g02 * g11
    m11 = g00 * g22 - g02 * g02
    m12 = g01 * g02 - g00 * g12
    m22 = g00 * g11 - g01 * g01
    scale = 1.0 / (g00 * m00 + g01 * m01 + g02 * m02)
    return [m00 * scale, m01 * scale, m02 * scale, m11 * scale, m12 * scale, m22 * scale]


def first(lo2, lo1, hi1, hi2):
    return (lo2 - hi2) + 8.0 * (hi1 - lo1)


def second(lo2, lo1, mid, hi1, hi2):
    return 16.0 * (lo1 + hi1) - (lo2 + hi2) - 30.0 * mid


def kernel(
    sizes,
    chi_in, met_in, cur_in, trk_in, gam_in,
    ham_out, mom_out, norm_out,
    F, R, DZ, DZZ, DZR, DX, DXX, ACC,
    YSG, YSR, YRG, YRR, YDZ, YZR, XYR, TAPS,
    ZP, ZPR, C1, C2, XE, XER, CXE,
    CS, CR, MINE, SUM_A, SUM_B,
    load_sem, send_sem, recv_sem, near_sem, far_sem,
):
    n_gx, n_gy, n_gz = sizes
    ix, iy, iz = lax.axis_index("gx"), lax.axis_index("gy"), lax.axis_index("gz")
    xs = {k: lax.rem(ix + k + n_gx, n_gx) for k in range(-2, n_gx)}
    ys = {k: lax.rem(iy + k + n_gy, n_gy) for k in range(-1, n_gy)}
    zs = {k: lax.rem(iz + k + n_gz, n_gz) for k in range(-2, n_gz)}

    def at(dx, dy, dz):
        return xs[dx], ys[dy], zs[dz]

    def remote(src, dst, place, device):
        return pltpu.make_async_remote_copy(
            src_ref=src, dst_ref=dst, send_sem=send_sem.at[place], recv_sem=recv_sem.at[place],
            device_id=device, device_id_type=MESH,
        )

    loads = [
        (chi_in, F.at[0, 2 : 2 + CX, OWN : OWN + CY]),
        (met_in, F.at[1:7, 2 : 2 + CX, OWN : OWN + CY]),
        (cur_in, R.at[0:6, 2 : 2 + CX, OWN : OWN + CY]),
        (trk_in, R.at[6, 2 : 2 + CX, OWN : OWN + CY]),
        (gam_in, R.at[7:10, 2 : 2 + CX, OWN : OWN + CY]),
    ]
    loads = [pltpu.make_async_copy(s, d, load_sem.at[i]) for i, (s, d) in enumerate(loads)]
    for copy in loads:
        copy.start()

    barrier = pltpu.get_barrier_semaphore()
    faces = [(-1, 0, 0), (1, 0, 0), (0, -1, 0), (0, 1, 0), (0, 0, -1), (0, 0, 1)]
    for step in faces:
        pl.semaphore_signal(barrier, inc=1, device_id=at(*step), device_id_type=MESH)

    lane = lane_ids()
    lane4, place = lane // 4, lax.rem(lane, 4)
    ends = (lane < 2) | (lane >= CZ - 2)
    zero = jnp.zeros((8, CZ), jnp.float32)

    def clear(c, _):
        for layer in (0, 1, LX - 2, LX - 1):
            for b in range(BLOCKS):
                R[c, layer, pl.ds(OWN + 8 * b, 8), :] = zero
        return 0

    lax.fori_loop(0, X_REST, clear, 0)
    ACC[...] = jnp.zeros_like(ACC)

    def packed(tiles):
        out = zero
        for t, tile in enumerate(tiles):
            turn = (4 * t + 2) % CZ
            out = jnp.where(lane4 == t, pltpu.roll(tile, turn, 1) if turn else tile, out)
        return out

    def own_tiles(ref, c):
        return [ref[c, 2 + x, pl.ds(OWN + 8 * b, 8), :] for x in range(CX) for b in range(BLOCKS)]

    def pack_y_geo(p, _):
        for c in range(GEO):
            for xi in range(2):
                rows = pl.ds(32 * p + c * 4 + xi * 2, 2)
                YSG[0, rows, :] = F[c, 2 + 2 * p + xi, OWN : OWN + 2, :]
                YSG[1, rows, :] = F[c, 2 + 2 * p + xi, OWN + CY - 2 : OWN + CY, :]
        return 0

    def pack_y_rest(x, _):
        rows = pl.ds(2 * x, 2)
        for n, c in enumerate(Y_REST):
            YSR[0, n, rows, :] = R[c, 2 + x, OWN : OWN + 2, :]
            YSR[1, n, rows, :] = R[c, 2 + x, OWN + CY - 2 : OWN + CY, :]
        return 0

    def geo_x(d, b):
        rows = pl.ds(OWN + 8 * b, 8)
        src = F.at[0:GEO, pl.ds(CX if d else 2, 2), rows]
        dst = F.at[0:GEO, pl.ds(0 if d else CX + 2, 2), rows]
        return remote(src, dst, S_GEO_X + 4 * d + b, at(2 * d - 1, 0, 0))

    geo_xs = [[geo_x(d, b) for b in range(BLOCKS)] for d in range(2)]
    ends_x = [remote(XE.at[d], XER.at[1 - d, 0], S_ENDS_X + d, at(2 * d - 1, 0, 0)) for d in range(2)]
    geo_ys = [remote(YSG.at[d], YRG.at[1 - d], S_GEO_Y + d, at(0, 2 * d - 1, 0)) for d in range(2)]
    geo_zs = [remote(ZP.at[0:GEO], ZPR.at[1 - d, 0:GEO], S_GEO_Z + d, at(0, 0, 2 * d - 1)) for d in range(2)]
    rest_ys = [remote(YSR.at[d], YRR.at[1 - d], S_REST_Y + d, at(0, 2 * d - 1, 0)) for d in range(2)]
    rest_zs = [
        remote(ZP.at[GEO : GEO + 8], ZPR.at[1 - d, GEO : GEO + 8], S_REST_Z + d, at(0, 0, 2 * d - 1)) for d in range(2)
    ]
    combos = [(a, b) for a in range(2) for b in range(2)]
    edge_xy = [
        remote(
            YSG.at[dy, pl.ds(96 if dx else 0, 32)], XYR.at[1 - dx, 1 - dy], S_EDGE_XY + 2 * dx + dy,
            at(2 * dx - 1, 2 * dy - 1, 0),
        )
        for dx, dy in combos
    ]
    edge_yz = [
        remote(
            YSG.at[dy, 128:136], YZR.at[1 - dz, 1 - dy], S_EDGE_YZ + 2 * dy + dz, at(0, 2 * dy - 1, 2 * dz - 1)
        )
        for dy, dz in combos
    ]
    edge_xz = [
        remote(XE.at[dx], XER.at[1 - dx, 2 - dz], S_EDGE_XZ + 2 * dx + dz, at(2 * dx - 1, 0, 2 * dz - 1))
        for dx, dz in combos
    ]

    column = lax.broadcasted_iota(jnp.int32, (CZ, 2 * CZ), 1)
    step = lax.rem(lax.broadcasted_iota(jnp.int32, (CZ, 2 * CZ), 0) - column + 2 * CZ, CZ)

    def weights(table):
        out = jnp.zeros((CZ, 2 * CZ), jnp.float32)
        for k, w in table:
            out = jnp.where(step == k % CZ, w, out)
        return out

    taps = jnp.where(
        column < CZ,
        weights(((-2, 1.0), (-1, -8.0), (1, 8.0), (2, -1.0))),
        weights(((-2, -1.0), (-1, 16.0), (0, -30.0), (1, 16.0), (2, -1.0))),
    ).astype(jnp.bfloat16)
    for k in range(3):
        TAPS[CZ * k : CZ * k + CZ, :] = taps
    for s in range(2):
        for p in range(PAIRS):
            YSG[s, 32 * p + 24 : 32 * p + 32, :] = zero

    def along_z(cells, width):
        high = cells.astype(jnp.bfloat16)
        rest = cells - high.astype(jnp.float32)
        middle = rest.astype(jnp.bfloat16)
        low = (rest - middle.astype(jnp.float32)).astype(jnp.bfloat16)
        pieces = jnp.concatenate([high, middle, low], axis=1)
        return jnp.dot(pieces, TAPS[:, 0:width], preferred_element_type=jnp.float32)

    loads[0].wait()
    loads[1].wait()
    pl.semaphore_wait(barrier, len(faces))
    for b in range(BLOCKS):
        for d in range(2):
            geo_xs[d][b].start()
    for c in range(GEO):
        ZP[c] = packed(own_tiles(F, c))
    for copy in geo_zs:
        copy.start()
    lax.fori_loop(0, PAIRS, pack_y_geo, 0)
    for s in range(2):
        YSG[s, 128:136, :] = packed([YSG[s, 8 * k : 8 * k + 8, :] for k in range(16)])
        for v in range(2):
            out = zero
            for c in range(4 * v, min(4 * v + 4, GEO)):
                turn = (32 * (c % 4) - 96 * s) % CZ
                out = jnp.where(lane // 32 == c % 4, pltpu.roll(ZP[c], turn, 1) if turn else ZP[c], out)
            XE[s, v] = out
    for copy in geo_ys + ends_x:
        copy.start()
    for copy in loads[2:]:
        copy.wait()
    lax.fori_loop(0, CX, pack_y_rest, 0)
    for n, c in enumerate(Z_REST):
        ZP[GEO + n] = packed(own_tiles(R, c))
    for copy in rest_zs + rest_ys:
        copy.start()

    own_rows = (slice(2, 2 + CX), slice(OWN, OWN + CY))

    def z_geo(c):
        out = along_z(F[c, own_rows[0], own_rows[1], :].reshape(CX * CY, CZ), 2 * CZ)
        DZ[c, own_rows[0], own_rows[1], :] = out[:, 0:CZ].reshape(CX, CY, CZ)
        DZZ[c] = out[:, CZ:].reshape(CX, CY, CZ)

    def z_rest(n):
        c = n + (n // 7) * 2
        DZR[n] = along_z(R[c, own_rows[0], own_rows[1], :].reshape(CX * CY, CZ), CZ).reshape(CX, CY, CZ)

    def x_rows(layers, tiles):
        def body(k, _):
            x = layers(k)
            for b in tiles:
                rows = slice(8 * b, 8 * b + 8)
                for c in range(GEO):
                    taps = [F[c, x + k, rows, :] for k in range(5)]
                    DX[c, x, rows, :] = first(taps[0], taps[1], taps[3], taps[4])
                    DXX[c, x, rows, :] = second(*taps)
            return 0

        lax.fori_loop(0, 4, body, 0)

    for c in range(GEO):
        z_geo(c)
    for n in range(8):
        z_rest(n)
    x_rows(lambda k: k + 2, (1, 2, 3, 4))
    for copy in geo_zs:
        copy.wait_recv()
    for copy in edge_yz + edge_xz:
        copy.start()
    for copy in geo_ys:
        copy.wait_recv()
    for copy in edge_xy:
        copy.start()

    def change(own, left, right):
        e = jnp.where(place < 2, left, right) - own
        hi2, hi1, lo1, lo2 = (pltpu.roll(e, k, 1) for k in (CZ - 2, CZ - 1, 1, 2))
        hi1 = jnp.where(place == 1, hi1, 0.0)
        lo1 = jnp.where(place == 2, lo1, 0.0)
        return (
            jnp.where(place < 2, 8.0 * hi1 - hi2, lo2 - 8.0 * lo1),
            16.0 * (hi1 + lo1) - jnp.where(place < 2, hi2, lo2),
        )

    def at_ends(change, turn):
        return jnp.where(ends, pltpu.roll(change, turn, 1), 0.0)

    for c in range(GEO):
        C1[c], C2[c] = change(ZP[c], ZPR[0, c], ZPR[1, c])

    def z_ends(half, _):
        for c in range(GEO):
            changed = C1[c]
            for k in range(4):
                x = 4 * half + k
                for b in range(BLOCKS):
                    rows = pl.ds(OWN + 8 * b, 8)
                    DZ[c, x + 2, rows, :] += at_ends(changed, CZ - 2 - 4 * (BLOCKS * x + b))
        return 0

    lax.fori_loop(0, 2, z_ends, 0)
    for copy in rest_zs + rest_ys:
        copy.wait_recv()
    for n in range(8):
        C1[GEO + n] = change(ZP[GEO + n], ZPR[0, GEO + n], ZPR[1, GEO + n])[0]

    def open_y_rest(x, _):
        rows = pl.ds(2 * x, 2)
        for n, c in enumerate(Y_REST):
            R[c, 2 + x, OWN - 2 : OWN, :] = YRR[0, n, rows, :]
            R[c, 2 + x, OWN + CY : OWN + CY + 2, :] = YRR[1, n, rows, :]
        return 0

    lax.fori_loop(0, CX, open_y_rest, 0)
    def open_y_geo(p, _):
        for c in range(GEO):
            for xi in range(2):
                rows = pl.ds(32 * p + c * 4 + xi * 2, 2)
                F[c, 2 + 2 * p + xi, OWN - 2 : OWN, :] = YRG[0, rows, :]
                F[c, 2 + 2 * p + xi, OWN + CY : OWN + CY + 2, :] = YRG[1, rows, :]
        return 0

    def y_ends(s):
        changed = change(YRG[s, 128:136, :], YZR[0, s], YZR[1, s])[0]
        out = along_z(YRG[s, 0:128, :], CZ)
        for k in range(16):
            rows = slice(8 * k, 8 * k + 8)
            YDZ[s, rows, :] = out[rows] + at_ends(changed, CZ - 2 - 4 * k)

    def open_y_dz(p, _):
        for c in range(GEO):
            for xi in range(2):
                rows = pl.ds(32 * p + c * 4 + xi * 2, 2)
                DZ[c, 2 + 2 * p + xi, OWN - 2 : OWN, :] = YDZ[0, rows, :]
                DZ[c, 2 + 2 * p + xi, OWN + CY : OWN + CY + 2, :] = YDZ[1, rows, :]
        return 0

    def cell(x, b):
        r0 = OWN + 8 * b
        mid = pl.ds(pl.multiple_of(r0, 8), 8)
        own = pl.ds(pl.multiple_of(8 * b, 8), 8)
        turn = CZ - 2 - 4 * (BLOCKS * x + b)

        def y_of(ref, c, layer):
            return [ref[c, layer, pl.ds(r0 + k, 8), :] for k in (-2, -1, 1, 2)]

        def x_of(ref, c):
            return [ref[c, x + 2 + k, mid, :] for k in (-2, -1, 1, 2)]

        g = [F[1 + n, x + 2, mid, :] for n in range(6)]
        chi = F[0, x + 2, mid, :]
        gu = inverse_of(g)
        wide = [gu[0], 2.0 * gu[1], 2.0 * gu[2], gu[3], 2.0 * gu[4], gu[5]]
        same = [12.0 * gu[0], 12.0 * gu[3], 12.0 * gu[5]]

        grads, bend = [[], [], []], []
        for c in range(GEO):
            f = F[c, x + 2, mid, :]
            ys = y_of(F, c, x + 2)
            grads[0].append(DX[c, x, mid, :])
            grads[1].append(first(*ys))
            grads[2].append(DZ[c, x + 2, mid, :])
            bend.append(
                same[0] * DXX[c, x, mid, :]
                + same[1] * second(ys[0], ys[1], f, ys[2], ys[3])
                + same[2] * (DZZ[c, x, own, :] + at_ends(C2[c], turn))
                + wide[1] * first(*y_of(DX, c, x))
                + wide[2] * first(*x_of(DZ, c))
                + wide[4] * first(*y_of(DZ, c, x + 2))
            )
        dchi = [grads[a][0] for a in range(3)]
        bend_g = sum(wide[n] * bend[1 + n] for n in range(1, 6)) + wide[0] * bend[1]

        def d(a, i, j):
            return grads[a][1 + PAIR[i][j]]

        def inv(i, j):
            return gu[PAIR[i][j]]

        trace, low = [], []
        for a in range(3):
            t = wide[0] * grads[a][1]
            for n in range(1, 6):
                t = t + wide[n] * grads[a][1 + n]
            trace.append(t)
            e = gu[0] * d(0, 0, a) + gu[3] * d(1, 1, a) + gu[5] * d(2, 2, a)
            e = e + gu[1] * (d(0, 1, a) + d(1, 0, a)) + gu[2] * (d(0, 2, a) + d(2, 0, a))
            e = e + gu[4] * (d(1, 2, a) + d(2, 1, a))
            low.append(e - 0.5 * t)
        gd = [inv(k, 0) * low[0] + inv(k, 1) * low[1] + inv(k, 2) * low[2] for k in range(3)]

        cyc = {
            (0, 0, 0): 3.0 * d(0, 0, 0), (1, 1, 1): 3.0 * d(1, 1, 1), (2, 2, 2): 3.0 * d(2, 2, 2),
            (0, 0, 1): 2.0 * d(0, 0, 1) + d(1, 0, 0), (0, 0, 2): 2.0 * d(0, 0, 2) + d(2, 0, 0),
            (0, 1, 1): 2.0 * d(1, 0, 1) + d(0, 1, 1), (1, 1, 2): 2.0 * d(1, 1, 2) + d(2, 1, 1),
            (0, 2, 2): 2.0 * d(2, 0, 2) + d(0, 2, 2), (1, 2, 2): 2.0 * d(2, 1, 2) + d(1, 2, 2),
            (0, 1, 2): d(0, 1, 2) + d(1, 0, 2) + d(2, 0, 1),
        }

        def s(*idx):
            return cyc[tuple(sorted(idx))]

        up = [[[None] * 3 for _ in range(3)] for _ in range(3)]
        for i in range(3):
            for l in range(3):
                for j in range(l, 3):
                    value = inv(i, 0) * s(0, l, j) + inv(i, 1) * s(1, l, j) + inv(i, 2) * s(2, l, j)
                    up[l][i][j] = value
                    up[j][i][l] = value
        squares = None
        for l in range(3):
            for m in range(l, 3):
                if l == m:
                    diag = up[l][0][0] * up[l][0][0] + up[l][1][1] * up[l][1][1] + up[l][2][2] * up[l][2][2]
                    off = up[l][0][1] * up[l][1][0] + up[l][0][2] * up[l][2][0] + up[l][1][2] * up[l][2][1]
                    trc = diag + 2.0 * off
                else:
                    trc = sum(up[l][i][j] * up[m][j][i] for i in range(3) for j in range(3) if i + j) + (
                        up[l][0][0] * up[m][0][0]
                    )
                term = wide[PAIR[l][m]] * trc
                squares = term if squares is None else squares + term

        def z_of(n):
            return DZR[n, x, own, :] + at_ends(C1[GEO + n], turn)

        rest_grad = [[], [], []]
        for n in range(7):
            rest_grad[0].append(first(*x_of(R, n)))
            rest_grad[1].append(first(*y_of(R, n, x + 2)))
            rest_grad[2].append(z_of(n))
        div = first(*x_of(R, 7)) + first(*y_of(R, 8, x + 2)) + z_of(7)
        A = [R[n, x + 2, mid, :] for n in range(6)]
        K = R[6, x + 2, mid, :]

        mixed = [
            [A[PAIR[i][0]] * inv(0, j) + A[PAIR[i][1]] * inv(1, j) + A[PAIR[i][2]] * inv(2, j) for j in range(3)]
            for i in range(3)
        ]
        raised = [
            inv(i, 0) * mixed[0][j] + inv(i, 1) * mixed[1][j] + inv(i, 2) * mixed[2][j]
            for i, j in ((0, 0), (0, 1), (0, 2), (1, 1), (1, 2), (2, 2))
        ]
        a_sq = mixed[0][0] * mixed[0][0] + mixed[1][1] * mixed[1][1] + mixed[2][2] * mixed[2][2]
        a_sq = a_sq + 2.0 * (
            mixed[0][1] * mixed[1][0] + mixed[0][2] * mixed[2][0] + mixed[1][2] * mixed[2][1]
        )
        chi_inv = 1.0 / chi
        dchi_up = [inv(k, 0) * dchi[0] + inv(k, 1) * dchi[1] + inv(k, 2) * dchi[2] for k in range(3)]
        grad_sq = dchi_up[0] * dchi[0] + dchi_up[1] * dchi[1] + dchi_up[2] * dchi[2]
        gd_trace = gd[0] * trace[0] + gd[1] * trace[1] + gd[2] * trace[2]
        gd_chi = gd[0] * dchi[0] + gd[1] * dchi[1] + gd[2] * dchi[2]
        ricci = 0.5 * (gd_trace - bend_g) + squares * (1.0 / 12.0) + 12.0 * div
        ham = (chi * ricci + 2.0 * (bend[0] - gd_chi) - 2.5 * grad_sq * chi_inv) * (1.0 / 144.0)
        ham_out[x, own, :] = ham + (2.0 / 3.0) * (K * K) - a_sq

        weight = 1.5 * chi_inv
        vec = [gd[l] + weight * dchi_up[l] for l in range(3)]
        twice = [0.5 * raised[0], raised[1], raised[2], 0.5 * raised[3], raised[4], 0.5 * raised[5]]
        for i in range(3):
            total = (-2.0 / 3.0) * rest_grad[i][6]
            for j in range(3):
                for k in range(3):
                    total = total + inv(j, k) * rest_grad[j][PAIR[k][i]]
            for l in range(3):
                total = total - vec[l] * A[PAIR[l][i]]
            for n in range(6):
                total = total - twice[n] * grads[i][1 + n]
            mom_out[i, x, own, :] = total * (1.0 / 12.0)

    def tally(x, b):
        own = pl.ds(pl.multiple_of(8 * b, 8), 8)
        ham = ham_out[x, own, :]
        m0, m1, m2 = [mom_out[n, x, own, :] for n in range(3)]
        ACC[0] += ham * ham
        ACC[1] += m0 * m0 + m1 * m1 + m2 * m2

    def term(d, b):
        rows = pl.ds(8 * b, 8)
        return remote(CS.at[d, :, :, rows], CR.at[1 - d, :, :, rows], S_TERM + 4 * d + b, at(2 * d - 1, 0, 0))

    terms = [[term(d, b) for b in range(BLOCKS)] for d in range(2)]

    def send_terms(b):
        mid = pl.ds(OWN + 8 * b, 8)
        for d in range(2):
            geo_xs[d][b].wait_recv()
        for d in range(2):
            halo = CX + 2 if d else 0
            for k in range(2):
                gu = inverse_of([F[1 + n, halo + k, mid, :] for n in range(6)])
                chi = F[0, halo + k, mid, :]

                def part(n):
                    if d == 0:
                        f0 = R[n, 2, mid, :]
                        return -f0 if k == 0 else 8.0 * f0 - R[n, 3, mid, :]
                    f7 = R[n, CX + 1, mid, :]
                    return R[n, CX, mid, :] - 8.0 * f7 if k == 0 else f7

                a = [part(n) for n in range(8)]
                own = pl.ds(8 * b, 8)
                CS[d, 0, k, own, :] = chi * a[7] * (1.0 / 12.0)
                for i in range(3):
                    value = gu[0] * a[PAIR[0][i]] + gu[1] * a[PAIR[1][i]] + gu[2] * a[PAIR[2][i]]
                    if i == 0:
                        value = value - (2.0 / 3.0) * a[6]
                    CS[d, 1 + i, k, own, :] = value * (1.0 / 12.0)
        for d in range(2):
            terms[d][b].start()

    def inner(lo, hi):
        def body(i, _):
            k = lax.rem(i, 8)
            x, odd, last = 2 + k // 2, lax.rem(k, 2), i // 8
            b = (1 - last) * (1 + odd) + last * 3 * odd
            cell(x, b)
            tally(x, b)
            return 0

        lax.fori_loop(lo, hi, body, 0)

    send_terms(0)
    for step in [(-2, 0, 0), (2, 0, 0), (0, 0, -2), (0, 0, 2)]:
        pl.semaphore_signal(near_sem, inc=1, device_id=at(*step), device_id_type=MESH)
    inner(0, 4)
    send_terms(1)
    inner(4, 8)
    send_terms(2)
    lax.fori_loop(0, PAIRS, open_y_geo, 0)
    x_rows(lambda k: k + 2, (0, 5))
    for copy in edge_yz:
        copy.wait_recv()
    for s in range(2):
        y_ends(s)
    lax.fori_loop(0, PAIRS, open_y_dz, 0)
    send_terms(3)
    inner(8, 16)
    pl.semaphore_wait(near_sem, 4)
    for k in range(1, n_gy):
        pl.semaphore_signal(far_sem, inc=1, device_id=at(0, k, 0), device_id_type=MESH)

    for copy in edge_xy + edge_xz + ends_x:
        copy.wait_recv()
    for sx in range(2):
        for sy in range(2):
            for c in range(GEO):
                for k in range(2):
                    layer = (CX + 2 if sx else 0) + k
                    row = OWN + CY if sy else OWN - 2
                    F[c, layer, row : row + 2, :] = XYR[sx, sy, c * 4 + k * 2 : c * 4 + k * 2 + 2, :]
        for v in range(2):
            CXE[sx, v] = change(XER[sx, 0, v], XER[sx, 1, v], XER[sx, 2, v])[0]

    def x_ends(c):
        for side in range(2):
            layers = slice(CX + 2, CX + 4) if side else slice(0, 2)
            out = along_z(F[c, layers, own_rows[1], :].reshape(2 * CY, CZ), CZ)
            changed = CXE[side, c // 4]
            for xi in range(2):
                for b in range(BLOCKS):
                    turn = CZ - 2 - 32 * (c % 4) - 4 * (BLOCKS * xi + b)
                    row = CY * xi + 8 * b
                    DZ[c, layers.start + xi, pl.ds(OWN + 8 * b, 8), :] = out[row : row + 8] + at_ends(changed, turn)

    for c in range(GEO):
        x_ends(c)
    x_rows(lambda k: k + (k // 2) * (CX - 4), (0, 1, 2, 3, 4, 5))

    def edge_cell(i, _):
        k = i // BLOCKS
        cell(k + (k // 2) * (CX - 4), lax.rem(i, BLOCKS))
        return 0

    lax.fori_loop(0, 4 * BLOCKS, edge_cell, 0)

    for d in range(2):
        for b in range(BLOCKS):
            terms[d][b].wait_recv()

    def finish(k, _):
        side, sub = k // 2, lax.rem(k, 2)
        x = k + side * (CX - 4)
        ham_out[x] = ham_out[x] + CR[side, 0, sub]
        for n in range(3):
            mom_out[n, x] = mom_out[n, x] + CR[side, 1 + n, sub]
        for b in range(BLOCKS):
            tally(x, b)
        return 0

    lax.fori_loop(0, 4, finish, 0)
    MINE[0, 0:1, :] = jnp.sum(ACC[0], axis=0, keepdims=True)
    MINE[0, 1:2, :] = jnp.sum(ACC[1], axis=0, keepdims=True)
    rank_a = iy * n_gz + iz
    n_plane = n_gy * n_gz
    SUM_A[rank_a] = MINE[0]
    pl.semaphore_wait(far_sem, n_gy - 1)
    for dy in range(n_gy):
        for dz in range(n_gz):
            if dy or dz:
                remote(MINE.at[0], SUM_A.at[rank_a], S_SUM_A, at(0, dy, dz)).start()
    others = remote(SUM_A.at[pl.ds(0, n_plane - 1)], SUM_A.at[pl.ds(0, n_plane - 1)], S_SUM_A, at(0, 1, 0))
    others.wait_recv()
    total = SUM_A[0]
    for k in range(1, n_plane):
        total = total + SUM_A[k]
    MINE[1] = total
    SUM_B[ix] = total
    for dx in range(1, n_gx):
        remote(MINE.at[1], SUM_B.at[ix], S_SUM_B, at(dx, 0, 0)).start()
    along = remote(SUM_B.at[pl.ds(0, n_gx - 1)], SUM_B.at[pl.ds(0, n_gx - 1)], S_SUM_B, at(1, 0, 0))
    along.wait_recv()
    total = SUM_B[0]
    for j in range(1, n_gx):
        total = total + SUM_B[j]
    sums = jnp.sum(total, axis=1, keepdims=True)
    cells = float(CX * CY * CZ * n_gx * n_gy * n_gz)
    column = lax.broadcasted_iota(jnp.int32, (1, 2), 1)
    ham_sum = jnp.broadcast_to(sums[0:1], (1, 2))
    mom_sum = jnp.broadcast_to(sums[1:2], (1, 2))
    norm_out[...] = jnp.sqrt(jnp.where(column == 0, ham_sum / cells, mom_sum / (3.0 * cells)))

    sent = geo_ys + geo_zs + rest_ys + rest_zs + edge_xy + edge_yz + edge_xz + ends_x + [others, along]
    for copy in [c for row in geo_xs + terms for c in row] + sent:
        copy.wait_send()


def write_out(ham, mom, norm, ham_out, mom_out, norm_out, sems):
    copies = [
        pltpu.make_async_copy(src, dst, sems.at[i])
        for i, (src, dst) in enumerate(((ham, ham_out), (mom, mom_out), (norm, norm_out)))
    ]
    for copy in copies:
        copy.start()
    for copy in copies:
        copy.wait()


def solution(mesh):
    sizes = (mesh.shape["gx"], mesh.shape["gy"], mesh.shape["gz"])
    n_plane = sizes[1] * sizes[2]
    f32 = jnp.float32

    def step(chi, met, cur, trk, gam):
        vm = lambda *shape: pltpu.VMEM(shape, f32)
        ham, mom, norm = pl.pallas_call(
            functools.partial(kernel, sizes),
            out_shape=(
                pltpu.VMEM((CX, CY, CZ), f32),
                pltpu.VMEM((3, CX, CY, CZ), f32),
                pltpu.VMEM((1, 2), f32),
            ),
            in_specs=[pl.BlockSpec(memory_space=pl.ANY)] * 5,
            out_specs=(
                pl.BlockSpec(memory_space=pltpu.VMEM),
                pl.BlockSpec(memory_space=pltpu.VMEM),
                pl.BlockSpec(memory_space=pltpu.VMEM),
            ),
            scratch_shapes=[
                vm(GEO, LX, ROWS, CZ), vm(REST, LX, ROWS, CZ),
                vm(GEO, LX, ROWS, CZ), vm(GEO, CX, CY, CZ), vm(8, CX, CY, CZ),
                vm(GEO, CX, ROWS, CZ), vm(GEO, CX, ROWS, CZ), vm(2, 8, CZ),
                vm(2, 136, CZ), vm(2, 8, 2 * CX, CZ), vm(2, 136, CZ), vm(2, 8, 2 * CX, CZ),
                vm(2, 128, CZ), vm(2, 2, 8, CZ), vm(2, 2, 32, CZ),
                pltpu.VMEM((3 * CZ, 2 * CZ), jnp.bfloat16),
                vm(15, 8, CZ), vm(2, 15, 8, CZ), vm(15, 8, CZ), vm(GEO, 8, CZ),
                vm(2, 2, 8, CZ), vm(2, 3, 2, 8, CZ), vm(2, 2, 8, CZ),
                vm(2, 4, 2, CY, CZ), vm(2, 4, 2, CY, CZ),
                vm(2, 2, CZ), vm(n_plane, 2, CZ), vm(sizes[0], 2, CZ),
                pltpu.SemaphoreType.DMA((5,)),
                pltpu.SemaphoreType.DMA((S_COUNT,)),
                pltpu.SemaphoreType.DMA((S_COUNT,)),
                pltpu.SemaphoreType.REGULAR,
                pltpu.SemaphoreType.REGULAR,
            ],
            compiler_params=pltpu.CompilerParams(collective_id=0, has_side_effects=True),
        )(chi, met, cur, trk, gam)
        ham, mom, norm = pl.pallas_call(
            write_out,
            out_shape=(
                jax.ShapeDtypeStruct((CX, CY, CZ), f32),
                jax.ShapeDtypeStruct((3, CX, CY, CZ), f32),
                jax.ShapeDtypeStruct((1, 2), f32),
            ),
            in_specs=[pl.BlockSpec(memory_space=pl.ANY)] * 3,
            out_specs=[pl.BlockSpec(memory_space=pl.ANY)] * 3,
            scratch_shapes=[pltpu.SemaphoreType.DMA((3,))],
        )(*[pltpu.with_memory_space_constraint(x, pltpu.VMEM) for x in (ham, mom, norm)])
        return ham, mom, norm.reshape(2)

    return jax.shard_map(
        step,
        mesh=mesh,
        in_specs=(
            P("gx", "gy", "gz"),
            P(None, "gx", "gy", "gz"),
            P(None, "gx", "gy", "gz"),
            P("gx", "gy", "gz"),
            P(None, "gx", "gy", "gz"),
        ),
        out_specs=(P("gx", "gy", "gz"), P(None, "gx", "gy", "gz"), P()),
        check_vma=False,
    )
```

```python
import functools

import jax
import jax.numpy as jnp
from jax import lax
from jax.experimental import pallas as pl
from jax.experimental.pallas import tpu as pltpu
from jax.sharding import PartitionSpec as P

MESH = pl.DeviceIdType.MESH
PAIR = ((0, 1, 2), (1, 3, 4), (2, 4, 5))

CX, CY, CZ = 8, 32, 128
LX, ROWS, OWN = CX + 4, 48, 8
BLOCKS = CY // 8
PAIRS = CX // 2
GEO, REST = 7, 10
Y_REST = (0, 1, 2, 3, 4, 5, 6, 8)
Z_REST = (0, 1, 2, 3, 4, 5, 6, 9)
X_REST = 8

S_GEO_X, S_EDGE_XY, S_EDGE_YZ, S_EDGE_XZ = 0, 8, 12, 16
S_GEO_Y, S_GEO_Z, S_REST_Y, S_REST_Z, S_TERM, S_ENDS_X = 20, 22, 24, 26, 28, 36
S_SUM_A, S_SUM_B, S_COUNT = 38, 39, 40


def lane_ids():
    return lax.broadcasted_iota(jnp.int32, (8, CZ), 1)


def inverse_of(g):
    g00, g01, g02, g11, g12, g22 = g
    m00 = g11 * g22 - g12 * g12
    m01 = g02 * g12 - g01 * g22
    m02 = g01 * g12 - g02 * g11
    m11 = g00 * g22 - g02 * g02
    m12 = g01 * g02 - g00 * g12
    m22 = g00 * g11 - g01 * g01
    scale = 1.0 / (g00 * m00 + g01 * m01 + g02 * m02)
    return [m00 * scale, m01 * scale, m02 * scale, m11 * scale, m12 * scale, m22 * scale]


def first(lo2, lo1, hi1, hi2):
    return (lo2 - hi2) + 8.0 * (hi1 - lo1)


def second(lo2, lo1, mid, hi1, hi2):
    return 16.0 * (lo1 + hi1) - (lo2 + hi2) - 30.0 * mid


def kernel(
    sizes,
    chi_in, met_in, cur_in, trk_in, gam_in,
    ham_out, mom_out, norm_out,
    F, R, DZ, DZZ, DZR, DX, DXX, ACC,
    YSG, YSR, YRG, YRR, YDZ, YZR, XYR, TAPS,
    ZP, ZPR, C1, C2, XE, XER, CXE,
    CS, CR, PT, MINE, SUM_A, SUM_B,
    load_sem, send_sem, recv_sem, two_sem, near_sem, far_sem,
):
    n_gx, n_gy, n_gz = sizes
    ix, iy, iz = lax.axis_index("gx"), lax.axis_index("gy"), lax.axis_index("gz")
    xs = {k: lax.rem(ix + k + n_gx, n_gx) for k in range(-2, n_gx)}
    ys = {k: lax.rem(iy + k + n_gy, n_gy) for k in range(-1, n_gy)}
    zs = {k: lax.rem(iz + k + n_gz, n_gz) for k in range(-2, n_gz)}

    def at(dx, dy, dz):
        return xs[dx], ys[dy], zs[dz]

    def remote(src, dst, place, device):
        return pltpu.make_async_remote_copy(
            src_ref=src, dst_ref=dst, send_sem=send_sem.at[place], recv_sem=recv_sem.at[place],
            device_id=device, device_id_type=MESH,
        )

    loads = [
        (chi_in, F.at[0, 2 : 2 + CX, OWN : OWN + CY]),
        (met_in.at[0:3], F.at[1:4, 2 : 2 + CX, OWN : OWN + CY]),
        (met_in.at[3:6], F.at[4:7, 2 : 2 + CX, OWN : OWN + CY]),
        (cur_in, R.at[0:6, 2 : 2 + CX, OWN : OWN + CY]),
        (trk_in, R.at[6, 2 : 2 + CX, OWN : OWN + CY]),
        (gam_in, R.at[7:10, 2 : 2 + CX, OWN : OWN + CY]),
    ]
    loads = [pltpu.make_async_copy(s, d, load_sem.at[i]) for i, (s, d) in enumerate(loads)]
    for copy in loads:
        copy.start()

    barrier = pltpu.get_barrier_semaphore()
    faces = [(-1, 0, 0), (1, 0, 0), (0, -1, 0), (0, 1, 0), (0, 0, -1), (0, 0, 1)]
    for step in faces:
        pl.semaphore_signal(barrier, inc=1, device_id=at(*step), device_id_type=MESH)

    lane = lane_ids()
    lane4, place = lane // 4, lax.rem(lane, 4)
    ends = (lane < 2) | (lane >= CZ - 2)
    zero = jnp.zeros((8, CZ), jnp.float32)

    def clear(c, _):
        for layer in (0, 1, LX - 2, LX - 1):
            for b in range(BLOCKS):
                R[c, layer, pl.ds(OWN + 8 * b, 8), :] = zero
        return 0

    lax.fori_loop(0, X_REST, clear, 0)
    ACC[...] = jnp.zeros_like(ACC)

    def packed(tiles):
        out = zero
        for t, tile in enumerate(tiles):
            turn = (4 * t + 2) % CZ
            out = jnp.where(lane4 == t, pltpu.roll(tile, turn, 1) if turn else tile, out)
        return out

    def own_tiles(ref, c):
        return [ref[c, 2 + x, pl.ds(OWN + 8 * b, 8), :] for x in range(CX) for b in range(BLOCKS)]

    def pack_y_geo(p, _):
        for c in range(GEO):
            for xi in range(2):
                rows = pl.ds(32 * p + c * 4 + xi * 2, 2)
                YSG[0, rows, :] = F[c, 2 + 2 * p + xi, OWN : OWN + 2, :]
                YSG[1, rows, :] = F[c, 2 + 2 * p + xi, OWN + CY - 2 : OWN + CY, :]
        return 0

    def pack_y_rest(x, _):
        rows = pl.ds(2 * x, 2)
        for n, c in enumerate(Y_REST):
            YSR[0, n, rows, :] = R[c, 2 + x, OWN : OWN + 2, :]
            YSR[1, n, rows, :] = R[c, 2 + x, OWN + CY - 2 : OWN + CY, :]
        return 0

    def geo_x(d, b):
        rows = pl.ds(OWN + 8 * b, 8)
        src = F.at[0:GEO, pl.ds(CX if d else 2, 2), rows]
        dst = F.at[0:GEO, pl.ds(0 if d else CX + 2, 2), rows]
        return remote(src, dst, S_GEO_X + 4 * d + b, at(2 * d - 1, 0, 0))

    geo_xs = [[geo_x(d, b) for b in range(BLOCKS)] for d in range(2)]
    ends_x = [remote(XE.at[d], XER.at[1 - d, 0], S_ENDS_X + d, at(2 * d - 1, 0, 0)) for d in range(2)]
    geo_ys = [remote(YSG.at[d], YRG.at[1 - d], S_GEO_Y + d, at(0, 2 * d - 1, 0)) for d in range(2)]
    geo_zs = [remote(ZP.at[0:GEO], ZPR.at[1 - d, 0:GEO], S_GEO_Z + d, at(0, 0, 2 * d - 1)) for d in range(2)]
    rest_ys = [remote(YSR.at[d], YRR.at[1 - d], S_REST_Y + d, at(0, 2 * d - 1, 0)) for d in range(2)]
    rest_zs = [
        remote(ZP.at[GEO : GEO + 8], ZPR.at[1 - d, GEO : GEO + 8], S_REST_Z + d, at(0, 0, 2 * d - 1)) for d in range(2)
    ]
    combos = [(a, b) for a in range(2) for b in range(2)]
    edge_xy = [
        remote(
            YSG.at[dy, pl.ds(96 if dx else 0, 32)], XYR.at[1 - dx, 1 - dy], S_EDGE_XY + 2 * dx + dy,
            at(2 * dx - 1, 2 * dy - 1, 0),
        )
        for dx, dy in combos
    ]
    edge_yz = [
        remote(
            YSG.at[dy, 128:136], YZR.at[1 - dz, 1 - dy], S_EDGE_YZ + 2 * dy + dz, at(0, 2 * dy - 1, 2 * dz - 1)
        )
        for dy, dz in combos
    ]
    edge_xz = [
        remote(XE.at[dx], XER.at[1 - dx, 2 - dz], S_EDGE_XZ + 2 * dx + dz, at(2 * dx - 1, 0, 2 * dz - 1))
        for dx, dz in combos
    ]

    column = lax.broadcasted_iota(jnp.int32, (CZ, 2 * CZ), 1)
    step = lax.rem(lax.broadcasted_iota(jnp.int32, (CZ, 2 * CZ), 0) - column + 2 * CZ, CZ)

    def weights(table):
        out = jnp.zeros((CZ, 2 * CZ), jnp.float32)
        for k, w in table:
            out = jnp.where(step == k % CZ, w, out)
        return out

    taps = jnp.where(
        column < CZ,
        weights(((-2, 1.0), (-1, -8.0), (1, 8.0), (2, -1.0))),
        weights(((-2, -1.0), (-1, 16.0), (0, -30.0), (1, 16.0), (2, -1.0))),
    ).astype(jnp.bfloat16)
    for k in range(3):
        TAPS[CZ * k : CZ * k + CZ, :] = taps
    for s in range(2):
        for p in range(PAIRS):
            YSG[s, 32 * p + 24 : 32 * p + 32, :] = zero

    def along_z(cells, width):
        high = cells.astype(jnp.bfloat16)
        rest = cells - high.astype(jnp.float32)
        middle = rest.astype(jnp.bfloat16)
        low = (rest - middle.astype(jnp.float32)).astype(jnp.bfloat16)
        pieces = jnp.concatenate([high, middle, low], axis=1)
        return jnp.dot(pieces, TAPS[:, 0:width], preferred_element_type=jnp.float32)

    for copy in loads[:3]:
        copy.wait()
    pl.semaphore_wait(barrier, len(faces))
    for step in faces:
        pl.semaphore_signal(two_sem, inc=1, device_id=at(*step), device_id_type=MESH)
    for b in range(BLOCKS - 1):
        for d in range(2):
            geo_xs[d][b].start()
    for c in range(GEO):
        ZP[c] = packed(own_tiles(F, c))
    for copy in geo_zs:
        copy.start()
    lax.fori_loop(0, PAIRS, pack_y_geo, 0)
    for s in range(2):
        YSG[s, 128:136, :] = packed([YSG[s, 8 * k : 8 * k + 8, :] for k in range(16)])
        for v in range(2):
            out = zero
            for c in range(4 * v, min(4 * v + 4, GEO)):
                turn = (32 * (c % 4) - 96 * s) % CZ
                out = jnp.where(lane // 32 == c % 4, pltpu.roll(ZP[c], turn, 1) if turn else ZP[c], out)
            XE[s, v] = out
    for copy in geo_ys + ends_x:
        copy.start()
    for copy in loads[3:]:
        copy.wait()
    for n, c in enumerate(Z_REST):
        ZP[GEO + n] = packed(own_tiles(R, c))
    for copy in rest_zs:
        copy.start()
    lax.fori_loop(0, CX, pack_y_rest, 0)
    for copy in rest_ys:
        copy.start()

    own_rows = (slice(2, 2 + CX), slice(OWN, OWN + CY))

    def z_geo(c):
        out = along_z(F[c, own_rows[0], own_rows[1], :].reshape(CX * CY, CZ), 2 * CZ)
        DZ[c, own_rows[0], own_rows[1], :] = out[:, 0:CZ].reshape(CX, CY, CZ)
        DZZ[c] = out[:, CZ:].reshape(CX, CY, CZ)

    def z_rest(n):
        c = n + (n // 7) * 2
        DZR[n] = along_z(R[c, own_rows[0], own_rows[1], :].reshape(CX * CY, CZ), CZ).reshape(CX, CY, CZ)

    def x_rows(layers, tiles):
        def body(k, _):
            x = layers(k)
            for b in tiles:
                rows = slice(8 * b, 8 * b + 8)
                for c in range(GEO):
                    taps = [F[c, x + k, rows, :] for k in range(5)]
                    DX[c, x, rows, :] = first(taps[0], taps[1], taps[3], taps[4])
                    DXX[c, x, rows, :] = second(*taps)
            return 0

        lax.fori_loop(0, 4, body, 0)

    for c in range(GEO):
        z_geo(c)
    pl.semaphore_wait(two_sem, len(faces))
    for copy in edge_yz + edge_xz + [geo_xs[0][BLOCKS - 1], geo_xs[1][BLOCKS - 1]] + edge_xy:
        copy.start()
    for step in [(-2, 0, 0), (2, 0, 0), (0, 0, -2), (0, 0, 2)]:
        pl.semaphore_signal(near_sem, inc=1, device_id=at(*step), device_id_type=MESH)
    for n in range(8):
        z_rest(n)
    x_rows(lambda k: k + 2, (1, 2, 3, 4))
    def point(i, _):
        x = i // 2
        for n in range(2):
            b = 2 * lax.rem(i, 2) + n
            mid = pl.ds(pl.multiple_of(OWN + 8 * b, 8), 8)
            own = pl.ds(pl.multiple_of(8 * b, 8), 8)
            g00, g01, g02, g11, g12, g22 = [F[1 + k, x + 2, mid, :] for k in range(6)]
            m00 = g11 * g22 - g12 * g12
            m01 = g02 * g12 - g01 * g22
            m02 = g01 * g12 - g02 * g11
            m11 = g00 * g22 - g02 * g02
            m12 = g01 * g02 - g00 * g12
            m22 = g00 * g11 - g01 * g01
            scale = 1.0 / (g00 * m00 + g01 * m01 + g02 * m02)
            gu = [m00 * scale, m01 * scale, m02 * scale, m11 * scale, m12 * scale, m22 * scale]
            d0 = 1.0 / g00
            m_inv = 1.0 / m22
            u01, u12 = -g01 * d0, m12 * m_inv

            def inv(i, j):
                return gu[PAIR[i][j]]

            A = [R[k, x + 2, mid, :] for k in range(6)]
            K = R[6, x + 2, mid, :]
            mixed = [
                [A[PAIR[i][0]] * inv(0, j) + A[PAIR[i][1]] * inv(1, j) + A[PAIR[i][2]] * inv(2, j) for j in range(3)]
                for i in range(3)
            ]
            raised = [
                inv(i, 0) * mixed[0][j] + inv(i, 1) * mixed[1][j] + inv(i, 2) * mixed[2][j]
                for i, j in ((0, 0), (0, 1), (0, 2), (1, 1), (1, 2), (2, 2))
            ]
            a_sq = mixed[0][0] * mixed[0][0] + mixed[1][1] * mixed[1][1] + mixed[2][2] * mixed[2][2]
            a_sq = a_sq + 2.0 * (
                mixed[0][1] * mixed[1][0] + mixed[0][2] * mixed[2][0] + mixed[1][2] * mixed[2][1]
            )
            twice = [0.5 * raised[0], raised[1], raised[2], 0.5 * raised[3], raised[4], 0.5 * raised[5]]
            kept = gu + twice + [(2.0 / 3.0) * (K * K) - a_sq]
            kept += [u01, m02 * m_inv - u12 * u01, u12, d0, g00 * m_inv]
            for k, value in enumerate(kept):
                PT[k, x, own, :] = value
        return 0

    lax.fori_loop(0, 2 * CX, point, 0)
    def term(d, b):
        rows = pl.ds(8 * b, 8)
        return remote(CS.at[d, :, :, rows], CR.at[1 - d, :, :, rows], S_TERM + 4 * d + b, at(2 * d - 1, 0, 0))

    terms = [[term(d, b) for b in range(BLOCKS)] for d in range(2)]

    def send_terms(b):
        mid = pl.ds(OWN + 8 * b, 8)
        for d in range(2):
            geo_xs[d][b].wait_recv()
        for d in range(2):
            halo = CX + 2 if d else 0
            for k in range(2):
                gu = inverse_of([F[1 + n, halo + k, mid, :] for n in range(6)])
                chi = F[0, halo + k, mid, :]

                def part(n):
                    if d == 0:
                        f0 = R[n, 2, mid, :]
                        return -f0 if k == 0 else 8.0 * f0 - R[n, 3, mid, :]
                    f7 = R[n, CX + 1, mid, :]
                    return R[n, CX, mid, :] - 8.0 * f7 if k == 0 else f7

                a = [part(n) for n in range(8)]
                own = pl.ds(8 * b, 8)
                CS[d, 0, k, own, :] = chi * a[7] * (1.0 / 12.0)
                for i in range(3):
                    value = gu[0] * a[PAIR[0][i]] + gu[1] * a[PAIR[1][i]] + gu[2] * a[PAIR[2][i]]
                    if i == 0:
                        value = value - (2.0 / 3.0) * a[6]
                    CS[d, 1 + i, k, own, :] = value * (1.0 / 12.0)
        for d in range(2):
            terms[d][b].start()

    for copy in geo_zs:
        copy.wait_recv()
    send_terms(0)

    def change(own, left, right):
        e = jnp.where(place < 2, left, right) - own
        hi2, hi1, lo1, lo2 = (pltpu.roll(e, k, 1) for k in (CZ - 2, CZ - 1, 1, 2))
        hi1 = jnp.where(place == 1, hi1, 0.0)
        lo1 = jnp.where(place == 2, lo1, 0.0)
        return (
            jnp.where(place < 2, 8.0 * hi1 - hi2, lo2 - 8.0 * lo1),
            16.0 * (hi1 + lo1) - jnp.where(place < 2, hi2, lo2),
        )

    def at_ends(change, turn):
        return jnp.where(ends, pltpu.roll(change, turn, 1), 0.0)

    for c in range(GEO):
        C1[c], C2[c] = change(ZP[c], ZPR[0, c], ZPR[1, c])

    def z_ends(half, _):
        for c in range(GEO):
            changed = C1[c]
            for k in range(4):
                x = 4 * half + k
                for b in range(BLOCKS):
                    rows = pl.ds(OWN + 8 * b, 8)
                    DZ[c, x + 2, rows, :] += at_ends(changed, CZ - 2 - 4 * (BLOCKS * x + b))
        return 0

    lax.fori_loop(0, 2, z_ends, 0)
    for copy in rest_zs:
        copy.wait_recv()
    for n in range(8):
        C1[GEO + n] = change(ZP[GEO + n], ZPR[0, GEO + n], ZPR[1, GEO + n])[0]

    send_terms(1)
    for copy in geo_ys:
        copy.wait_recv()

    def open_y_rest(x, _):
        rows = pl.ds(2 * x, 2)
        for n, c in enumerate(Y_REST):
            R[c, 2 + x, OWN - 2 : OWN, :] = YRR[0, n, rows, :]
            R[c, 2 + x, OWN + CY : OWN + CY + 2, :] = YRR[1, n, rows, :]
        return 0

    def open_y_geo(p, _):
        for c in range(GEO):
            for xi in range(2):
                rows = pl.ds(32 * p + c * 4 + xi * 2, 2)
                F[c, 2 + 2 * p + xi, OWN - 2 : OWN, :] = YRG[0, rows, :]
                F[c, 2 + 2 * p + xi, OWN + CY : OWN + CY + 2, :] = YRG[1, rows, :]
        return 0

    def y_ends(s):
        changed = change(YRG[s, 128:136, :], YZR[0, s], YZR[1, s])[0]
        out = along_z(YRG[s, 0:128, :], CZ)
        for k in range(16):
            rows = slice(8 * k, 8 * k + 8)
            YDZ[s, rows, :] = out[rows] + at_ends(changed, CZ - 2 - 4 * k)

    def open_y_dz(p, _):
        for c in range(GEO):
            for xi in range(2):
                rows = pl.ds(32 * p + c * 4 + xi * 2, 2)
                DZ[c, 2 + 2 * p + xi, OWN - 2 : OWN, :] = YDZ[0, rows, :]
                DZ[c, 2 + 2 * p + xi, OWN + CY : OWN + CY + 2, :] = YDZ[1, rows, :]
        return 0

    def cell(x, b):
        r0 = OWN + 8 * b
        mid = pl.ds(pl.multiple_of(r0, 8), 8)
        own = pl.ds(pl.multiple_of(8 * b, 8), 8)
        turn = CZ - 2 - 4 * (BLOCKS * x + b)

        def y_of(ref, c, layer):
            return [ref[c, layer, pl.ds(r0 + k, 8), :] for k in (-2, -1, 1, 2)]

        def x_of(ref, c):
            return [ref[c, x + 2 + k, mid, :] for k in (-2, -1, 1, 2)]

        chi = F[0, x + 2, mid, :]
        gu = [PT[n, x, own, :] for n in range(6)]
        wide = [gu[0], 2.0 * gu[1], 2.0 * gu[2], gu[3], 2.0 * gu[4], gu[5]]
        same = [12.0 * gu[0], 12.0 * gu[3], 12.0 * gu[5]]

        grads, bend = [[], [], []], []
        for c in range(GEO):
            f = F[c, x + 2, mid, :]
            ys = y_of(F, c, x + 2)
            grads[0].append(DX[c, x, mid, :])
            grads[1].append(first(*ys))
            grads[2].append(DZ[c, x + 2, mid, :])
            bend.append(
                same[0] * DXX[c, x, mid, :]
                + same[1] * second(ys[0], ys[1], f, ys[2], ys[3])
                + same[2] * (DZZ[c, x, own, :] + at_ends(C2[c], turn))
                + wide[1] * first(*y_of(DX, c, x))
                + wide[2] * first(*x_of(DZ, c))
                + wide[4] * first(*y_of(DZ, c, x + 2))
            )
        dchi = [grads[a][0] for a in range(3)]
        bend_g = sum(wide[n] * bend[1 + n] for n in range(1, 6)) + wide[0] * bend[1]

        def d(a, i, j):
            return grads[a][1 + PAIR[i][j]]

        def inv(i, j):
            return gu[PAIR[i][j]]

        def along(values):
            one = values[1] + u01 * values[0]
            return [values[0], one, values[2] + u12 * one + u02 * values[0]]

        u01, u02, u12, d0, d1 = [PT[n, x, own, :] for n in range(13, 18)]
        d2 = gu[5]
        trace = []
        for a in range(3):
            t = wide[0] * grads[a][1]
            for n in range(1, 6):
                t = t + wide[n] * grads[a][1 + n]
            trace.append(t)
        trace = along(trace)
        dchi = along(dchi)

        cyc = {
            (0, 0, 0): 3.0 * d(0, 0, 0), (1, 1, 1): 3.0 * d(1, 1, 1), (2, 2, 2): 3.0 * d(2, 2, 2),
            (0, 0, 1): 2.0 * d(0, 0, 1) + d(1, 0, 0), (0, 0, 2): 2.0 * d(0, 0, 2) + d(2, 0, 0),
            (0, 1, 1): 2.0 * d(1, 0, 1) + d(0, 1, 1), (1, 1, 2): 2.0 * d(1, 1, 2) + d(2, 1, 1),
            (0, 2, 2): 2.0 * d(2, 0, 2) + d(0, 2, 2), (1, 2, 2): 2.0 * d(2, 1, 2) + d(1, 2, 2),
            (0, 1, 2): d(0, 1, 2) + d(1, 0, 2) + d(2, 0, 1),
        }

        s000 = cyc[0, 0, 0]
        s001 = cyc[0, 0, 1] + u01 * s000
        s011 = cyc[0, 1, 1] + u01 * cyc[0, 0, 1]
        s111 = cyc[1, 1, 1] + u01 * cyc[0, 1, 1] + u01 * s011
        s011 = s011 + u01 * s001
        s111 = s111 + u01 * s011
        a00 = cyc[0, 0, 2]
        a01 = cyc[0, 1, 2] + u01 * a00
        a11 = cyc[1, 1, 2] + u01 * cyc[0, 1, 2] + u01 * a01
        b0 = cyc[0, 2, 2]
        b1 = cyc[1, 2, 2] + u01 * b0
        b2 = cyc[2, 2, 2] + u12 * b1 + u02 * b0
        s002 = a00 + u12 * s001 + u02 * s000
        s012 = a01 + u12 * s011 + u02 * s001
        s112 = a11 + u12 * s111 + u02 * s011
        b0 = b0 + u12 * a01 + u02 * a00
        b1 = b1 + u12 * a11 + u02 * a01
        s022 = b0 + u12 * s012 + u02 * s002
        s122 = b1 + u12 * s112 + u02 * s012
        s222 = b2 + u12 * b1 + u02 * b0 + u12 * s122 + u02 * s022
        low = [
            0.5 * (d0 * s000 + d1 * s011 + d2 * s022) - trace[0],
            0.5 * (d0 * s001 + d1 * s111 + d2 * s122) - trace[1],
            0.5 * (d0 * s002 + d1 * s112 + d2 * s222) - trace[2],
        ]
        three1, three2 = 3.0 * d1, 3.0 * d2
        both2 = three2 * d2
        squares = d0 * (
            d0 * (d0 * (s000 * s000) + three1 * (s001 * s001) + three2 * (s002 * s002))
            + three1 * (d1 * (s011 * s011) + (2.0 * d2) * (s012 * s012))
            + both2 * (s022 * s022)
        )
        squares = squares + d1 * (
            d1 * (d1 * (s111 * s111) + three2 * (s112 * s112)) + both2 * (s122 * s122)
        )
        squares = squares + (d2 * d2) * (d2 * (s222 * s222))

        def z_of(n):
            return DZR[n, x, own, :] + at_ends(C1[GEO + n], turn)

        rest_grad = [[], [], []]
        for n in range(7):
            rest_grad[0].append(first(*x_of(R, n)))
            rest_grad[1].append(first(*y_of(R, n, x + 2)))
            rest_grad[2].append(z_of(n))
        div = first(*x_of(R, 7)) + first(*y_of(R, 8, x + 2)) + z_of(7)
        A = [R[n, x + 2, mid, :] for n in range(6)]
        chi_inv = 1.0 / chi
        gd = [d0 * low[0], d1 * low[1], d2 * low[2]]
        dchi_up = [d0 * dchi[0], d1 * dchi[1], d2 * dchi[2]]
        grad_sq = dchi_up[0] * dchi[0] + dchi_up[1] * dchi[1] + dchi_up[2] * dchi[2]
        gd_trace = gd[0] * trace[0] + gd[1] * trace[1] + gd[2] * trace[2]
        gd_chi = gd[0] * dchi[0] + gd[1] * dchi[1] + gd[2] * dchi[2]
        ricci = 0.5 * (gd_trace - bend_g) + squares * (1.0 / 12.0) + 12.0 * div
        ham = (chi * ricci + 2.0 * (bend[0] - gd_chi) - 2.5 * grad_sq * chi_inv) * (1.0 / 144.0)
        ham = ham + PT[12, x, own, :]
        ham_out[x, own, :] = ham

        weight = 1.5 * chi_inv
        vec = [gd[l] + weight * dchi_up[l] for l in range(3)]
        vec[1] = vec[1] + u12 * vec[2]
        vec[0] = vec[0] + u01 * vec[1] + u02 * vec[2]
        twice = [PT[6 + n, x, own, :] for n in range(6)]
        squared = None
        for i in range(3):
            total = (-2.0 / 3.0) * rest_grad[i][6]
            for j in range(3):
                for k in range(3):
                    total = total + inv(j, k) * rest_grad[j][PAIR[k][i]]
            for l in range(3):
                total = total - vec[l] * A[PAIR[l][i]]
            for n in range(6):
                total = total - twice[n] * grads[i][1 + n]
            total = total * (1.0 / 12.0)
            mom_out[i, x, own, :] = total
            squared = total * total if squared is None else squared + total * total
        return ham * ham, squared

    def tally(x, b):
        own = pl.ds(pl.multiple_of(8 * b, 8), 8)
        ham = ham_out[x, own, :]
        m0, m1, m2 = [mom_out[n, x, own, :] for n in range(3)]
        ACC[0] += ham * ham
        ACC[1] += m0 * m0 + m1 * m1 + m2 * m2

    def inner(lo, hi):
        def body(i, _):
            x, last = 2 + lax.rem(i, 4), i // 4
            one, two = [cell(x, (1 - last) * (1 + n) + last * 3 * n) for n in range(2)]
            ACC[0] += one[0] + two[0]
            ACC[1] += one[1] + two[1]
            return 0

        lax.fori_loop(lo, hi, body, 0)

    inner(0, 4)
    send_terms(2)
    lax.fori_loop(0, PAIRS, open_y_geo, 0)
    x_rows(lambda k: k + 2, (0, 5))
    for copy in edge_yz:
        copy.wait_recv()
    for s in range(2):
        y_ends(s)
    lax.fori_loop(0, PAIRS, open_y_dz, 0)
    for copy in rest_ys:
        copy.wait_recv()
    lax.fori_loop(0, CX, open_y_rest, 0)
    inner(4, 8)
    send_terms(3)
    pl.semaphore_wait(near_sem, 4)
    for k in range(1, n_gy):
        pl.semaphore_signal(far_sem, inc=1, device_id=at(0, k, 0), device_id_type=MESH)

    for copy in edge_xz + ends_x:
        copy.wait_recv()
    for sx in range(2):
        for v in range(2):
            CXE[sx, v] = change(XER[sx, 0, v], XER[sx, 1, v], XER[sx, 2, v])[0]

    def x_ends(c):
        for side in range(2):
            layers = slice(CX + 2, CX + 4) if side else slice(0, 2)
            out = along_z(F[c, layers, own_rows[1], :].reshape(2 * CY, CZ), CZ)
            changed = CXE[side, c // 4]
            for xi in range(2):
                for b in range(BLOCKS):
                    turn = CZ - 2 - 32 * (c % 4) - 4 * (BLOCKS * xi + b)
                    row = CY * xi + 8 * b
                    DZ[c, layers.start + xi, pl.ds(OWN + 8 * b, 8), :] = out[row : row + 8] + at_ends(changed, turn)

    for c in range(GEO):
        x_ends(c)
    x_rows(lambda k: k + (k // 2) * (CX - 4), (1, 2, 3, 4))

    def outer(lo, hi):
        def body(i, _):
            k, last = lax.rem(i, 4), i // 4
            for n in range(2):
                cell(k + (k // 2) * (CX - 4), (1 - last) * (1 + n) + last * 3 * n)
            return 0

        lax.fori_loop(lo, hi, body, 0)

    outer(0, 4)
    for copy in edge_xy:
        copy.wait_recv()
    for sx in range(2):
        for sy in range(2):
            for c in range(GEO):
                for k in range(2):
                    layer = (CX + 2 if sx else 0) + k
                    row = OWN + CY if sy else OWN - 2
                    F[c, layer, row : row + 2, :] = XYR[sx, sy, c * 4 + k * 2 : c * 4 + k * 2 + 2, :]
    x_rows(lambda k: k + (k // 2) * (CX - 4), (0, 5))
    outer(4, 8)
    for d in range(2):
        for b in range(BLOCKS):
            terms[d][b].wait_recv()

    def finish(k, _):
        side, sub = k // 2, lax.rem(k, 2)
        x = k + side * (CX - 4)
        ham_out[x] = ham_out[x] + CR[side, 0, sub]
        for n in range(3):
            mom_out[n, x] = mom_out[n, x] + CR[side, 1 + n, sub]
        for b in range(BLOCKS):
            tally(x, b)
        return 0

    lax.fori_loop(0, 4, finish, 0)
    MINE[0, 0:1, :] = jnp.sum(ACC[0], axis=0, keepdims=True)
    MINE[0, 1:2, :] = jnp.sum(ACC[1], axis=0, keepdims=True)
    rank_a = iy * n_gz + iz
    n_plane = n_gy * n_gz
    SUM_A[rank_a] = MINE[0]
    pl.semaphore_wait(far_sem, n_gy - 1)
    for dy in range(n_gy):
        for dz in range(n_gz):
            if dy or dz:
                remote(MINE.at[0], SUM_A.at[rank_a], S_SUM_A, at(0, dy, dz)).start()
    others = remote(SUM_A.at[pl.ds(0, n_plane - 1)], SUM_A.at[pl.ds(0, n_plane - 1)], S_SUM_A, at(0, 1, 0))
    others.wait_recv()
    total = SUM_A[0]
    for k in range(1, n_plane):
        total = total + SUM_A[k]
    MINE[1] = total
    SUM_B[ix] = total
    for dx in range(1, n_gx):
        remote(MINE.at[1], SUM_B.at[ix], S_SUM_B, at(dx, 0, 0)).start()
    along = remote(SUM_B.at[pl.ds(0, n_gx - 1)], SUM_B.at[pl.ds(0, n_gx - 1)], S_SUM_B, at(1, 0, 0))
    along.wait_recv()
    total = SUM_B[0]
    for j in range(1, n_gx):
        total = total + SUM_B[j]
    sums = jnp.sum(total, axis=1, keepdims=True)
    cells = float(CX * CY * CZ * n_gx * n_gy * n_gz)
    column = lax.broadcasted_iota(jnp.int32, (1, 2), 1)
    ham_sum = jnp.broadcast_to(sums[0:1], (1, 2))
    mom_sum = jnp.broadcast_to(sums[1:2], (1, 2))
    norm_out[...] = jnp.sqrt(jnp.where(column == 0, ham_sum / cells, mom_sum / (3.0 * cells)))

    sent = geo_ys + geo_zs + rest_ys + rest_zs + edge_xy + edge_yz + edge_xz + ends_x + [others, along]
    for copy in [c for row in geo_xs + terms for c in row] + sent:
        copy.wait_send()


def write_out(ham, mom, norm, ham_out, mom_out, norm_out, sems):
    copies = [
        pltpu.make_async_copy(src, dst, sems.at[i])
        for i, (src, dst) in enumerate(((ham, ham_out), (mom, mom_out), (norm, norm_out)))
    ]
    for copy in copies:
        copy.start()
    for copy in copies:
        copy.wait()


def solution(mesh):
    sizes = (mesh.shape["gx"], mesh.shape["gy"], mesh.shape["gz"])
    n_plane = sizes[1] * sizes[2]
    f32 = jnp.float32

    def step(chi, met, cur, trk, gam):
        vm = lambda *shape: pltpu.VMEM(shape, f32)
        ham, mom, norm = pl.pallas_call(
            functools.partial(kernel, sizes),
            out_shape=(
                pltpu.VMEM((CX, CY, CZ), f32),
                pltpu.VMEM((3, CX, CY, CZ), f32),
                pltpu.VMEM((1, 2), f32),
            ),
            in_specs=[pl.BlockSpec(memory_space=pl.ANY)] * 5,
            out_specs=(
                pl.BlockSpec(memory_space=pltpu.VMEM),
                pl.BlockSpec(memory_space=pltpu.VMEM),
                pl.BlockSpec(memory_space=pltpu.VMEM),
            ),
            scratch_shapes=[
                vm(GEO, LX, ROWS, CZ), vm(REST, LX, ROWS, CZ),
                vm(GEO, LX, ROWS, CZ), vm(GEO, CX, CY, CZ), vm(8, CX, CY, CZ),
                vm(GEO, CX, ROWS, CZ), vm(GEO, CX, ROWS, CZ), vm(2, 8, CZ),
                vm(2, 136, CZ), vm(2, 8, 2 * CX, CZ), vm(2, 136, CZ), vm(2, 8, 2 * CX, CZ),
                vm(2, 128, CZ), vm(2, 2, 8, CZ), vm(2, 2, 32, CZ),
                pltpu.VMEM((3 * CZ, 2 * CZ), jnp.bfloat16),
                vm(15, 8, CZ), vm(2, 15, 8, CZ), vm(15, 8, CZ), vm(GEO, 8, CZ),
                vm(2, 2, 8, CZ), vm(2, 3, 2, 8, CZ), vm(2, 2, 8, CZ),
                vm(2, 4, 2, CY, CZ), vm(2, 4, 2, CY, CZ), vm(18, CX, CY, CZ),
                vm(2, 2, CZ), vm(n_plane, 2, CZ), vm(sizes[0], 2, CZ),
                pltpu.SemaphoreType.DMA((6,)),
                pltpu.SemaphoreType.DMA((S_COUNT,)),
                pltpu.SemaphoreType.DMA((S_COUNT,)),
                pltpu.SemaphoreType.REGULAR,
                pltpu.SemaphoreType.REGULAR,
                pltpu.SemaphoreType.REGULAR,
            ],
            compiler_params=pltpu.CompilerParams(collective_id=0, has_side_effects=True),
        )(chi, met, cur, trk, gam)
        ham, mom, norm = pl.pallas_call(
            write_out,
            out_shape=(
                jax.ShapeDtypeStruct((CX, CY, CZ), f32),
                jax.ShapeDtypeStruct((3, CX, CY, CZ), f32),
                jax.ShapeDtypeStruct((1, 2), f32),
            ),
            in_specs=[pl.BlockSpec(memory_space=pl.ANY)] * 3,
            out_specs=[pl.BlockSpec(memory_space=pl.ANY)] * 3,
            scratch_shapes=[pltpu.SemaphoreType.DMA((3,))],
        )(*[pltpu.with_memory_space_constraint(x, pltpu.VMEM) for x in (ham, mom, norm)])
        return ham, mom, norm.reshape(2)

    return jax.shard_map(
        step,
        mesh=mesh,
        in_specs=(
            P("gx", "gy", "gz"),
            P(None, "gx", "gy", "gz"),
            P(None, "gx", "gy", "gz"),
            P("gx", "gy", "gz"),
            P(None, "gx", "gy", "gz"),
        ),
        out_specs=(P("gx", "gy", "gz"), P(None, "gx", "gy", "gz"), P()),
        check_vma=False,
    )
```

```python
import functools

import jax
import jax.numpy as jnp
from jax import lax
from jax.experimental import pallas as pl
from jax.experimental.pallas import tpu as pltpu
from jax.sharding import PartitionSpec as P

MESH = pl.DeviceIdType.MESH
PAIR = ((0, 1, 2), (1, 3, 4), (2, 4, 5))

CX, CY, CZ = 8, 32, 128
LX, ROWS, OWN = CX + 4, 48, 8
BLOCKS = CY // 8
PAIRS = CX // 2
GEO, REST = 7, 10
Y_REST = (0, 1, 2, 3, 4, 5, 6, 8)
Z_REST = (0, 1, 2, 3, 4, 5, 6, 9)
X_REST = 8

S_GEO_X, S_EDGE_XY, S_EDGE_YZ, S_EDGE_XZ = 0, 8, 12, 16
S_GEO_Y, S_GEO_Z, S_REST_Y, S_REST_Z, S_TERM = 20, 22, 24, 26, 28
S_SUM_A, S_SUM_B, S_DIRECT, S_LINE, S_LEAD = 36, 37, 38, 39, 54
LEADS = ((0, 0, 1),)
S_COUNT = S_LEAD + len(LEADS)


def lane_ids():
    return lax.broadcasted_iota(jnp.int32, (8, CZ), 1)


def inverse_of(g):
    g00, g01, g02, g11, g12, g22 = g
    m00 = g11 * g22 - g12 * g12
    m01 = g02 * g12 - g01 * g22
    m02 = g01 * g12 - g02 * g11
    m11 = g00 * g22 - g02 * g02
    m12 = g01 * g02 - g00 * g12
    m22 = g00 * g11 - g01 * g01
    scale = 1.0 / (g00 * m00 + g01 * m01 + g02 * m02)
    return [m00 * scale, m01 * scale, m02 * scale, m11 * scale, m12 * scale, m22 * scale]


def first(lo2, lo1, hi1, hi2):
    return (lo2 - hi2) + 8.0 * (hi1 - lo1)


def second(lo2, lo1, mid, hi1, hi2):
    return 16.0 * (lo1 + hi1) - (lo2 + hi2) - 30.0 * mid


def kernel(
    sizes,
    chi_in, met_in, cur_in, trk_in, gam_in,
    ham_out, mom_out, norm_out,
    F, R, DZ, DZZ, DZR, DX, DXX, ACC,
    YSG, YSR, YRG, YRR, YDZ, YZR, XYR, TAPS,
    ZP, ZPR, C1, C2, XE, XER, CXE,
    CS, CR, PT, MINE, SUM_A, SUM_B, ALL,
    load_sem, send_sem, recv_sem, two_sem, near_sem, far_sem, last_sem,
):
    n_gx, n_gy, n_gz = sizes
    ix, iy, iz = lax.axis_index("gx"), lax.axis_index("gy"), lax.axis_index("gz")
    xs = {k: lax.rem(ix + k + n_gx, n_gx) for k in range(-2, n_gx)}
    ys = {k: lax.rem(iy + k + n_gy, n_gy) for k in range(-1, n_gy)}
    zs = {k: lax.rem(iz + k + n_gz, n_gz) for k in range(-2, n_gz)}

    def at(dx, dy, dz):
        return xs[dx], ys[dy], zs[dz]

    def remote(src, dst, place, device):
        return pltpu.make_async_remote_copy(
            src_ref=src, dst_ref=dst, send_sem=send_sem.at[place], recv_sem=recv_sem.at[place],
            device_id=device, device_id_type=MESH,
        )

    def block(src, dst, lo, hi):
        if len(src.shape) == 3:
            return src.at[lo:hi], dst.at[2 + lo : 2 + hi, OWN : OWN + CY]
        return src.at[:, lo:hi], dst.at[:, 2 + lo : 2 + hi, OWN : OWN + CY]

    layers = ((0, 2), (CX - 2, CX), (2, CX - 2))
    loads = [block(src, dst, lo, hi) for lo, hi in layers for src, dst in ((chi_in, F.at[0]), (met_in, F.at[1:7]))]
    loads += [
        block(src, dst, 0, CX) for src, dst in ((cur_in, R.at[0:6]), (trk_in, R.at[6]), (gam_in, R.at[7:10]))
    ]
    loads = [pltpu.make_async_copy(s, d, load_sem.at[i]) for i, (s, d) in enumerate(loads)]
    for copy in loads:
        copy.start()

    barrier = pltpu.get_barrier_semaphore()
    faces = [(-1, 0, 0), (1, 0, 0), (0, -1, 0), (0, 1, 0), (0, 0, -1), (0, 0, 1)]
    for step in faces:
        pl.semaphore_signal(barrier, inc=1, device_id=at(*step), device_id_type=MESH)

    lane = lane_ids()
    lane4, place = lane // 4, lax.rem(lane, 4)
    ends = (lane < 2) | (lane >= CZ - 2)
    zero = jnp.zeros((8, CZ), jnp.float32)

    def clear(c, _):
        for layer in (0, 1, LX - 2, LX - 1):
            for b in range(BLOCKS):
                R[c, layer, pl.ds(OWN + 8 * b, 8), :] = zero
        return 0

    lax.fori_loop(0, X_REST, clear, 0)
    ACC[...] = jnp.zeros_like(ACC)

    def packed(tiles):
        out = zero
        for t, tile in enumerate(tiles):
            if tile is None:
                continue
            turn = (4 * t + 2) % CZ
            out = jnp.where(lane4 == t, pltpu.roll(tile, turn, 1) if turn else tile, out)
        return out

    def own_tiles(ref, c):
        return [ref[c, 2 + x, pl.ds(OWN + 8 * b, 8), :] for x in range(CX) for b in range(BLOCKS)]

    def pack_y_geo(p, _):
        for c in range(GEO):
            for xi in range(2):
                rows = pl.ds(32 * p + c * 4 + xi * 2, 2)
                YSG[0, rows, :] = F[c, 2 + 2 * p + xi, OWN : OWN + 2, :]
                YSG[1, rows, :] = F[c, 2 + 2 * p + xi, OWN + CY - 2 : OWN + CY, :]
        return 0

    def pack_y_rest(x, _):
        rows = pl.ds(2 * x, 2)
        for n, c in enumerate(Y_REST):
            YSR[0, n, rows, :] = R[c, 2 + x, OWN : OWN + 2, :]
            YSR[1, n, rows, :] = R[c, 2 + x, OWN + CY - 2 : OWN + CY, :]
        return 0

    def geo_x(d, b):
        rows = pl.ds(OWN + 8 * b, 8)
        src = F.at[0:GEO, pl.ds(CX if d else 2, 2), rows]
        dst = F.at[0:GEO, pl.ds(0 if d else CX + 2, 2), rows]
        return remote(src, dst, S_GEO_X + 4 * d + b, at(2 * d - 1, 0, 0))

    geo_xs = [[geo_x(d, b) for b in range(BLOCKS)] for d in range(2)]
    geo_ys = [remote(YSG.at[d], YRG.at[1 - d], S_GEO_Y + d, at(0, 2 * d - 1, 0)) for d in range(2)]
    geo_zs = [remote(ZP.at[0:GEO], ZPR.at[1 - d, 0:GEO], S_GEO_Z + d, at(0, 0, 2 * d - 1)) for d in range(2)]
    rest_ys = [remote(YSR.at[d], YRR.at[1 - d], S_REST_Y + d, at(0, 2 * d - 1, 0)) for d in range(2)]
    rest_zs = [
        remote(ZP.at[GEO : GEO + 8], ZPR.at[1 - d, GEO : GEO + 8], S_REST_Z + d, at(0, 0, 2 * d - 1)) for d in range(2)
    ]
    combos = [(a, b) for a in range(2) for b in range(2)]
    edge_xy = [
        remote(
            YSG.at[dy, pl.ds(96 if dx else 0, 32)], XYR.at[1 - dx, 1 - dy], S_EDGE_XY + 2 * dx + dy,
            at(2 * dx - 1, 2 * dy - 1, 0),
        )
        for dx, dy in combos
    ]
    edge_yz = [
        remote(
            YSG.at[dy, 128:136], YZR.at[1 - dz, 1 - dy], S_EDGE_YZ + 2 * dy + dz, at(0, 2 * dy - 1, 2 * dz - 1)
        )
        for dy, dz in combos
    ]
    edge_xz = [
        remote(XE.at[dx, dz], XER.at[1 - dx, 1 - dz], S_EDGE_XZ + 2 * dx + dz, at(2 * dx - 1, 0, 2 * dz - 1))
        for dx, dz in combos
    ]

    column = lax.broadcasted_iota(jnp.int32, (CZ, 2 * CZ), 1)
    step = lax.rem(lax.broadcasted_iota(jnp.int32, (CZ, 2 * CZ), 0) - column + 2 * CZ, CZ)

    def weights(table):
        out = jnp.zeros((CZ, 2 * CZ), jnp.float32)
        for k, w in table:
            out = jnp.where(step == k % CZ, w, out)
        return out

    taps = jnp.where(
        column < CZ,
        weights(((-2, 1.0), (-1, -8.0), (1, 8.0), (2, -1.0))),
        weights(((-2, -1.0), (-1, 16.0), (0, -30.0), (1, 16.0), (2, -1.0))),
    ).astype(jnp.bfloat16)
    for k in range(3):
        TAPS[CZ * k : CZ * k + CZ, :] = taps
    for s in range(2):
        for p in range(PAIRS):
            YSG[s, 32 * p + 24 : 32 * p + 32, :] = zero

    def along_z(cells, width):
        high = cells.astype(jnp.bfloat16)
        rest = cells - high.astype(jnp.float32)
        middle = rest.astype(jnp.bfloat16)
        low = (rest - middle.astype(jnp.float32)).astype(jnp.bfloat16)
        pieces = jnp.concatenate([high, middle, low], axis=1)
        return jnp.dot(pieces, TAPS[:, 0:width], preferred_element_type=jnp.float32)

    for copy in loads[:4]:
        copy.wait()
    pl.semaphore_wait(barrier, len(faces))
    for step in faces:
        pl.semaphore_signal(two_sem, inc=1, device_id=at(*step), device_id_type=MESH)
    for b in range(BLOCKS - 1):
        for d in range(2):
            geo_xs[d][b].start()
    for copy in loads[4:6]:
        copy.wait()
    for c in range(GEO):
        ZP[c] = packed(own_tiles(F, c))
    for copy in geo_zs:
        copy.start()
    lax.fori_loop(0, PAIRS, pack_y_geo, 0)
    for s in range(2):
        YSG[s, 128:136, :] = packed([YSG[s, 8 * k : 8 * k + 8, :] for k in range(16)])
        parts = []
        for v in range(2):
            out = zero
            for c in range(4 * v, min(4 * v + 4, GEO)):
                turn = (32 * (c % 4) - 96 * s) % CZ
                out = jnp.where(lane // 32 == c % 4, pltpu.roll(ZP[c], turn, 1) if turn else ZP[c], out)
            parts.append(out)
        XE[s, 0] = jnp.where(place < 2, pltpu.roll(parts[0], CZ - 2, 1), parts[1])
        XE[s, 1] = jnp.where(place < 2, parts[0], pltpu.roll(parts[1], 2, 1))
    for copy in geo_ys:
        copy.start()
    for copy in loads[6:]:
        copy.wait()
    for n, c in enumerate(Z_REST):
        ZP[GEO + n] = packed(own_tiles(R, c))
    for copy in rest_zs:
        copy.start()
    lax.fori_loop(0, CX, pack_y_rest, 0)
    for copy in rest_ys:
        copy.start()

    own_rows = (slice(2, 2 + CX), slice(OWN, OWN + CY))

    def z_geo(c):
        out = along_z(F[c, own_rows[0], own_rows[1], :].reshape(CX * CY, CZ), 2 * CZ)
        DZ[c, own_rows[0], own_rows[1], :] = out[:, 0:CZ].reshape(CX, CY, CZ)
        DZZ[c] = out[:, CZ:].reshape(CX, CY, CZ)

    def z_rest(n):
        c = n + (n // 7) * 2
        DZR[n] = along_z(R[c, own_rows[0], own_rows[1], :].reshape(CX * CY, CZ), CZ).reshape(CX, CY, CZ)

    def x_rows(layers, tiles):
        def body(k, _):
            x = layers(k)
            for b in tiles:
                rows = slice(8 * b, 8 * b + 8)
                for c in range(GEO):
                    taps = [F[c, x + k, rows, :] for k in range(5)]
                    DX[c, x, rows, :] = first(taps[0], taps[1], taps[3], taps[4])
                    DXX[c, x, rows, :] = second(*taps)
            return 0

        lax.fori_loop(0, 4, body, 0)

    for c in range(GEO):
        z_geo(c)
    for n in range(8):
        z_rest(n)
    pl.semaphore_wait(two_sem, len(faces))
    for copy in edge_yz + edge_xz + [geo_xs[0][BLOCKS - 1], geo_xs[1][BLOCKS - 1]] + edge_xy:
        copy.start()
    for step in [(-2, 0, 0), (2, 0, 0), (0, 0, -2), (0, 0, 2)]:
        pl.semaphore_signal(near_sem, inc=1, device_id=at(*step), device_id_type=MESH)
    x_rows(lambda k: k + 2, (1, 2, 3, 4))
    def point(i, _):
        x = i // 2
        for n in range(2):
            b = 2 * lax.rem(i, 2) + n
            mid = pl.ds(pl.multiple_of(OWN + 8 * b, 8), 8)
            own = pl.ds(pl.multiple_of(8 * b, 8), 8)
            g00, g01, g02, g11, g12, g22 = [F[1 + k, x + 2, mid, :] for k in range(6)]
            m00 = g11 * g22 - g12 * g12
            m01 = g02 * g12 - g01 * g22
            m02 = g01 * g12 - g02 * g11
            m11 = g00 * g22 - g02 * g02
            m12 = g01 * g02 - g00 * g12
            m22 = g00 * g11 - g01 * g01
            scale = 1.0 / (g00 * m00 + g01 * m01 + g02 * m02)
            gu = [m00 * scale, m01 * scale, m02 * scale, m11 * scale, m12 * scale, m22 * scale]
            d0 = 1.0 / g00
            m_inv = 1.0 / m22
            u01, u12 = -g01 * d0, m12 * m_inv

            def inv(i, j):
                return gu[PAIR[i][j]]

            A = [R[k, x + 2, mid, :] for k in range(6)]
            K = R[6, x + 2, mid, :]
            mixed = [
                [A[PAIR[i][0]] * inv(0, j) + A[PAIR[i][1]] * inv(1, j) + A[PAIR[i][2]] * inv(2, j) for j in range(3)]
                for i in range(3)
            ]
            raised = [
                inv(i, 0) * mixed[0][j] + inv(i, 1) * mixed[1][j] + inv(i, 2) * mixed[2][j]
                for i, j in ((0, 0), (0, 1), (0, 2), (1, 1), (1, 2), (2, 2))
            ]
            a_sq = mixed[0][0] * mixed[0][0] + mixed[1][1] * mixed[1][1] + mixed[2][2] * mixed[2][2]
            a_sq = a_sq + 2.0 * (
                mixed[0][1] * mixed[1][0] + mixed[0][2] * mixed[2][0] + mixed[1][2] * mixed[2][1]
            )
            twice = [0.5 * raised[0], raised[1], raised[2], 0.5 * raised[3], raised[4], 0.5 * raised[5]]
            kept = gu + twice + [(2.0 / 3.0) * (K * K) - a_sq]
            kept += [u01, m02 * m_inv - u12 * u01, u12, d0, g00 * m_inv]
            for k, value in enumerate(kept):
                PT[k, x, own, :] = value
        return 0

    lax.fori_loop(0, 2 * CX, point, 0)
    def term(d, b):
        rows = pl.ds(8 * b, 8)
        return remote(CS.at[d, :, :, rows], CR.at[1 - d, :, :, rows], S_TERM + 4 * d + b, at(2 * d - 1, 0, 0))

    terms = [[term(d, b) for b in range(BLOCKS)] for d in range(2)]

    def send_terms(b):
        mid = pl.ds(OWN + 8 * b, 8)
        for d in range(2):
            geo_xs[d][b].wait_recv()
        for d in range(2):
            halo = CX + 2 if d else 0
            for k in range(2):
                gu = inverse_of([F[1 + n, halo + k, mid, :] for n in range(6)])
                chi = F[0, halo + k, mid, :]

                def part(n):
                    if d == 0:
                        f0 = R[n, 2, mid, :]
                        return -f0 if k == 0 else 8.0 * f0 - R[n, 3, mid, :]
                    f7 = R[n, CX + 1, mid, :]
                    return R[n, CX, mid, :] - 8.0 * f7 if k == 0 else f7

                a = [part(n) for n in range(8)]
                own = pl.ds(8 * b, 8)
                CS[d, 0, k, own, :] = chi * a[7] * (1.0 / 12.0)
                for i in range(3):
                    value = gu[0] * a[PAIR[0][i]] + gu[1] * a[PAIR[1][i]] + gu[2] * a[PAIR[2][i]]
                    if i == 0:
                        value = value - (2.0 / 3.0) * a[6]
                    CS[d, 1 + i, k, own, :] = value * (1.0 / 12.0)
        for d in range(2):
            terms[d][b].start()

    for copy in geo_zs:
        copy.wait_recv()

    def change(own, left, right):
        e = jnp.where(place < 2, left, right) - own
        hi2, hi1, lo1, lo2 = (pltpu.roll(e, k, 1) for k in (CZ - 2, CZ - 1, 1, 2))
        hi1 = jnp.where(place == 1, hi1, 0.0)
        lo1 = jnp.where(place == 2, lo1, 0.0)
        return (
            jnp.where(place < 2, 8.0 * hi1 - hi2, lo2 - 8.0 * lo1),
            16.0 * (hi1 + lo1) - jnp.where(place < 2, hi2, lo2),
        )

    def at_ends(change, turn):
        return jnp.where(ends, pltpu.roll(change, turn, 1), 0.0)

    for c in range(GEO):
        C1[c], C2[c] = change(ZP[c], ZPR[0, c], ZPR[1, c])

    def z_ends(half, _):
        for c in range(GEO):
            changed = C1[c]
            for k in range(4):
                x = 4 * half + k
                for b in range(BLOCKS):
                    rows = pl.ds(OWN + 8 * b, 8)
                    DZ[c, x + 2, rows, :] += at_ends(changed, CZ - 2 - 4 * (BLOCKS * x + b))
        return 0

    lax.fori_loop(0, 2, z_ends, 0)
    for copy in rest_zs:
        copy.wait_recv()
    for n in range(8):
        C1[GEO + n] = change(ZP[GEO + n], ZPR[0, GEO + n], ZPR[1, GEO + n])[0]

    def open_y_rest(x, _):
        rows = pl.ds(2 * x, 2)
        for n, c in enumerate(Y_REST):
            R[c, 2 + x, OWN - 2 : OWN, :] = YRR[0, n, rows, :]
            R[c, 2 + x, OWN + CY : OWN + CY + 2, :] = YRR[1, n, rows, :]
        return 0

    def open_y_geo(p, _):
        for c in range(GEO):
            for xi in range(2):
                rows = pl.ds(32 * p + c * 4 + xi * 2, 2)
                F[c, 2 + 2 * p + xi, OWN - 2 : OWN, :] = YRG[0, rows, :]
                F[c, 2 + 2 * p + xi, OWN + CY : OWN + CY + 2, :] = YRG[1, rows, :]
        return 0

    def y_ends(s):
        changed = change(YRG[s, 128:136, :], YZR[0, s], YZR[1, s])[0]
        out = along_z(YRG[s, 0:128, :], CZ)
        for k in range(16):
            rows = slice(8 * k, 8 * k + 8)
            YDZ[s, rows, :] = out[rows] + at_ends(changed, CZ - 2 - 4 * k)

    def open_y_dz(p, _):
        for c in range(GEO):
            for xi in range(2):
                rows = pl.ds(32 * p + c * 4 + xi * 2, 2)
                DZ[c, 2 + 2 * p + xi, OWN - 2 : OWN, :] = YDZ[0, rows, :]
                DZ[c, 2 + 2 * p + xi, OWN + CY : OWN + CY + 2, :] = YDZ[1, rows, :]
        return 0

    def cell(x, b):
        r0 = OWN + 8 * b
        mid = pl.ds(pl.multiple_of(r0, 8), 8)
        own = pl.ds(pl.multiple_of(8 * b, 8), 8)
        turn = CZ - 2 - 4 * (BLOCKS * x + b)

        def y_of(ref, c, layer):
            return [ref[c, layer, pl.ds(r0 + k, 8), :] for k in (-2, -1, 1, 2)]

        def x_of(ref, c):
            return [ref[c, x + 2 + k, mid, :] for k in (-2, -1, 1, 2)]

        chi = F[0, x + 2, mid, :]
        gu = [PT[n, x, own, :] for n in range(6)]
        wide = [gu[0], 2.0 * gu[1], 2.0 * gu[2], gu[3], 2.0 * gu[4], gu[5]]
        same = [12.0 * gu[0], 12.0 * gu[3], 12.0 * gu[5]]

        grads, bend = [[], [], []], []
        for c in range(GEO):
            f = F[c, x + 2, mid, :]
            ys = y_of(F, c, x + 2)
            grads[0].append(DX[c, x, mid, :])
            grads[1].append(first(*ys))
            grads[2].append(DZ[c, x + 2, mid, :])
            bend.append(
                same[0] * DXX[c, x, mid, :]
                + same[1] * second(ys[0], ys[1], f, ys[2], ys[3])
                + same[2] * (DZZ[c, x, own, :] + at_ends(C2[c], turn))
                + wide[1] * first(*y_of(DX, c, x))
                + wide[2] * first(*x_of(DZ, c))
                + wide[4] * first(*y_of(DZ, c, x + 2))
            )
        dchi = [grads[a][0] for a in range(3)]
        bend_g = sum(wide[n] * bend[1 + n] for n in range(1, 6)) + wide[0] * bend[1]

        def d(a, i, j):
            return grads[a][1 + PAIR[i][j]]

        def inv(i, j):
            return gu[PAIR[i][j]]

        def along(values):
            one = values[1] + u01 * values[0]
            return [values[0], one, values[2] + u12 * one + u02 * values[0]]

        u01, u02, u12, d0, d1 = [PT[n, x, own, :] for n in range(13, 18)]
        d2 = gu[5]
        trace = []
        for a in range(3):
            t = wide[0] * grads[a][1]
            for n in range(1, 6):
                t = t + wide[n] * grads[a][1 + n]
            trace.append(t)
        trace = along(trace)
        dchi = along(dchi)

        cyc = {
            (0, 0, 0): 3.0 * d(0, 0, 0), (1, 1, 1): 3.0 * d(1, 1, 1), (2, 2, 2): 3.0 * d(2, 2, 2),
            (0, 0, 1): 2.0 * d(0, 0, 1) + d(1, 0, 0), (0, 0, 2): 2.0 * d(0, 0, 2) + d(2, 0, 0),
            (0, 1, 1): 2.0 * d(1, 0, 1) + d(0, 1, 1), (1, 1, 2): 2.0 * d(1, 1, 2) + d(2, 1, 1),
            (0, 2, 2): 2.0 * d(2, 0, 2) + d(0, 2, 2), (1, 2, 2): 2.0 * d(2, 1, 2) + d(1, 2, 2),
            (0, 1, 2): d(0, 1, 2) + d(1, 0, 2) + d(2, 0, 1),
        }

        s000 = cyc[0, 0, 0]
        s001 = cyc[0, 0, 1] + u01 * s000
        s011 = cyc[0, 1, 1] + u01 * cyc[0, 0, 1]
        s111 = cyc[1, 1, 1] + u01 * cyc[0, 1, 1] + u01 * s011
        s011 = s011 + u01 * s001
        s111 = s111 + u01 * s011
        a00 = cyc[0, 0, 2]
        a01 = cyc[0, 1, 2] + u01 * a00
        a11 = cyc[1, 1, 2] + u01 * cyc[0, 1, 2] + u01 * a01
        b0 = cyc[0, 2, 2]
        b1 = cyc[1, 2, 2] + u01 * b0
        b2 = cyc[2, 2, 2] + u12 * b1 + u02 * b0
        s002 = a00 + u12 * s001 + u02 * s000
        s012 = a01 + u12 * s011 + u02 * s001
        s112 = a11 + u12 * s111 + u02 * s011
        b0 = b0 + u12 * a01 + u02 * a00
        b1 = b1 + u12 * a11 + u02 * a01
        s022 = b0 + u12 * s012 + u02 * s002
        s122 = b1 + u12 * s112 + u02 * s012
        s222 = b2 + u12 * b1 + u02 * b0 + u12 * s122 + u02 * s022
        low = [
            0.5 * (d0 * s000 + d1 * s011 + d2 * s022) - trace[0],
            0.5 * (d0 * s001 + d1 * s111 + d2 * s122) - trace[1],
            0.5 * (d0 * s002 + d1 * s112 + d2 * s222) - trace[2],
        ]
        three1, three2 = 3.0 * d1, 3.0 * d2
        both2 = three2 * d2
        squares = d0 * (
            d0 * (d0 * (s000 * s000) + three1 * (s001 * s001) + three2 * (s002 * s002))
            + three1 * (d1 * (s011 * s011) + (2.0 * d2) * (s012 * s012))
            + both2 * (s022 * s022)
        )
        squares = squares + d1 * (
            d1 * (d1 * (s111 * s111) + three2 * (s112 * s112)) + both2 * (s122 * s122)
        )
        squares = squares + (d2 * d2) * (d2 * (s222 * s222))

        def z_of(n):
            return DZR[n, x, own, :] + at_ends(C1[GEO + n], turn)

        rest_grad = [[], [], []]
        for n in range(7):
            rest_grad[0].append(first(*x_of(R, n)))
            rest_grad[1].append(first(*y_of(R, n, x + 2)))
            rest_grad[2].append(z_of(n))
        div = first(*x_of(R, 7)) + first(*y_of(R, 8, x + 2)) + z_of(7)
        A = [R[n, x + 2, mid, :] for n in range(6)]
        chi_inv = 1.0 / chi
        gd = [d0 * low[0], d1 * low[1], d2 * low[2]]
        dchi_up = [d0 * dchi[0], d1 * dchi[1], d2 * dchi[2]]
        grad_sq = dchi_up[0] * dchi[0] + dchi_up[1] * dchi[1] + dchi_up[2] * dchi[2]
        gd_trace = gd[0] * trace[0] + gd[1] * trace[1] + gd[2] * trace[2]
        gd_chi = gd[0] * dchi[0] + gd[1] * dchi[1] + gd[2] * dchi[2]
        ricci = 0.5 * (gd_trace - bend_g) + squares * (1.0 / 12.0) + 12.0 * div
        ham = (chi * ricci + 2.0 * (bend[0] - gd_chi) - 2.5 * grad_sq * chi_inv) * (1.0 / 144.0)
        ham = ham + PT[12, x, own, :]
        ham_out[x, own, :] = ham

        weight = 1.5 * chi_inv
        vec = [gd[l] + weight * dchi_up[l] for l in range(3)]
        vec[1] = vec[1] + u12 * vec[2]
        vec[0] = vec[0] + u01 * vec[1] + u02 * vec[2]
        twice = [PT[6 + n, x, own, :] for n in range(6)]
        squared = None
        for i in range(3):
            total = (-2.0 / 3.0) * rest_grad[i][6]
            for j in range(3):
                for k in range(3):
                    total = total + inv(j, k) * rest_grad[j][PAIR[k][i]]
            for l in range(3):
                total = total - vec[l] * A[PAIR[l][i]]
            for n in range(6):
                total = total - twice[n] * grads[i][1 + n]
            total = total * (1.0 / 12.0)
            mom_out[i, x, own, :] = total
            squared = total * total if squared is None else squared + total * total
        return ham * ham, squared

    def tally(x, b):
        own = pl.ds(pl.multiple_of(8 * b, 8), 8)
        ham = ham_out[x, own, :]
        m0, m1, m2 = [mom_out[n, x, own, :] for n in range(3)]
        ACC[0] += ham * ham
        ACC[1] += m0 * m0 + m1 * m1 + m2 * m2

    def inner(lo, hi):
        def body(i, _):
            x, last = 2 + lax.rem(i, 4), i // 4
            one, two = [cell(x, (1 - last) * (1 + n) + last * 3 * n) for n in range(2)]
            ACC[0] += one[0] + two[0]
            ACC[1] += one[1] + two[1]
            return 0

        lax.fori_loop(lo, hi, body, 0)

    inner(0, 4)
    send_terms(0)
    pl.semaphore_wait(near_sem, 4)
    twin = (ix, iy, iz + 1 - 2 * lax.rem(iz, 2))
    for device in [at(0, k, 0) for k in range(1, n_gy)] + [twin]:
        pl.semaphore_signal(far_sem, inc=1, device_id=device, device_id_type=MESH)
    for copy in geo_ys:
        copy.wait_recv()
    lax.fori_loop(0, PAIRS, open_y_geo, 0)
    x_rows(lambda k: k + 2, (0, 5))
    for copy in edge_yz:
        copy.wait_recv()
    for s in range(2):
        y_ends(s)
    lax.fori_loop(0, PAIRS, open_y_dz, 0)
    for copy in rest_ys:
        copy.wait_recv()
    lax.fori_loop(0, CX, open_y_rest, 0)
    send_terms(1)
    inner(4, 8)
    send_terms(2)
    pl.semaphore_wait(far_sem, n_gy)
    for k in range(1, n_gx):
        pl.semaphore_signal(last_sem, inc=1, device_id=at(k, 0, 0), device_id_type=MESH)

    for copy in edge_xz:
        copy.wait_recv()
    def x_changes(half):
        for sx in range(2):
            left, right = XER[sx, 0], XER[sx, 1]
            lefts = left, pltpu.roll(left, CZ - 2, 1)
            rights = pltpu.roll(right, 2, 1), right
            for v in range(2):
                own = packed([
                    F[c, (CX + 2) * sx + xi, OWN + 8 * b : OWN + 8 * b + 8, :] if b // 2 == half else None
                    for c in range(4 * v, min(4 * v + 4, GEO)) for xi in range(2) for b in range(BLOCKS)
                ])
                CXE[sx, v] = change(own, lefts[v], rights[v])[0]

    def x_ends(c, half):
        rows = slice(OWN + half * CY // 2, OWN + half * CY // 2 + CY // 2)
        for side in range(2):
            layers = slice(CX + 2, CX + 4) if side else slice(0, 2)
            out = along_z(F[c, layers, rows, :].reshape(CY, CZ), CZ)
            changed = CXE[side, c // 4]
            for xi in range(2):
                for b in range(2):
                    turn = CZ - 2 - 32 * (c % 4) - 4 * (BLOCKS * xi + 2 * half + b)
                    row = CY // 2 * xi + 8 * b
                    target = slice(rows.start + 8 * b, rows.start + 8 * b + 8)
                    DZ[c, layers.start + xi, target, :] = out[row : row + 8] + at_ends(changed, turn)

    def x_edge_rows(*tiles):
        x_rows(lambda k: k + (k // 2) * (CX - 4), tiles)

    def outer(b):
        def body(i, _):
            for n in range(2):
                cell((CX - 2) * i + n, b)
            return 0

        lax.fori_loop(0, 2, body, 0)

    x_changes(0)
    for c in range(GEO):
        x_ends(c, 0)
    x_edge_rows(1, 2, 3)
    send_terms(3)
    outer(1)
    x_changes(1)
    for c in range(GEO):
        x_ends(c, 1)
    x_edge_rows(4)
    outer(2)
    for copy in edge_xy:
        copy.wait_recv()
    for sx in range(2):
        for sy in range(2):
            for c in range(GEO):
                for k in range(2):
                    layer = (CX + 2 if sx else 0) + k
                    row = OWN + CY if sy else OWN - 2
                    F[c, layer, row : row + 2, :] = XYR[sx, sy, c * 4 + k * 2 : c * 4 + k * 2 + 2, :]
    x_edge_rows(0, 5)
    outer(0)
    outer(3)
    for d in range(2):
        for b in range(BLOCKS):
            terms[d][b].wait_recv()

    def finish(k, _):
        side, sub = k // 2, lax.rem(k, 2)
        x = k + side * (CX - 4)
        ham_out[x] = ham_out[x] + CR[side, 0, sub]
        for n in range(3):
            mom_out[n, x] = mom_out[n, x] + CR[side, 1 + n, sub]
        for b in range(BLOCKS):
            tally(x, b)
        return 0

    lax.fori_loop(0, 4, finish, 0)
    halves = [jnp.sum(ACC[n], axis=0, keepdims=True) for n in range(2)]
    halves = [half + pltpu.roll(half, CZ // 2, 1) for half in halves]
    lower = lax.broadcasted_iota(jnp.int32, (1, CZ), 1) < CZ // 2
    MINE[0] = jnp.where(lower, halves[0], halves[1])
    n_chips = n_gz // 2
    n_plane, n_line = n_gy * n_chips, 2 * n_gx
    core = lax.rem(iz, 2)
    rank_a, rank_b = iy * n_chips + iz // 2, 2 * ix + core
    SUM_A[rank_a] = MINE[0]
    pl.semaphore_wait(last_sem, n_gx - 1)
    def is_at(device, other):
        return (device[0] == other[0]) & (device[1] == other[1]) & (device[2] == other[2])

    def leads(device):
        return functools.reduce(jnp.logical_or, [is_at(device, lead) for lead in LEADS])

    own = rank_b * n_plane + rank_a
    leading = leads((ix, iy, iz))
    ALL[own] = MINE[0]
    direct = []
    for lead in LEADS:
        copy = pltpu.make_async_remote_copy(
            src_ref=MINE.at[0], dst_ref=ALL.at[own], send_sem=send_sem.at[S_LEAD + len(direct)],
            recv_sem=recv_sem.at[S_DIRECT], device_id=lead, device_id_type=MESH,
        )
        direct.append((copy, jnp.logical_not(is_at((ix, iy, iz), lead))))
    for copy, wanted in direct:
        pl.when(wanted)(copy.start)

    far_first = sorted(
        ((dy, k) for dy in range(n_gy) for k in range(n_chips) if dy or k),
        key=lambda p: -min(p[0], n_gy - p[0]) - min(p[1], n_chips - p[1]),
    )
    for dy, k in far_first:
        remote(MINE.at[0], SUM_A.at[rank_a], S_SUM_A, at(0, dy, 2 * k)).start()
    others = remote(SUM_A.at[pl.ds(0, n_plane - 1)], SUM_A.at[pl.ds(0, n_plane - 1)], S_SUM_A, at(0, 1, 0))
    others.wait_recv()
    total = SUM_A[0]
    for k in range(1, n_plane):
        total = total + SUM_A[k]
    MINE[1] = total
    SUM_B[rank_b] = total
    line = []
    for dx in sorted(range(n_gx), key=lambda k: -min(k, n_gx - k)):
        for z in [zs[0], twin[2]] if dx else [twin[2]]:
            copy = pltpu.make_async_remote_copy(
                src_ref=MINE.at[1], dst_ref=SUM_B.at[rank_b], send_sem=send_sem.at[S_LINE + len(line)],
                recv_sem=recv_sem.at[S_SUM_B], device_id=(xs[dx], iy, z), device_id_type=MESH,
            )
            line.append((copy, jnp.logical_not(leads((xs[dx], iy, z)))))
    for copy, wanted in line:
        pl.when(wanted)(copy.start)

    def norms(total):
        cells = float(CX * CY * CZ * n_gx * n_gy * n_gz)
        column = lax.broadcasted_iota(jnp.int32, (1, 2), 1)
        ham_sum = jnp.sum(jnp.where(lower, total, 0.0), axis=1, keepdims=True)
        mom_sum = jnp.sum(jnp.where(lower, 0.0, total), axis=1, keepdims=True)
        ham_sum, mom_sum = jnp.broadcast_to(ham_sum, (1, 2)), jnp.broadcast_to(mom_sum, (1, 2))
        norm_out[...] = jnp.sqrt(jnp.where(column == 0, ham_sum / cells, mom_sum / (3.0 * cells)))

    @pl.when(jnp.logical_not(leading))
    def _():
        whole = SUM_B.at[pl.ds(0, n_line - 1)]
        remote(whole, whole, S_SUM_B, twin).wait_recv()
        total = SUM_B[0]
        for j in range(1, n_line):
            total = total + SUM_B[j]
        norms(total)

    @pl.when(leading)
    def _():
        whole = ALL.at[pl.ds(0, n_line * n_plane - 1)]
        remote(whole, whole, S_DIRECT, twin).wait_recv()

        def group(j):
            rows = ALL[n_plane * j]
            for k in range(1, n_plane):
                rows = rows + ALL[n_plane * j + k]
            return rows

        norms(lax.fori_loop(1, n_line, lambda j, total: total + group(j), group(0)))

    sent = geo_ys + geo_zs + rest_ys + rest_zs + edge_xy + edge_yz + edge_xz + [others]
    for copy in [c for row in geo_xs + terms for c in row] + sent:
        copy.wait_send()
    for copy, wanted in line + direct:
        pl.when(wanted)(copy.wait_send)


def write_out(ham, mom, norm, ham_out, mom_out, norm_out, sems):
    copies = [
        pltpu.make_async_copy(src, dst, sems.at[i])
        for i, (src, dst) in enumerate(((ham, ham_out), (mom, mom_out), (norm, norm_out)))
    ]
    for copy in copies:
        copy.start()
    for copy in copies:
        copy.wait()


def solution(mesh):
    sizes = (mesh.shape["gx"], mesh.shape["gy"], mesh.shape["gz"])
    f32 = jnp.float32

    def step(chi, met, cur, trk, gam):
        vm = lambda *shape: pltpu.VMEM(shape, f32)
        ham, mom, norm = pl.pallas_call(
            functools.partial(kernel, sizes),
            out_shape=(
                pltpu.VMEM((CX, CY, CZ), f32),
                pltpu.VMEM((3, CX, CY, CZ), f32),
                pltpu.VMEM((1, 2), f32),
            ),
            in_specs=[pl.BlockSpec(memory_space=pl.ANY)] * 5,
            out_specs=(
                pl.BlockSpec(memory_space=pltpu.VMEM),
                pl.BlockSpec(memory_space=pltpu.VMEM),
                pl.BlockSpec(memory_space=pltpu.VMEM),
            ),
            scratch_shapes=[
                vm(GEO, LX, ROWS, CZ), vm(REST, LX, ROWS, CZ),
                vm(GEO, LX, ROWS, CZ), vm(GEO, CX, CY, CZ), vm(8, CX, CY, CZ),
                vm(GEO, CX, ROWS, CZ), vm(GEO, CX, ROWS, CZ), vm(2, 8, CZ),
                vm(2, 136, CZ), vm(2, 8, 2 * CX, CZ), vm(2, 136, CZ), vm(2, 8, 2 * CX, CZ),
                vm(2, 128, CZ), vm(2, 2, 8, CZ), vm(2, 2, 32, CZ),
                pltpu.VMEM((3 * CZ, 2 * CZ), jnp.bfloat16),
                vm(15, 8, CZ), vm(2, 15, 8, CZ), vm(15, 8, CZ), vm(GEO, 8, CZ),
                vm(2, 2, 8, CZ), vm(2, 2, 8, CZ), vm(2, 2, 8, CZ),
                vm(2, 4, 2, CY, CZ), vm(2, 4, 2, CY, CZ), vm(18, CX, CY, CZ),
                vm(2, 1, CZ), vm(sizes[1] * sizes[2] // 2, 1, CZ), vm(2 * sizes[0], 1, CZ), vm(sizes[0] * sizes[1] * sizes[2], 1, CZ),
                pltpu.SemaphoreType.DMA((9,)),
                pltpu.SemaphoreType.DMA((S_COUNT,)),
                pltpu.SemaphoreType.DMA((S_COUNT,)),
                pltpu.SemaphoreType.REGULAR,
                pltpu.SemaphoreType.REGULAR,
                pltpu.SemaphoreType.REGULAR,
                pltpu.SemaphoreType.REGULAR,
            ],
            compiler_params=pltpu.CompilerParams(collective_id=0, has_side_effects=True),
        )(chi, met, cur, trk, gam)
        ham, mom, norm = pl.pallas_call(
            write_out,
            out_shape=(
                jax.ShapeDtypeStruct((CX, CY, CZ), f32),
                jax.ShapeDtypeStruct((3, CX, CY, CZ), f32),
                jax.ShapeDtypeStruct((1, 2), f32),
            ),
            in_specs=[pl.BlockSpec(memory_space=pl.ANY)] * 3,
            out_specs=[pl.BlockSpec(memory_space=pl.ANY)] * 3,
            scratch_shapes=[pltpu.SemaphoreType.DMA((3,))],
        )(*[pltpu.with_memory_space_constraint(x, pltpu.VMEM) for x in (ham, mom, norm)])
        return ham, mom, norm.reshape(2)

    return jax.shard_map(
        step,
        mesh=mesh,
        in_specs=(
            P("gx", "gy", "gz"),
            P(None, "gx", "gy", "gz"),
            P(None, "gx", "gy", "gz"),
            P("gx", "gy", "gz"),
            P(None, "gx", "gy", "gz"),
        ),
        out_specs=(P("gx", "gy", "gz"), P(None, "gx", "gy", "gz"), P()),
        check_vma=False,
    )
```

```python
import functools

import jax
import jax.numpy as jnp
from jax import lax
from jax.experimental import pallas as pl
from jax.experimental.pallas import tpu as pltpu
from jax.sharding import PartitionSpec as P

MESH = pl.DeviceIdType.MESH
PAIR = ((0, 1, 2), (1, 3, 4), (2, 4, 5))

CX, CY, CZ = 8, 32, 128
LX, ROWS, OWN = CX + 4, 48, 8
BLOCKS = CY // 8
PAIRS = CX // 2
GEO, REST = 7, 10
Y_REST = (0, 1, 2, 3, 4, 5, 6, 8)
Z_REST = (0, 1, 2, 3, 4, 5, 6, 9)
X_REST = 8

S_GEO_Y, S_GEO_Z, S_REST_Y, S_REST_Z, S_EDGE_XY, S_EDGE_YZ, S_EDGE_XZ, S_TERM = range(8)
S_SUM_A, S_SUM_B, S_DIRECT, S_GEO_X = 8, 9, 10, 11
LEAD = (0, 0, 1)


def lane_ids():
    return lax.broadcasted_iota(jnp.int32, (8, CZ), 1)


def inverse_of(g):
    g00, g01, g02, g11, g12, g22 = g
    m00 = g11 * g22 - g12 * g12
    m01 = g02 * g12 - g01 * g22
    m02 = g01 * g12 - g02 * g11
    m11 = g00 * g22 - g02 * g02
    m12 = g01 * g02 - g00 * g12
    m22 = g00 * g11 - g01 * g01
    scale = 1.0 / (g00 * m00 + g01 * m01 + g02 * m02)
    return [m00 * scale, m01 * scale, m02 * scale, m11 * scale, m12 * scale, m22 * scale]


def first(lo2, lo1, hi1, hi2):
    return (lo2 - hi2) + 8.0 * (hi1 - lo1)


def second(lo2, lo1, mid, hi1, hi2):
    return 16.0 * (lo1 + hi1) - (lo2 + hi2) - 30.0 * mid


def kernel(
    sizes,
    chi_in, met_in, cur_in, trk_in, gam_in,
    ham_out, mom_out, norm_out,
    F, R, DZ, DZZ, DZR, DX, DXX, ACC,
    YSG, YSR, YRG, YRR, YDZ, YZR, XYR, TAPS,
    ZP, ZPR, C1, C2, XE, XER, CXE,
    CS, CR, PT, MINE, SUM_A, SUM_B, ALL,
    load_sem, send_sem, recv_sem, two_sem, near_sem, far_sem, last_sem,
):
    n_gx, n_gy, n_gz = sizes
    ix, iy, iz = lax.axis_index("gx"), lax.axis_index("gy"), lax.axis_index("gz")
    xs = {k: lax.rem(ix + k + n_gx, n_gx) for k in range(-2, n_gx)}
    ys = {k: lax.rem(iy + k + n_gy, n_gy) for k in range(-1, n_gy)}
    zs = {k: lax.rem(iz + k + n_gz, n_gz) for k in range(-2, n_gz)}

    def at(dx, dy, dz):
        return xs[dx], ys[dy], zs[dz]

    def remote(src, dst, place, device, part=0):
        return pltpu.make_async_remote_copy(
            src_ref=src, dst_ref=dst, send_sem=send_sem.at[place], recv_sem=recv_sem.at[place + part],
            device_id=device, device_id_type=MESH,
        )

    def group(whole, place, part=0):
        return remote(whole, whole, place, at(1, 0, 0), part)

    barrier = pltpu.get_barrier_semaphore()
    faces = [(-1, 0, 0), (1, 0, 0), (0, -1, 0), (0, 1, 0), (0, 0, -1), (0, 0, 1)]
    for step in faces:
        pl.semaphore_signal(barrier, inc=1, device_id=at(*step), device_id_type=MESH)

    def block(src, dst, lo, hi):
        if len(src.shape) == 3:
            return src.at[lo:hi], dst.at[2 + lo : 2 + hi, OWN : OWN + CY]
        return src.at[:, lo:hi], dst.at[:, 2 + lo : 2 + hi, OWN : OWN + CY]

    layers = ((0, 2), (CX - 2, CX), (2, CX - 2))
    loads = [block(src, dst, lo, hi) for lo, hi in layers for src, dst in ((chi_in, F.at[0]), (met_in, F.at[1:7]))]
    loads += [
        block(src, dst, 0, CX) for src, dst in ((cur_in, R.at[0:6]), (trk_in, R.at[6]), (gam_in, R.at[7:10]))
    ]
    loads = [pltpu.make_async_copy(s, d, load_sem.at[(i > 3) + (i > 5)]) for i, (s, d) in enumerate(loads)]
    for copy in loads:
        copy.start()

    lane = lane_ids()
    lane4, place = lane // 4, lax.rem(lane, 4)
    ends = (lane < 2) | (lane >= CZ - 2)
    zero = jnp.zeros((8, CZ), jnp.float32)

    def clear(c, _):
        for layer in (0, 1, LX - 2, LX - 1):
            for b in range(BLOCKS):
                R[c, layer, pl.ds(OWN + 8 * b, 8), :] = zero
        return 0

    lax.fori_loop(0, X_REST, clear, 0)
    ACC[...] = jnp.zeros_like(ACC)

    def packed(tiles):
        out = zero
        for t, tile in enumerate(tiles):
            if tile is None:
                continue
            turn = (4 * t + 2) % CZ
            out = jnp.where(lane4 == t, pltpu.roll(tile, turn, 1) if turn else tile, out)
        return out

    def own_tiles(ref, c):
        return [ref[c, 2 + x, pl.ds(OWN + 8 * b, 8), :] for x in range(CX) for b in range(BLOCKS)]

    def pack_y_geo(p, _):
        for c in range(GEO):
            for xi in range(2):
                rows = pl.ds(32 * p + c * 4 + xi * 2, 2)
                YSG[0, rows, :] = F[c, 2 + 2 * p + xi, OWN : OWN + 2, :]
                YSG[1, rows, :] = F[c, 2 + 2 * p + xi, OWN + CY - 2 : OWN + CY, :]
        return 0

    def pack_y_rest(x, _):
        rows = pl.ds(2 * x, 2)
        for n, c in enumerate(Y_REST):
            YSR[0, n, rows, :] = R[c, 2 + x, OWN : OWN + 2, :]
            YSR[1, n, rows, :] = R[c, 2 + x, OWN + CY - 2 : OWN + CY, :]
        return 0

    def geo_x(d, b):
        rows = pl.ds(OWN + 8 * b, 8)
        src = F.at[0:GEO, pl.ds(CX if d else 2, 2), rows]
        dst = F.at[0:GEO, pl.ds(0 if d else CX + 2, 2), rows]
        return remote(src, dst, S_GEO_X, at(2 * d - 1, 0, 0), b)

    geo_xs = [[geo_x(d, b) for b in range(BLOCKS)] for d in range(2)]
    geo_ys = [remote(YSG.at[d], YRG.at[1 - d], S_GEO_Y, at(0, 2 * d - 1, 0)) for d in range(2)]
    geo_zs = [remote(ZP.at[0:GEO], ZPR.at[1 - d, 0:GEO], S_GEO_Z, at(0, 0, 2 * d - 1)) for d in range(2)]
    rest_ys = [remote(YSR.at[d], YRR.at[1 - d], S_REST_Y, at(0, 2 * d - 1, 0)) for d in range(2)]
    rest_zs = [
        remote(ZP.at[GEO : GEO + 8], ZPR.at[1 - d, GEO : GEO + 8], S_REST_Z, at(0, 0, 2 * d - 1)) for d in range(2)
    ]
    combos = [(a, b) for a in range(2) for b in range(2)]
    edge_xy = [
        remote(
            YSG.at[dy, pl.ds(96 if dx else 0, 32)], XYR.at[1 - dx, 1 - dy], S_EDGE_XY,
            at(2 * dx - 1, 2 * dy - 1, 0),
        )
        for dx, dy in combos
    ]
    edge_yz = [
        remote(
            YSG.at[dy, 128:136], YZR.at[1 - dz, 1 - dy], S_EDGE_YZ, at(0, 2 * dy - 1, 2 * dz - 1)
        )
        for dy, dz in combos
    ]
    edge_xz = [
        remote(XE.at[dx, dz], XER.at[1 - dx, 1 - dz], S_EDGE_XZ, at(2 * dx - 1, 0, 2 * dz - 1))
        for dx, dz in combos
    ]

    column = lax.broadcasted_iota(jnp.int32, (CZ, 2 * CZ), 1)
    step = lax.rem(lax.broadcasted_iota(jnp.int32, (CZ, 2 * CZ), 0) - column + 2 * CZ, CZ)

    def weights(table):
        out = jnp.zeros((CZ, 2 * CZ), jnp.float32)
        for k, w in table:
            out = jnp.where(step == k % CZ, w, out)
        return out

    taps = jnp.where(
        column < CZ,
        weights(((-2, 1.0), (-1, -8.0), (1, 8.0), (2, -1.0))),
        weights(((-2, -1.0), (-1, 16.0), (0, -30.0), (1, 16.0), (2, -1.0))),
    ).astype(jnp.bfloat16)
    for k in range(3):
        TAPS[CZ * k : CZ * k + CZ, :] = taps
    for s in range(2):
        for p in range(PAIRS):
            YSG[s, 32 * p + 24 : 32 * p + 32, :] = zero

    def along_z(cells, width):
        high = cells.astype(jnp.bfloat16)
        rest = cells - high.astype(jnp.float32)
        middle = rest.astype(jnp.bfloat16)
        low = (rest - middle.astype(jnp.float32)).astype(jnp.bfloat16)
        pieces = jnp.concatenate([high, middle, low], axis=1)
        return jnp.dot(pieces, TAPS[:, 0:width], preferred_element_type=jnp.float32)

    all_geo_x = group(F.at[:, 2 : 2 + CX // 2, OWN : OWN + CY], S_GEO_X)
    all_geo_y, all_rest_y = group(YRG, S_GEO_Y), group(YRR, S_REST_Y)
    all_geo_z, all_rest_z = group(ZPR.at[:, 0:GEO], S_GEO_Z), group(ZPR.at[:, GEO : GEO + 8], S_REST_Z)
    all_xy, all_yz, all_xz = group(XYR, S_EDGE_XY), group(YZR, S_EDGE_YZ), group(XER, S_EDGE_XZ)
    all_terms = group(CR, S_TERM)

    half = F.at[:, 2 : 2 + CX // 2, OWN : OWN + CY]
    pltpu.make_async_copy(half, half, load_sem.at[0]).wait()
    pl.semaphore_wait(barrier, len(faces))
    for step in faces:
        pl.semaphore_signal(two_sem, inc=1, device_id=at(*step), device_id_type=MESH)
    for b in range(BLOCKS - 1):
        for d in range(2):
            geo_xs[d][b].start()
    pltpu.make_async_copy(half, half, load_sem.at[1]).wait()
    for c in range(GEO):
        ZP[c] = packed(own_tiles(F, c))
    for copy in geo_zs:
        copy.start()
    lax.fori_loop(0, PAIRS, pack_y_geo, 0)
    for s in range(2):
        YSG[s, 128:136, :] = packed([YSG[s, 8 * k : 8 * k + 8, :] for k in range(16)])
        parts = []
        for v in range(2):
            out = zero
            for c in range(4 * v, min(4 * v + 4, GEO)):
                turn = (32 * (c % 4) - 96 * s) % CZ
                out = jnp.where(lane // 32 == c % 4, pltpu.roll(ZP[c], turn, 1) if turn else ZP[c], out)
            parts.append(out)
        XE[s, 0] = jnp.where(place < 2, pltpu.roll(parts[0], CZ - 2, 1), parts[1])
        XE[s, 1] = jnp.where(place < 2, parts[0], pltpu.roll(parts[1], 2, 1))
    for copy in geo_ys:
        copy.start()
    whole = R.at[:, 2 : 2 + CX, OWN : OWN + CY]
    pltpu.make_async_copy(whole, whole, load_sem.at[2]).wait()
    for n, c in enumerate(Z_REST):
        ZP[GEO + n] = packed(own_tiles(R, c))
    for copy in rest_zs:
        copy.start()
    lax.fori_loop(0, CX, pack_y_rest, 0)
    for copy in rest_ys:
        copy.start()

    own_rows = (slice(2, 2 + CX), slice(OWN, OWN + CY))

    def z_geo(c):
        out = along_z(F[c, own_rows[0], own_rows[1], :].reshape(CX * CY, CZ), 2 * CZ)
        DZ[c, own_rows[0], own_rows[1], :] = out[:, 0:CZ].reshape(CX, CY, CZ)
        DZZ[c] = out[:, CZ:].reshape(CX, CY, CZ)

    def z_rest(n):
        c = n + (n // 7) * 2
        DZR[n] = along_z(R[c, own_rows[0], own_rows[1], :].reshape(CX * CY, CZ), CZ).reshape(CX, CY, CZ)

    def x_rows(layers, tiles):
        def body(k, _):
            x = layers(k)
            for b in tiles:
                rows = slice(8 * b, 8 * b + 8)
                for c in range(GEO):
                    taps = [F[c, x + k, rows, :] for k in range(5)]
                    DX[c, x, rows, :] = first(taps[0], taps[1], taps[3], taps[4])
                    DXX[c, x, rows, :] = second(*taps)
            return 0

        lax.fori_loop(0, 4, body, 0)

    for c in range(GEO):
        z_geo(c)
    for n in range(8):
        z_rest(n)
    pl.semaphore_wait(two_sem, len(faces))
    for copy in edge_yz + edge_xz + [geo_xs[0][BLOCKS - 1], geo_xs[1][BLOCKS - 1]] + edge_xy:
        copy.start()
    for step in [(-2, 0, 0), (2, 0, 0), (0, 0, -2), (0, 0, 2)]:
        pl.semaphore_signal(near_sem, inc=1, device_id=at(*step), device_id_type=MESH)
    x_rows(lambda k: k + 2, (1, 2, 3, 4))
    def point(i, _):
        x = i // 2
        for n in range(2):
            b = 2 * lax.rem(i, 2) + n
            mid = pl.ds(pl.multiple_of(OWN + 8 * b, 8), 8)
            own = pl.ds(pl.multiple_of(8 * b, 8), 8)
            g00, g01, g02, g11, g12, g22 = [F[1 + k, x + 2, mid, :] for k in range(6)]
            m00 = g11 * g22 - g12 * g12
            m01 = g02 * g12 - g01 * g22
            m02 = g01 * g12 - g02 * g11
            m11 = g00 * g22 - g02 * g02
            m12 = g01 * g02 - g00 * g12
            m22 = g00 * g11 - g01 * g01
            scale = 1.0 / (g00 * m00 + g01 * m01 + g02 * m02)
            gu = [m00 * scale, m01 * scale, m02 * scale, m11 * scale, m12 * scale, m22 * scale]
            d0 = 1.0 / g00
            m_inv = 1.0 / m22
            u01, u12 = -g01 * d0, m12 * m_inv

            def inv(i, j):
                return gu[PAIR[i][j]]

            A = [R[k, x + 2, mid, :] for k in range(6)]
            K = R[6, x + 2, mid, :]
            mixed = [
                [A[PAIR[i][0]] * inv(0, j) + A[PAIR[i][1]] * inv(1, j) + A[PAIR[i][2]] * inv(2, j) for j in range(3)]
                for i in range(3)
            ]
            raised = [
                inv(i, 0) * mixed[0][j] + inv(i, 1) * mixed[1][j] + inv(i, 2) * mixed[2][j]
                for i, j in ((0, 0), (0, 1), (0, 2), (1, 1), (1, 2), (2, 2))
            ]
            a_sq = mixed[0][0] * mixed[0][0] + mixed[1][1] * mixed[1][1] + mixed[2][2] * mixed[2][2]
            a_sq = a_sq + 2.0 * (
                mixed[0][1] * mixed[1][0] + mixed[0][2] * mixed[2][0] + mixed[1][2] * mixed[2][1]
            )
            twice = [0.5 * raised[0], raised[1], raised[2], 0.5 * raised[3], raised[4], 0.5 * raised[5]]
            kept = gu + twice + [(2.0 / 3.0) * (K * K) - a_sq]
            kept += [u01, m02 * m_inv - u12 * u01, u12, d0, g00 * m_inv]
            for k, value in enumerate(kept):
                PT[k, x, own, :] = value
        return 0

    lax.fori_loop(0, 2 * CX, point, 0)
    def term(d, b):
        rows = pl.ds(8 * b, 8)
        return remote(CS.at[d, :, :, rows], CR.at[1 - d, :, :, rows], S_TERM, at(2 * d - 1, 0, 0))

    terms = [[term(d, b) for b in range(BLOCKS)] for d in range(2)]

    def send_terms(b):
        mid = pl.ds(OWN + 8 * b, 8)
        group(F.at[:, 2 : 2 + CX // 2, OWN : OWN + 8], S_GEO_X, b).wait_recv()
        for d in range(2):
            halo = CX + 2 if d else 0
            for k in range(2):
                gu = inverse_of([F[1 + n, halo + k, mid, :] for n in range(6)])
                chi = F[0, halo + k, mid, :]

                def part(n):
                    if d == 0:
                        f0 = R[n, 2, mid, :]
                        return -f0 if k == 0 else 8.0 * f0 - R[n, 3, mid, :]
                    f7 = R[n, CX + 1, mid, :]
                    return R[n, CX, mid, :] - 8.0 * f7 if k == 0 else f7

                a = [part(n) for n in range(8)]
                own = pl.ds(8 * b, 8)
                CS[d, 0, k, own, :] = chi * a[7] * (1.0 / 12.0)
                for i in range(3):
                    value = gu[0] * a[PAIR[0][i]] + gu[1] * a[PAIR[1][i]] + gu[2] * a[PAIR[2][i]]
                    if i == 0:
                        value = value - (2.0 / 3.0) * a[6]
                    CS[d, 1 + i, k, own, :] = value * (1.0 / 12.0)
        for d in range(2):
            terms[d][b].start()

    all_geo_z.wait_recv()

    def change(own, left, right):
        e = jnp.where(place < 2, left, right) - own
        hi2, hi1, lo1, lo2 = (pltpu.roll(e, k, 1) for k in (CZ - 2, CZ - 1, 1, 2))
        hi1 = jnp.where(place == 1, hi1, 0.0)
        lo1 = jnp.where(place == 2, lo1, 0.0)
        return (
            jnp.where(place < 2, 8.0 * hi1 - hi2, lo2 - 8.0 * lo1),
            16.0 * (hi1 + lo1) - jnp.where(place < 2, hi2, lo2),
        )

    def at_ends(change, turn):
        return jnp.where(ends, pltpu.roll(change, turn, 1), 0.0)

    for c in range(GEO):
        C1[c], C2[c] = change(ZP[c], ZPR[0, c], ZPR[1, c])

    def z_ends(half, _):
        for c in range(GEO):
            changed = C1[c]
            for k in range(4):
                x = 4 * half + k
                for b in range(BLOCKS):
                    rows = pl.ds(OWN + 8 * b, 8)
                    DZ[c, x + 2, rows, :] += at_ends(changed, CZ - 2 - 4 * (BLOCKS * x + b))
        return 0

    lax.fori_loop(0, 2, z_ends, 0)
    all_rest_z.wait_recv()
    for n in range(8):
        C1[GEO + n] = change(ZP[GEO + n], ZPR[0, GEO + n], ZPR[1, GEO + n])[0]

    def open_y_rest(x, _):
        rows = pl.ds(2 * x, 2)
        for n, c in enumerate(Y_REST):
            R[c, 2 + x, OWN - 2 : OWN, :] = YRR[0, n, rows, :]
            R[c, 2 + x, OWN + CY : OWN + CY + 2, :] = YRR[1, n, rows, :]
        return 0

    def open_y_geo(p, _):
        for c in range(GEO):
            for xi in range(2):
                rows = pl.ds(32 * p + c * 4 + xi * 2, 2)
                F[c, 2 + 2 * p + xi, OWN - 2 : OWN, :] = YRG[0, rows, :]
                F[c, 2 + 2 * p + xi, OWN + CY : OWN + CY + 2, :] = YRG[1, rows, :]
        return 0

    def y_ends(s):
        changed = change(YRG[s, 128:136, :], YZR[0, s], YZR[1, s])[0]
        out = along_z(YRG[s, 0:128, :], CZ)
        for k in range(16):
            rows = slice(8 * k, 8 * k + 8)
            YDZ[s, rows, :] = out[rows] + at_ends(changed, CZ - 2 - 4 * k)

    def open_y_dz(p, _):
        for c in range(GEO):
            for xi in range(2):
                rows = pl.ds(32 * p + c * 4 + xi * 2, 2)
                DZ[c, 2 + 2 * p + xi, OWN - 2 : OWN, :] = YDZ[0, rows, :]
                DZ[c, 2 + 2 * p + xi, OWN + CY : OWN + CY + 2, :] = YDZ[1, rows, :]
        return 0

    def cell(x, b):
        r0 = OWN + 8 * b
        mid = pl.ds(pl.multiple_of(r0, 8), 8)
        own = pl.ds(pl.multiple_of(8 * b, 8), 8)
        turn = CZ - 2 - 4 * (BLOCKS * x + b)

        def y_of(ref, c, layer):
            return [ref[c, layer, pl.ds(r0 + k, 8), :] for k in (-2, -1, 1, 2)]

        def x_of(ref, c):
            return [ref[c, x + 2 + k, mid, :] for k in (-2, -1, 1, 2)]

        chi = F[0, x + 2, mid, :]
        gu = [PT[n, x, own, :] for n in range(6)]
        wide = [gu[0], 2.0 * gu[1], 2.0 * gu[2], gu[3], 2.0 * gu[4], gu[5]]
        same = [12.0 * gu[0], 12.0 * gu[3], 12.0 * gu[5]]

        grads, bend = [[], [], []], []
        for c in range(GEO):
            f = F[c, x + 2, mid, :]
            ys = y_of(F, c, x + 2)
            grads[0].append(DX[c, x, mid, :])
            grads[1].append(first(*ys))
            grads[2].append(DZ[c, x + 2, mid, :])
            bend.append(
                same[0] * DXX[c, x, mid, :]
                + same[1] * second(ys[0], ys[1], f, ys[2], ys[3])
                + same[2] * (DZZ[c, x, own, :] + at_ends(C2[c], turn))
                + wide[1] * first(*y_of(DX, c, x))
                + wide[2] * first(*x_of(DZ, c))
                + wide[4] * first(*y_of(DZ, c, x + 2))
            )
        dchi = [grads[a][0] for a in range(3)]
        bend_g = sum(wide[n] * bend[1 + n] for n in range(1, 6)) + wide[0] * bend[1]

        def d(a, i, j):
            return grads[a][1 + PAIR[i][j]]

        def inv(i, j):
            return gu[PAIR[i][j]]

        def along(values):
            one = values[1] + u01 * values[0]
            return [values[0], one, values[2] + u12 * one + u02 * values[0]]

        u01, u02, u12, d0, d1 = [PT[n, x, own, :] for n in range(13, 18)]
        d2 = gu[5]
        trace = []
        for a in range(3):
            t = wide[0] * grads[a][1]
            for n in range(1, 6):
                t = t + wide[n] * grads[a][1 + n]
            trace.append(t)
        trace = along(trace)
        dchi = along(dchi)

        cyc = {
            (0, 0, 0): 3.0 * d(0, 0, 0), (1, 1, 1): 3.0 * d(1, 1, 1), (2, 2, 2): 3.0 * d(2, 2, 2),
            (0, 0, 1): 2.0 * d(0, 0, 1) + d(1, 0, 0), (0, 0, 2): 2.0 * d(0, 0, 2) + d(2, 0, 0),
            (0, 1, 1): 2.0 * d(1, 0, 1) + d(0, 1, 1), (1, 1, 2): 2.0 * d(1, 1, 2) + d(2, 1, 1),
            (0, 2, 2): 2.0 * d(2, 0, 2) + d(0, 2, 2), (1, 2, 2): 2.0 * d(2, 1, 2) + d(1, 2, 2),
            (0, 1, 2): d(0, 1, 2) + d(1, 0, 2) + d(2, 0, 1),
        }

        s000 = cyc[0, 0, 0]
        s001 = cyc[0, 0, 1] + u01 * s000
        s011 = cyc[0, 1, 1] + u01 * cyc[0, 0, 1]
        s111 = cyc[1, 1, 1] + u01 * cyc[0, 1, 1] + u01 * s011
        s011 = s011 + u01 * s001
        s111 = s111 + u01 * s011
        a00 = cyc[0, 0, 2]
        a01 = cyc[0, 1, 2] + u01 * a00
        a11 = cyc[1, 1, 2] + u01 * cyc[0, 1, 2] + u01 * a01
        b0 = cyc[0, 2, 2]
        b1 = cyc[1, 2, 2] + u01 * b0
        b2 = cyc[2, 2, 2] + u12 * b1 + u02 * b0
        s002 = a00 + u12 * s001 + u02 * s000
        s012 = a01 + u12 * s011 + u02 * s001
        s112 = a11 + u12 * s111 + u02 * s011
        b0 = b0 + u12 * a01 + u02 * a00
        b1 = b1 + u12 * a11 + u02 * a01
        s022 = b0 + u12 * s012 + u02 * s002
        s122 = b1 + u12 * s112 + u02 * s012
        s222 = b2 + u12 * b1 + u02 * b0 + u12 * s122 + u02 * s022
        low = [
            0.5 * (d0 * s000 + d1 * s011 + d2 * s022) - trace[0],
            0.5 * (d0 * s001 + d1 * s111 + d2 * s122) - trace[1],
            0.5 * (d0 * s002 + d1 * s112 + d2 * s222) - trace[2],
        ]
        three1, three2 = 3.0 * d1, 3.0 * d2
        both2 = three2 * d2
        squares = d0 * (
            d0 * (d0 * (s000 * s000) + three1 * (s001 * s001) + three2 * (s002 * s002))
            + three1 * (d1 * (s011 * s011) + (2.0 * d2) * (s012 * s012))
            + both2 * (s022 * s022)
        )
        squares = squares + d1 * (
            d1 * (d1 * (s111 * s111) + three2 * (s112 * s112)) + both2 * (s122 * s122)
        )
        squares = squares + (d2 * d2) * (d2 * (s222 * s222))

        def z_of(n):
            return DZR[n, x, own, :] + at_ends(C1[GEO + n], turn)

        rest_grad = [[], [], []]
        for n in range(7):
            rest_grad[0].append(first(*x_of(R, n)))
            rest_grad[1].append(first(*y_of(R, n, x + 2)))
            rest_grad[2].append(z_of(n))
        div = first(*x_of(R, 7)) + first(*y_of(R, 8, x + 2)) + z_of(7)
        A = [R[n, x + 2, mid, :] for n in range(6)]
        chi_inv = 1.0 / chi
        gd = [d0 * low[0], d1 * low[1], d2 * low[2]]
        dchi_up = [d0 * dchi[0], d1 * dchi[1], d2 * dchi[2]]
        grad_sq = dchi_up[0] * dchi[0] + dchi_up[1] * dchi[1] + dchi_up[2] * dchi[2]
        gd_trace = gd[0] * trace[0] + gd[1] * trace[1] + gd[2] * trace[2]
        gd_chi = gd[0] * dchi[0] + gd[1] * dchi[1] + gd[2] * dchi[2]
        ricci = 0.5 * (gd_trace - bend_g) + squares * (1.0 / 12.0) + 12.0 * div
        ham = (chi * ricci + 2.0 * (bend[0] - gd_chi) - 2.5 * grad_sq * chi_inv) * (1.0 / 144.0)
        ham = ham + PT[12, x, own, :]
        ham_out[x, own, :] = ham

        weight = 1.5 * chi_inv
        vec = [gd[l] + weight * dchi_up[l] for l in range(3)]
        vec[1] = vec[1] + u12 * vec[2]
        vec[0] = vec[0] + u01 * vec[1] + u02 * vec[2]
        twice = [PT[6 + n, x, own, :] for n in range(6)]
        squared = None
        for i in range(3):
            total = (-2.0 / 3.0) * rest_grad[i][6]
            for j in range(3):
                for k in range(3):
                    total = total + inv(j, k) * rest_grad[j][PAIR[k][i]]
            for l in range(3):
                total = total - vec[l] * A[PAIR[l][i]]
            for n in range(6):
                total = total - twice[n] * grads[i][1 + n]
            total = total * (1.0 / 12.0)
            mom_out[i, x, own, :] = total
            squared = total * total if squared is None else squared + total * total
        return ham * ham, squared

    def tally(x, b):
        own = pl.ds(pl.multiple_of(8 * b, 8), 8)
        ham = ham_out[x, own, :]
        m0, m1, m2 = [mom_out[n, x, own, :] for n in range(3)]
        ACC[0] += ham * ham
        ACC[1] += m0 * m0 + m1 * m1 + m2 * m2

    def inner(lo, hi):
        def body(i, _):
            x, last = 2 + lax.rem(i, 4), i // 4
            one, two = [cell(x, (1 - last) * (1 + n) + last * 3 * n) for n in range(2)]
            ACC[0] += one[0] + two[0]
            ACC[1] += one[1] + two[1]
            return 0

        lax.fori_loop(lo, hi, body, 0)

    inner(0, 4)
    send_terms(0)
    pl.semaphore_wait(near_sem, 4)
    twin = (ix, iy, iz + 1 - 2 * lax.rem(iz, 2))
    for device in [at(0, k, 0) for k in range(1, n_gy)] + [twin]:
        pl.semaphore_signal(far_sem, inc=1, device_id=device, device_id_type=MESH)
    all_geo_y.wait_recv()
    lax.fori_loop(0, PAIRS, open_y_geo, 0)
    x_rows(lambda k: k + 2, (0, 5))
    all_yz.wait_recv()
    for s in range(2):
        y_ends(s)
    lax.fori_loop(0, PAIRS, open_y_dz, 0)
    all_rest_y.wait_recv()
    lax.fori_loop(0, CX, open_y_rest, 0)
    send_terms(1)
    inner(4, 8)
    send_terms(2)
    pl.semaphore_wait(far_sem, n_gy)
    for k in range(1, n_gx):
        pl.semaphore_signal(last_sem, inc=1, device_id=at(k, 0, 0), device_id_type=MESH)

    all_xz.wait_recv()
    def x_changes(half):
        for sx in range(2):
            left, right = XER[sx, 0], XER[sx, 1]
            lefts = left, pltpu.roll(left, CZ - 2, 1)
            rights = pltpu.roll(right, 2, 1), right
            for v in range(2):
                own = packed([
                    F[c, (CX + 2) * sx + xi, OWN + 8 * b : OWN + 8 * b + 8, :] if b // 2 == half else None
                    for c in range(4 * v, min(4 * v + 4, GEO)) for xi in range(2) for b in range(BLOCKS)
                ])
                CXE[sx, v] = change(own, lefts[v], rights[v])[0]

    def x_ends(c, half):
        rows = slice(OWN + half * CY // 2, OWN + half * CY // 2 + CY // 2)
        for side in range(2):
            layers = slice(CX + 2, CX + 4) if side else slice(0, 2)
            out = along_z(F[c, layers, rows, :].reshape(CY, CZ), CZ)
            changed = CXE[side, c // 4]
            for xi in range(2):
                for b in range(2):
                    turn = CZ - 2 - 32 * (c % 4) - 4 * (BLOCKS * xi + 2 * half + b)
                    row = CY // 2 * xi + 8 * b
                    target = slice(rows.start + 8 * b, rows.start + 8 * b + 8)
                    DZ[c, layers.start + xi, target, :] = out[row : row + 8] + at_ends(changed, turn)

    def x_edge_rows(*tiles):
        x_rows(lambda k: k + (k // 2) * (CX - 4), tiles)

    def outer(b):
        def body(i, _):
            for n in range(2):
                cell((CX - 2) * i + n, b)
            return 0

        lax.fori_loop(0, 2, body, 0)

    x_changes(0)
    for c in range(GEO):
        x_ends(c, 0)
    x_edge_rows(1, 2, 3)
    send_terms(3)
    outer(1)
    x_changes(1)
    for c in range(GEO):
        x_ends(c, 1)
    x_edge_rows(4)
    outer(2)
    all_xy.wait_recv()
    for sx in range(2):
        for sy in range(2):
            for c in range(GEO):
                for k in range(2):
                    layer = (CX + 2 if sx else 0) + k
                    row = OWN + CY if sy else OWN - 2
                    F[c, layer, row : row + 2, :] = XYR[sx, sy, c * 4 + k * 2 : c * 4 + k * 2 + 2, :]
    x_edge_rows(0, 5)
    outer(0)
    outer(3)
    all_terms.wait_recv()

    def finish(k, _):
        side, sub = k // 2, lax.rem(k, 2)
        x = k + side * (CX - 4)
        ham_out[x] = ham_out[x] + CR[side, 0, sub]
        for n in range(3):
            mom_out[n, x] = mom_out[n, x] + CR[side, 1 + n, sub]
        for b in range(BLOCKS):
            tally(x, b)
        return 0

    lax.fori_loop(0, 4, finish, 0)
    halves = [jnp.sum(ACC[n], axis=0, keepdims=True) for n in range(2)]
    halves = [half + pltpu.roll(half, CZ // 2, 1) for half in halves]
    lower = lax.broadcasted_iota(jnp.int32, (1, CZ), 1) < CZ // 2
    MINE[0] = jnp.where(lower, halves[0], halves[1])
    n_chips = n_gz // 2
    n_plane, n_line = n_gy * n_chips, 2 * n_gx
    core = lax.rem(iz, 2)
    rank_a, rank_b = iy * n_chips + iz // 2, 2 * ix + core
    SUM_A[rank_a] = MINE[0]
    pl.semaphore_wait(last_sem, n_gx - 1)
    def is_lead(device):
        return (device[0] == LEAD[0]) & (device[1] == LEAD[1]) & (device[2] == LEAD[2])

    own = rank_b * n_plane + rank_a
    leading = is_lead((ix, iy, iz))
    ALL[own] = MINE[0]
    direct = remote(MINE.at[0], ALL.at[own], S_DIRECT, LEAD)
    pl.when(jnp.logical_not(leading))(direct.start)

    far_first = sorted(
        ((dy, k) for dy in range(n_gy) for k in range(n_chips) if dy or k),
        key=lambda p: -min(p[0], n_gy - p[0]) - min(p[1], n_chips - p[1]),
    )
    for dy, k in far_first:
        remote(MINE.at[0], SUM_A.at[rank_a], S_SUM_A, at(0, dy, 2 * k)).start()
    others = remote(SUM_A.at[pl.ds(0, n_plane - 1)], SUM_A.at[pl.ds(0, n_plane - 1)], S_SUM_A, at(0, 1, 0))
    others.wait_recv()
    total = SUM_A[0]
    for k in range(1, n_plane):
        total = total + SUM_A[k]
    MINE[1] = total
    SUM_B[rank_b] = total
    for dx in sorted(range(n_gx), key=lambda k: -min(k, n_gx - k)):
        for z in [zs[0], twin[2]] if dx else [twin[2]]:
            copy = remote(MINE.at[1], SUM_B.at[rank_b], S_SUM_B, (xs[dx], iy, z))
            pl.when(jnp.logical_not(is_lead((xs[dx], iy, z))))(copy.start)

    def norms(total):
        cells = float(CX * CY * CZ * n_gx * n_gy * n_gz)
        column = lax.broadcasted_iota(jnp.int32, (1, 2), 1)
        ham_sum = jnp.sum(jnp.where(lower, total, 0.0), axis=1, keepdims=True)
        mom_sum = jnp.sum(jnp.where(lower, 0.0, total), axis=1, keepdims=True)
        ham_sum, mom_sum = jnp.broadcast_to(ham_sum, (1, 2)), jnp.broadcast_to(mom_sum, (1, 2))
        norm_out[...] = jnp.sqrt(jnp.where(column == 0, ham_sum / cells, mom_sum / (3.0 * cells)))

    @pl.when(jnp.logical_not(leading))
    def _():
        group(SUM_B.at[0 : n_line - 1], S_SUM_B).wait_recv()
        total = SUM_B[0]
        for j in range(1, n_line):
            total = total + SUM_B[j]
        norms(total)

    @pl.when(leading)
    def _():
        group(ALL.at[0 : n_line * n_plane - 1], S_DIRECT).wait_recv()

        def rows_of(j):
            rows = ALL[n_plane * j]
            for k in range(1, n_plane):
                rows = rows + ALL[n_plane * j + k]
            return rows

        norms(lax.fori_loop(1, n_line, lambda j, total: total + rows_of(j), rows_of(0)))

    for sent in (all_geo_x, all_geo_y, all_geo_z, all_rest_y, all_rest_z, all_xy, all_yz, all_xz, all_terms, others):
        sent.wait_send()
    pl.when(jnp.logical_not(leading))(direct.wait_send)
    fewer = jnp.logical_not(leading) & (iy == LEAD[1]) & (iz // 2 == LEAD[2] // 2)
    pl.when(fewer)(group(SUM_B.at[0 : n_line - 2], S_SUM_B).wait_send)
    pl.when(jnp.logical_not(fewer))(group(SUM_B.at[0 : n_line - 1], S_SUM_B).wait_send)


def write_out(ham, mom, norm, ham_out, mom_out, norm_out, sems):
    copies = [
        pltpu.make_async_copy(src, dst, sems.at[i])
        for i, (src, dst) in enumerate(((ham, ham_out), (mom, mom_out), (norm, norm_out)))
    ]
    for copy in copies:
        copy.start()
    for copy in copies:
        copy.wait()


def solution(mesh):
    sizes = (mesh.shape["gx"], mesh.shape["gy"], mesh.shape["gz"])
    f32 = jnp.float32

    def step(chi, met, cur, trk, gam):
        vm = lambda *shape: pltpu.VMEM(shape, f32)
        ham, mom, norm = pl.pallas_call(
            functools.partial(kernel, sizes),
            out_shape=(
                pltpu.VMEM((CX, CY, CZ), f32),
                pltpu.VMEM((3, CX, CY, CZ), f32),
                pltpu.VMEM((1, 2), f32),
            ),
            in_specs=[pl.BlockSpec(memory_space=pl.ANY)] * 5,
            out_specs=(
                pl.BlockSpec(memory_space=pltpu.VMEM),
                pl.BlockSpec(memory_space=pltpu.VMEM),
                pl.BlockSpec(memory_space=pltpu.VMEM),
            ),
            scratch_shapes=[
                vm(GEO, LX, ROWS, CZ), vm(REST, LX, ROWS, CZ),
                vm(GEO, LX, ROWS, CZ), vm(GEO, CX, CY, CZ), vm(8, CX, CY, CZ),
                vm(GEO, CX, ROWS, CZ), vm(GEO, CX, ROWS, CZ), vm(2, 8, CZ),
                vm(2, 136, CZ), vm(2, 8, 2 * CX, CZ), vm(2, 136, CZ), vm(2, 8, 2 * CX, CZ),
                vm(2, 128, CZ), vm(2, 2, 8, CZ), vm(2, 2, 32, CZ),
                pltpu.VMEM((3 * CZ, 2 * CZ), jnp.bfloat16),
                vm(15, 8, CZ), vm(2, 15, 8, CZ), vm(15, 8, CZ), vm(GEO, 8, CZ),
                vm(2, 2, 8, CZ), vm(2, 2, 8, CZ), vm(2, 2, 8, CZ),
                vm(2, 4, 2, CY, CZ), vm(2, 4, 2, CY, CZ), vm(18, CX, CY, CZ),
                vm(2, 1, CZ), vm(sizes[1] * sizes[2] // 2, 1, CZ), vm(2 * sizes[0], 1, CZ), vm(sizes[0] * sizes[1] * sizes[2], 1, CZ),
                pltpu.SemaphoreType.DMA((3,)),
                pltpu.SemaphoreType.DMA((S_GEO_X + 1,)),
                pltpu.SemaphoreType.DMA((S_GEO_X + BLOCKS,)),
                pltpu.SemaphoreType.REGULAR,
                pltpu.SemaphoreType.REGULAR,
                pltpu.SemaphoreType.REGULAR,
                pltpu.SemaphoreType.REGULAR,
            ],
            compiler_params=pltpu.CompilerParams(collective_id=0, has_side_effects=True),
        )(chi, met, cur, trk, gam)
        ham, mom, norm = pl.pallas_call(
            write_out,
            out_shape=(
                jax.ShapeDtypeStruct((CX, CY, CZ), f32),
                jax.ShapeDtypeStruct((3, CX, CY, CZ), f32),
                jax.ShapeDtypeStruct((1, 2), f32),
            ),
            in_specs=[pl.BlockSpec(memory_space=pl.ANY)] * 3,
            out_specs=[pl.BlockSpec(memory_space=pl.ANY)] * 3,
            scratch_shapes=[pltpu.SemaphoreType.DMA((3,))],
        )(*[pltpu.with_memory_space_constraint(x, pltpu.VMEM) for x in (ham, mom, norm)])
        return ham, mom, norm.reshape(2)

    return jax.shard_map(
        step,
        mesh=mesh,
        in_specs=(
            P("gx", "gy", "gz"),
            P(None, "gx", "gy", "gz"),
            P(None, "gx", "gy", "gz"),
            P("gx", "gy", "gz"),
            P(None, "gx", "gy", "gz"),
        ),
        out_specs=(P("gx", "gy", "gz"), P(None, "gx", "gy", "gz"), P()),
        check_vma=False,
    )
```

```python
import functools

import jax
import jax.numpy as jnp
from jax import lax
from jax.experimental import pallas as pl
from jax.experimental.pallas import tpu as pltpu
from jax.sharding import PartitionSpec as P

MESH = pl.DeviceIdType.MESH
PAIR = ((0, 1, 2), (1, 3, 4), (2, 4, 5))

CX, CY, CZ = 8, 32, 128
LX, ROWS, OWN = CX + 4, 48, 8
BLOCKS = CY // 8
PAIRS = CX // 2
GEO, REST = 7, 10
Y_REST = (0, 1, 2, 3, 4, 5, 6, 8)
Z_REST = (0, 1, 2, 3, 4, 5, 6, 9)
X_REST = 8

S_GEO_Y, S_GEO_Z, S_REST_Y, S_REST_Z, S_EDGE_XY, S_EDGE_YZ, S_EDGE_XZ, S_TERM = range(8)
S_SUM_A, S_SUM_B, S_DIRECT, S_GEO_X = 8, 9, 10, 11
SENT = {
    S_GEO_X: 0, S_REST_Y: 0, S_REST_Z: 0, S_EDGE_XY: 0, S_TERM: 0,
    S_GEO_Y: 1, S_GEO_Z: 1, S_EDGE_YZ: 1, S_EDGE_XZ: 1, S_SUM_A: 2, S_SUM_B: 3, S_DIRECT: 4,
}
LEAD = (0, 0, 1)


def lane_ids():
    return lax.broadcasted_iota(jnp.int32, (8, CZ), 1)


def inverse_of(g):
    g00, g01, g02, g11, g12, g22 = g
    m00 = g11 * g22 - g12 * g12
    m01 = g02 * g12 - g01 * g22
    m02 = g01 * g12 - g02 * g11
    m11 = g00 * g22 - g02 * g02
    m12 = g01 * g02 - g00 * g12
    m22 = g00 * g11 - g01 * g01
    scale = 1.0 / (g00 * m00 + g01 * m01 + g02 * m02)
    return [m00 * scale, m01 * scale, m02 * scale, m11 * scale, m12 * scale, m22 * scale]


def first(lo2, lo1, hi1, hi2):
    return (lo2 - hi2) + 8.0 * (hi1 - lo1)


def second(lo2, lo1, mid, hi1, hi2):
    return 16.0 * (lo1 + hi1) - (lo2 + hi2) - 30.0 * mid


def kernel(
    sizes,
    chi_in, met_in, cur_in, trk_in, gam_in,
    ham_out, mom_out, norm_out,
    F, R, DZ, DZZ, DZR, DX, DXX, ACC,
    YSG, YSR, YRG, YRR, YDZ, YZR, XYR, TAPS,
    ZP, ZPR, C1, C2, XE, XER, CXE,
    CS, CR, PT, MINE, SUM_A, SUM_B, ALL,
    load_sem, send_sem, recv_sem, two_sem, near_sem, far_sem, last_sem,
):
    n_gx, n_gy, n_gz = sizes
    ix, iy, iz = lax.axis_index("gx"), lax.axis_index("gy"), lax.axis_index("gz")
    xs = {k: lax.rem(ix + k + n_gx, n_gx) for k in range(-2, n_gx)}
    ys = {k: lax.rem(iy + k + n_gy, n_gy) for k in range(-1, n_gy)}
    zs = {k: lax.rem(iz + k + n_gz, n_gz) for k in range(-2, n_gz)}

    def at(dx, dy, dz):
        return xs[dx], ys[dy], zs[dz]

    def remote(src, dst, place, device, part=0):
        return pltpu.make_async_remote_copy(
            src_ref=src, dst_ref=dst, send_sem=send_sem.at[SENT[place]], recv_sem=recv_sem.at[place + part],
            device_id=device, device_id_type=MESH,
        )

    def group(whole, place, part=0):
        return remote(whole, whole, place, at(1, 0, 0), part)

    def block(src, dst, lo, hi):
        if len(src.shape) == 3:
            return src.at[lo:hi], dst.at[2 + lo : 2 + hi, OWN : OWN + CY]
        return src.at[:, lo:hi], dst.at[:, 2 + lo : 2 + hi, OWN : OWN + CY]

    layers = ((0, 2), (CX - 2, CX), (2, CX - 2))
    loads = [block(src, dst, lo, hi) for lo, hi in layers for src, dst in ((chi_in, F.at[0]), (met_in, F.at[1:7]))]
    loads += [
        block(src, dst, 0, CX) for src, dst in ((cur_in, R.at[0:6]), (trk_in, R.at[6]), (gam_in, R.at[7:10]))
    ]
    loads = [pltpu.make_async_copy(s, d, load_sem.at[(i > 3) + (i > 5)]) for i, (s, d) in enumerate(loads)]
    for copy in loads:
        copy.start()

    barrier = pltpu.get_barrier_semaphore()
    faces = [(-1, 0, 0), (1, 0, 0), (0, -1, 0), (0, 1, 0), (0, 0, -1), (0, 0, 1)]
    for step in faces:
        pl.semaphore_signal(barrier, inc=1, device_id=at(*step), device_id_type=MESH)

    lane = lane_ids()
    lane4, place = lane // 4, lax.rem(lane, 4)
    ends = (lane < 2) | (lane >= CZ - 2)
    zero = jnp.zeros((8, CZ), jnp.float32)

    def clear(c, _):
        for layer in (0, 1, LX - 2, LX - 1):
            for b in range(BLOCKS):
                R[c, layer, pl.ds(OWN + 8 * b, 8), :] = zero
        return 0

    lax.fori_loop(0, X_REST, clear, 0)
    ACC[...] = jnp.zeros_like(ACC)

    def packed(tiles):
        out = zero
        for t, tile in enumerate(tiles):
            if tile is None:
                continue
            turn = (4 * t + 2) % CZ
            out = jnp.where(lane4 == t, pltpu.roll(tile, turn, 1) if turn else tile, out)
        return out

    def own_tiles(ref, c):
        return [ref[c, 2 + x, pl.ds(OWN + 8 * b, 8), :] for x in range(CX) for b in range(BLOCKS)]

    def pack_y_geo(p, _):
        for c in range(GEO):
            for xi in range(2):
                rows = pl.ds(32 * p + c * 4 + xi * 2, 2)
                YSG[0, rows, :] = F[c, 2 + 2 * p + xi, OWN : OWN + 2, :]
                YSG[1, rows, :] = F[c, 2 + 2 * p + xi, OWN + CY - 2 : OWN + CY, :]
        return 0

    def pack_y_rest(x, _):
        rows = pl.ds(2 * x, 2)
        for n, c in enumerate(Y_REST):
            YSR[0, n, rows, :] = R[c, 2 + x, OWN : OWN + 2, :]
            YSR[1, n, rows, :] = R[c, 2 + x, OWN + CY - 2 : OWN + CY, :]
        return 0

    def geo_x(d, b):
        rows = pl.ds(OWN + 8 * b, 8)
        src = F.at[0:GEO, pl.ds(CX if d else 2, 2), rows]
        dst = F.at[0:GEO, pl.ds(0 if d else CX + 2, 2), rows]
        return remote(src, dst, S_GEO_X, at(2 * d - 1, 0, 0), b)

    geo_xs = [[geo_x(d, b) for b in range(BLOCKS)] for d in range(2)]
    geo_ys = [remote(YSG.at[d], YRG.at[1 - d], S_GEO_Y, at(0, 2 * d - 1, 0)) for d in range(2)]
    geo_zs = [remote(ZP.at[0:GEO], ZPR.at[1 - d, 0:GEO], S_GEO_Z, at(0, 0, 2 * d - 1)) for d in range(2)]
    rest_ys = [remote(YSR.at[d], YRR.at[1 - d], S_REST_Y, at(0, 2 * d - 1, 0)) for d in range(2)]
    rest_zs = [
        remote(ZP.at[GEO : GEO + 8], ZPR.at[1 - d, GEO : GEO + 8], S_REST_Z, at(0, 0, 2 * d - 1)) for d in range(2)
    ]
    combos = [(a, b) for a in range(2) for b in range(2)]
    edge_xy = [
        remote(
            YSG.at[dy, pl.ds(96 if dx else 0, 32)], XYR.at[1 - dx, 1 - dy], S_EDGE_XY,
            at(2 * dx - 1, 2 * dy - 1, 0),
        )
        for dx, dy in combos
    ]
    edge_yz = [
        remote(
            YSG.at[dy, 128:136], YZR.at[1 - dz, 1 - dy], S_EDGE_YZ, at(0, 2 * dy - 1, 2 * dz - 1)
        )
        for dy, dz in combos
    ]
    edge_xz = [
        remote(XE.at[dx, dz], XER.at[1 - dx, 1 - dz], S_EDGE_XZ, at(2 * dx - 1, 0, 2 * dz - 1))
        for dx, dz in combos
    ]

    column = lax.broadcasted_iota(jnp.int32, (CZ, 2 * CZ), 1)
    step = lax.rem(lax.broadcasted_iota(jnp.int32, (CZ, 2 * CZ), 0) - column + 2 * CZ, CZ)

    def weights(table):
        out = jnp.zeros((CZ, 2 * CZ), jnp.float32)
        for k, w in table:
            out = jnp.where(step == k % CZ, w, out)
        return out

    taps = jnp.where(
        column < CZ,
        weights(((-2, 1.0), (-1, -8.0), (1, 8.0), (2, -1.0))),
        weights(((-2, -1.0), (-1, 16.0), (0, -30.0), (1, 16.0), (2, -1.0))),
    ).astype(jnp.bfloat16)
    for k in range(3):
        TAPS[CZ * k : CZ * k + CZ, :] = taps
    for s in range(2):
        for p in range(PAIRS):
            YSG[s, 32 * p + 24 : 32 * p + 32, :] = zero

    def along_z(cells, width):
        high = cells.astype(jnp.bfloat16)
        rest = cells - high.astype(jnp.float32)
        middle = rest.astype(jnp.bfloat16)
        low = (rest - middle.astype(jnp.float32)).astype(jnp.bfloat16)
        pieces = jnp.concatenate([high, middle, low], axis=1)
        return jnp.dot(pieces, TAPS[:, 0:width], preferred_element_type=jnp.float32)

    all_geo_y, all_rest_y = group(YRG, S_GEO_Y), group(YRR, S_REST_Y)
    all_geo_z, all_rest_z = group(ZPR.at[:, 0:GEO], S_GEO_Z), group(ZPR.at[:, GEO : GEO + 8], S_REST_Z)
    all_xy, all_yz, all_xz = group(XYR, S_EDGE_XY), group(YZR, S_EDGE_YZ), group(XER, S_EDGE_XZ)
    all_terms = group(CR, S_TERM)

    half = F.at[:, 2 : 2 + CX // 2, OWN : OWN + CY]
    pltpu.make_async_copy(half, half, load_sem.at[0]).wait()
    pl.semaphore_wait(barrier, len(faces))
    for step in faces:
        pl.semaphore_signal(two_sem, inc=1, device_id=at(*step), device_id_type=MESH)
    for b in range(BLOCKS - 1):
        for d in range(2):
            geo_xs[d][b].start()
    pltpu.make_async_copy(half, half, load_sem.at[1]).wait()
    for c in range(GEO):
        ZP[c] = packed(own_tiles(F, c))
    for copy in geo_zs:
        copy.start()
    lax.fori_loop(0, PAIRS, pack_y_geo, 0)
    for s in range(2):
        YSG[s, 128:136, :] = packed([YSG[s, 8 * k : 8 * k + 8, :] for k in range(16)])
        parts = []
        for v in range(2):
            out = zero
            for c in range(4 * v, min(4 * v + 4, GEO)):
                turn = (32 * (c % 4) - 96 * s) % CZ
                out = jnp.where(lane // 32 == c % 4, pltpu.roll(ZP[c], turn, 1) if turn else ZP[c], out)
            parts.append(out)
        XE[s, 0] = jnp.where(place < 2, pltpu.roll(parts[0], CZ - 2, 1), parts[1])
        XE[s, 1] = jnp.where(place < 2, parts[0], pltpu.roll(parts[1], 2, 1))
    for copy in geo_ys:
        copy.start()
    whole = R.at[:, 2 : 2 + CX, OWN : OWN + CY]
    pltpu.make_async_copy(whole, whole, load_sem.at[2]).wait()
    for n, c in enumerate(Z_REST):
        ZP[GEO + n] = packed(own_tiles(R, c))
    for copy in rest_zs:
        copy.start()
    lax.fori_loop(0, CX, pack_y_rest, 0)
    for copy in rest_ys:
        copy.start()

    own_rows = (slice(2, 2 + CX), slice(OWN, OWN + CY))

    def z_geo(c):
        out = along_z(F[c, own_rows[0], own_rows[1], :].reshape(CX * CY, CZ), 2 * CZ)
        DZ[c, own_rows[0], own_rows[1], :] = out[:, 0:CZ].reshape(CX, CY, CZ)
        DZZ[c] = out[:, CZ:].reshape(CX, CY, CZ)

    def z_rest(n):
        c = n + (n // 7) * 2
        DZR[n] = along_z(R[c, own_rows[0], own_rows[1], :].reshape(CX * CY, CZ), CZ).reshape(CX, CY, CZ)

    def x_rows(layers, tiles):
        def body(k, _):
            x = layers(k)
            for b in tiles:
                rows = slice(8 * b, 8 * b + 8)
                for c in range(GEO):
                    taps = [F[c, x + k, rows, :] for k in range(5)]
                    DX[c, x, rows, :] = first(taps[0], taps[1], taps[3], taps[4])
                    DXX[c, x, rows, :] = second(*taps)
            return 0

        lax.fori_loop(0, 4, body, 0)

    for c in range(GEO):
        z_geo(c)
    for n in range(8):
        z_rest(n)
    pl.semaphore_wait(two_sem, len(faces))
    for copy in edge_yz + [geo_xs[0][BLOCKS - 1], geo_xs[1][BLOCKS - 1]] + edge_xz + edge_xy:
        copy.start()
    for step in [(-2, 0, 0), (2, 0, 0), (0, 0, -2), (0, 0, 2)]:
        pl.semaphore_signal(near_sem, inc=1, device_id=at(*step), device_id_type=MESH)
    x_rows(lambda k: k + 2, (1, 2, 3, 4))
    def point(i, _):
        x = i // 2
        for n in range(2):
            b = 2 * lax.rem(i, 2) + n
            mid = pl.ds(pl.multiple_of(OWN + 8 * b, 8), 8)
            own = pl.ds(pl.multiple_of(8 * b, 8), 8)
            g00, g01, g02, g11, g12, g22 = [F[1 + k, x + 2, mid, :] for k in range(6)]
            m00 = g11 * g22 - g12 * g12
            m01 = g02 * g12 - g01 * g22
            m02 = g01 * g12 - g02 * g11
            m11 = g00 * g22 - g02 * g02
            m12 = g01 * g02 - g00 * g12
            m22 = g00 * g11 - g01 * g01
            scale = 1.0 / (g00 * m00 + g01 * m01 + g02 * m02)
            gu = [m00 * scale, m01 * scale, m02 * scale, m11 * scale, m12 * scale, m22 * scale]
            d0 = 1.0 / g00
            m_inv = 1.0 / m22
            u01, u12 = -g01 * d0, m12 * m_inv

            def inv(i, j):
                return gu[PAIR[i][j]]

            A = [R[k, x + 2, mid, :] for k in range(6)]
            K = R[6, x + 2, mid, :]
            mixed = [
                [A[PAIR[i][0]] * inv(0, j) + A[PAIR[i][1]] * inv(1, j) + A[PAIR[i][2]] * inv(2, j) for j in range(3)]
                for i in range(3)
            ]
            raised = [
                inv(i, 0) * mixed[0][j] + inv(i, 1) * mixed[1][j] + inv(i, 2) * mixed[2][j]
                for i, j in ((0, 0), (0, 1), (0, 2), (1, 1), (1, 2), (2, 2))
            ]
            a_sq = mixed[0][0] * mixed[0][0] + mixed[1][1] * mixed[1][1] + mixed[2][2] * mixed[2][2]
            a_sq = a_sq + 2.0 * (
                mixed[0][1] * mixed[1][0] + mixed[0][2] * mixed[2][0] + mixed[1][2] * mixed[2][1]
            )
            twice = [0.5 * raised[0], raised[1], raised[2], 0.5 * raised[3], raised[4], 0.5 * raised[5]]
            kept = gu + twice + [(2.0 / 3.0) * (K * K) - a_sq]
            kept += [u01, m02 * m_inv - u12 * u01, u12, d0, g00 * m_inv]
            for k, value in enumerate(kept):
                PT[k, x, own, :] = value
        return 0

    lax.fori_loop(0, 2 * CX, point, 0)
    def term(d, b):
        rows = pl.ds(8 * b, 8)
        return remote(CS.at[d, :, :, rows], CR.at[1 - d, :, :, rows], S_TERM, at(2 * d - 1, 0, 0))

    terms = [[term(d, b) for b in range(BLOCKS)] for d in range(2)]

    def send_terms(b):
        mid = pl.ds(OWN + 8 * b, 8)
        group(F.at[:, 2 : 2 + CX // 2, OWN : OWN + 8], S_GEO_X, b).wait_recv()
        for d in range(2):
            halo = CX + 2 if d else 0
            for k in range(2):
                gu = inverse_of([F[1 + n, halo + k, mid, :] for n in range(6)])
                chi = F[0, halo + k, mid, :]

                def part(n):
                    if d == 0:
                        f0 = R[n, 2, mid, :]
                        return -f0 if k == 0 else 8.0 * f0 - R[n, 3, mid, :]
                    f7 = R[n, CX + 1, mid, :]
                    return R[n, CX, mid, :] - 8.0 * f7 if k == 0 else f7

                a = [part(n) for n in range(8)]
                own = pl.ds(8 * b, 8)
                CS[d, 0, k, own, :] = chi * a[7] * (1.0 / 12.0)
                for i in range(3):
                    value = gu[0] * a[PAIR[0][i]] + gu[1] * a[PAIR[1][i]] + gu[2] * a[PAIR[2][i]]
                    if i == 0:
                        value = value - (2.0 / 3.0) * a[6]
                    CS[d, 1 + i, k, own, :] = value * (1.0 / 12.0)
        for d in range(2):
            terms[d][b].start()

    all_geo_z.wait_recv()

    def change(own, left, right):
        e = jnp.where(place < 2, left, right) - own
        hi2, hi1, lo1, lo2 = (pltpu.roll(e, k, 1) for k in (CZ - 2, CZ - 1, 1, 2))
        hi1 = jnp.where(place == 1, hi1, 0.0)
        lo1 = jnp.where(place == 2, lo1, 0.0)
        return (
            jnp.where(place < 2, 8.0 * hi1 - hi2, lo2 - 8.0 * lo1),
            16.0 * (hi1 + lo1) - jnp.where(place < 2, hi2, lo2),
        )

    def at_ends(change, turn):
        return jnp.where(ends, pltpu.roll(change, turn, 1), 0.0)

    for c in range(GEO):
        C1[c], C2[c] = change(ZP[c], ZPR[0, c], ZPR[1, c])

    def z_ends(half, _):
        for c in range(GEO):
            changed = C1[c]
            for k in range(4):
                x = 4 * half + k
                for b in range(BLOCKS):
                    rows = pl.ds(OWN + 8 * b, 8)
                    DZ[c, x + 2, rows, :] += at_ends(changed, CZ - 2 - 4 * (BLOCKS * x + b))
        return 0

    lax.fori_loop(0, 2, z_ends, 0)
    all_rest_z.wait_recv()
    for n in range(8):
        C1[GEO + n] = change(ZP[GEO + n], ZPR[0, GEO + n], ZPR[1, GEO + n])[0]

    def open_y_rest(x, _):
        rows = pl.ds(2 * x, 2)
        for n, c in enumerate(Y_REST):
            R[c, 2 + x, OWN - 2 : OWN, :] = YRR[0, n, rows, :]
            R[c, 2 + x, OWN + CY : OWN + CY + 2, :] = YRR[1, n, rows, :]
        return 0

    def open_y_geo(p, _):
        for c in range(GEO):
            for xi in range(2):
                rows = pl.ds(32 * p + c * 4 + xi * 2, 2)
                F[c, 2 + 2 * p + xi, OWN - 2 : OWN, :] = YRG[0, rows, :]
                F[c, 2 + 2 * p + xi, OWN + CY : OWN + CY + 2, :] = YRG[1, rows, :]
        return 0

    def y_ends(s):
        changed = change(YRG[s, 128:136, :], YZR[0, s], YZR[1, s])[0]
        out = along_z(YRG[s, 0:128, :], CZ)
        for k in range(16):
            rows = slice(8 * k, 8 * k + 8)
            YDZ[s, rows, :] = out[rows] + at_ends(changed, CZ - 2 - 4 * k)

    def open_y_dz(p, _):
        for c in range(GEO):
            for xi in range(2):
                rows = pl.ds(32 * p + c * 4 + xi * 2, 2)
                DZ[c, 2 + 2 * p + xi, OWN - 2 : OWN, :] = YDZ[0, rows, :]
                DZ[c, 2 + 2 * p + xi, OWN + CY : OWN + CY + 2, :] = YDZ[1, rows, :]
        return 0

    def cell(x, b):
        r0 = OWN + 8 * b
        mid = pl.ds(pl.multiple_of(r0, 8), 8)
        own = pl.ds(pl.multiple_of(8 * b, 8), 8)
        turn = CZ - 2 - 4 * (BLOCKS * x + b)

        def y_of(ref, c, layer):
            return [ref[c, layer, pl.ds(r0 + k, 8), :] for k in (-2, -1, 1, 2)]

        def x_of(ref, c):
            return [ref[c, x + 2 + k, mid, :] for k in (-2, -1, 1, 2)]

        chi = F[0, x + 2, mid, :]
        gu = [PT[n, x, own, :] for n in range(6)]
        wide = [gu[0], 2.0 * gu[1], 2.0 * gu[2], gu[3], 2.0 * gu[4], gu[5]]
        same = [12.0 * gu[0], 12.0 * gu[3], 12.0 * gu[5]]

        grads, bend = [[], [], []], []
        for c in range(GEO):
            f = F[c, x + 2, mid, :]
            ys = y_of(F, c, x + 2)
            grads[0].append(DX[c, x, mid, :])
            grads[1].append(first(*ys))
            grads[2].append(DZ[c, x + 2, mid, :])
            bend.append(
                same[0] * DXX[c, x, mid, :]
                + same[1] * second(ys[0], ys[1], f, ys[2], ys[3])
                + same[2] * (DZZ[c, x, own, :] + at_ends(C2[c], turn))
                + wide[1] * first(*y_of(DX, c, x))
                + wide[2] * first(*x_of(DZ, c))
                + wide[4] * first(*y_of(DZ, c, x + 2))
            )
        dchi = [grads[a][0] for a in range(3)]
        bend_g = sum(wide[n] * bend[1 + n] for n in range(1, 6)) + wide[0] * bend[1]

        def d(a, i, j):
            return grads[a][1 + PAIR[i][j]]

        def inv(i, j):
            return gu[PAIR[i][j]]

        def along(values):
            one = values[1] + u01 * values[0]
            return [values[0], one, values[2] + u12 * one + u02 * values[0]]

        u01, u02, u12, d0, d1 = [PT[n, x, own, :] for n in range(13, 18)]
        d2 = gu[5]
        trace = []
        for a in range(3):
            t = wide[0] * grads[a][1]
            for n in range(1, 6):
                t = t + wide[n] * grads[a][1 + n]
            trace.append(t)
        trace = along(trace)
        dchi = along(dchi)

        cyc = {
            (0, 0, 0): 3.0 * d(0, 0, 0), (1, 1, 1): 3.0 * d(1, 1, 1), (2, 2, 2): 3.0 * d(2, 2, 2),
            (0, 0, 1): 2.0 * d(0, 0, 1) + d(1, 0, 0), (0, 0, 2): 2.0 * d(0, 0, 2) + d(2, 0, 0),
            (0, 1, 1): 2.0 * d(1, 0, 1) + d(0, 1, 1), (1, 1, 2): 2.0 * d(1, 1, 2) + d(2, 1, 1),
            (0, 2, 2): 2.0 * d(2, 0, 2) + d(0, 2, 2), (1, 2, 2): 2.0 * d(2, 1, 2) + d(1, 2, 2),
            (0, 1, 2): d(0, 1, 2) + d(1, 0, 2) + d(2, 0, 1),
        }

        s000 = cyc[0, 0, 0]
        s001 = cyc[0, 0, 1] + u01 * s000
        s011 = cyc[0, 1, 1] + u01 * cyc[0, 0, 1]
        s111 = cyc[1, 1, 1] + u01 * cyc[0, 1, 1] + u01 * s011
        s011 = s011 + u01 * s001
        s111 = s111 + u01 * s011
        a00 = cyc[0, 0, 2]
        a01 = cyc[0, 1, 2] + u01 * a00
        a11 = cyc[1, 1, 2] + u01 * cyc[0, 1, 2] + u01 * a01
        b0 = cyc[0, 2, 2]
        b1 = cyc[1, 2, 2] + u01 * b0
        b2 = cyc[2, 2, 2] + u12 * b1 + u02 * b0
        s002 = a00 + u12 * s001 + u02 * s000
        s012 = a01 + u12 * s011 + u02 * s001
        s112 = a11 + u12 * s111 + u02 * s011
        b0 = b0 + u12 * a01 + u02 * a00
        b1 = b1 + u12 * a11 + u02 * a01
        s022 = b0 + u12 * s012 + u02 * s002
        s122 = b1 + u12 * s112 + u02 * s012
        s222 = b2 + u12 * b1 + u02 * b0 + u12 * s122 + u02 * s022
        low = [
            0.5 * (d0 * s000 + d1 * s011 + d2 * s022) - trace[0],
            0.5 * (d0 * s001 + d1 * s111 + d2 * s122) - trace[1],
            0.5 * (d0 * s002 + d1 * s112 + d2 * s222) - trace[2],
        ]
        three1, three2 = 3.0 * d1, 3.0 * d2
        both2 = three2 * d2
        squares = d0 * (
            d0 * (d0 * (s000 * s000) + three1 * (s001 * s001) + three2 * (s002 * s002))
            + three1 * (d1 * (s011 * s011) + (2.0 * d2) * (s012 * s012))
            + both2 * (s022 * s022)
        )
        squares = squares + d1 * (
            d1 * (d1 * (s111 * s111) + three2 * (s112 * s112)) + both2 * (s122 * s122)
        )
        squares = squares + (d2 * d2) * (d2 * (s222 * s222))

        def z_of(n):
            return DZR[n, x, own, :] + at_ends(C1[GEO + n], turn)

        rest_grad = [[], [], []]
        for n in range(7):
            rest_grad[0].append(first(*x_of(R, n)))
            rest_grad[1].append(first(*y_of(R, n, x + 2)))
            rest_grad[2].append(z_of(n))
        div = first(*x_of(R, 7)) + first(*y_of(R, 8, x + 2)) + z_of(7)
        A = [R[n, x + 2, mid, :] for n in range(6)]
        chi_inv = 1.0 / chi
        gd = [d0 * low[0], d1 * low[1], d2 * low[2]]
        dchi_up = [d0 * dchi[0], d1 * dchi[1], d2 * dchi[2]]
        grad_sq = dchi_up[0] * dchi[0] + dchi_up[1] * dchi[1] + dchi_up[2] * dchi[2]
        gd_trace = gd[0] * trace[0] + gd[1] * trace[1] + gd[2] * trace[2]
        gd_chi = gd[0] * dchi[0] + gd[1] * dchi[1] + gd[2] * dchi[2]
        ricci = 0.5 * (gd_trace - bend_g) + squares * (1.0 / 12.0) + 12.0 * div
        ham = (chi * ricci + 2.0 * (bend[0] - gd_chi) - 2.5 * grad_sq * chi_inv) * (1.0 / 144.0)
        ham = ham + PT[12, x, own, :]
        ham_out[x, own, :] = ham

        weight = 1.5 * chi_inv
        vec = [gd[l] + weight * dchi_up[l] for l in range(3)]
        vec[1] = vec[1] + u12 * vec[2]
        vec[0] = vec[0] + u01 * vec[1] + u02 * vec[2]
        twice = [PT[6 + n, x, own, :] for n in range(6)]
        squared = None
        for i in range(3):
            total = (-2.0 / 3.0) * rest_grad[i][6]
            for j in range(3):
                for k in range(3):
                    total = total + inv(j, k) * rest_grad[j][PAIR[k][i]]
            for l in range(3):
                total = total - vec[l] * A[PAIR[l][i]]
            for n in range(6):
                total = total - twice[n] * grads[i][1 + n]
            total = total * (1.0 / 12.0)
            mom_out[i, x, own, :] = total
            squared = total * total if squared is None else squared + total * total
        return ham * ham, squared

    def tally(x, b):
        own = pl.ds(pl.multiple_of(8 * b, 8), 8)
        ham = ham_out[x, own, :]
        m0, m1, m2 = [mom_out[n, x, own, :] for n in range(3)]
        ACC[0] += ham * ham
        ACC[1] += m0 * m0 + m1 * m1 + m2 * m2

    def inner(lo, hi):
        def body(i, _):
            x, last = 2 + lax.rem(i, 4), i // 4
            one, two = [cell(x, (1 - last) * (1 + n) + last * 3 * n) for n in range(2)]
            ACC[0] += one[0] + two[0]
            ACC[1] += one[1] + two[1]
            return 0

        lax.fori_loop(lo, hi, body, 0)

    inner(0, 4)
    send_terms(0)
    pl.semaphore_wait(near_sem, 4)
    twin = (ix, iy, iz + 1 - 2 * lax.rem(iz, 2))
    for device in [at(0, k, 0) for k in range(1, n_gy)] + [twin]:
        pl.semaphore_signal(far_sem, inc=1, device_id=device, device_id_type=MESH)
    all_geo_y.wait_recv()
    lax.fori_loop(0, PAIRS, open_y_geo, 0)
    x_rows(lambda k: k + 2, (0, 5))
    all_yz.wait_recv()
    for s in range(2):
        y_ends(s)
    lax.fori_loop(0, PAIRS, open_y_dz, 0)
    all_rest_y.wait_recv()
    lax.fori_loop(0, CX, open_y_rest, 0)
    send_terms(1)
    inner(4, 6)
    send_terms(2)
    inner(6, 8)
    pl.semaphore_wait(far_sem, n_gy)
    for k in range(1, n_gx):
        pl.semaphore_signal(last_sem, inc=1, device_id=at(k, 0, 0), device_id_type=MESH)

    send_terms(3)
    all_xz.wait_recv()
    def x_changes(half):
        for sx in range(2):
            left, right = XER[sx, 0], XER[sx, 1]
            lefts = left, pltpu.roll(left, CZ - 2, 1)
            rights = pltpu.roll(right, 2, 1), right
            for v in range(2):
                own = packed([
                    F[c, (CX + 2) * sx + xi, OWN + 8 * b : OWN + 8 * b + 8, :] if b // 2 == half else None
                    for c in range(4 * v, min(4 * v + 4, GEO)) for xi in range(2) for b in range(BLOCKS)
                ])
                CXE[sx, v] = change(own, lefts[v], rights[v])[0]

    def x_ends(c, half):
        rows = slice(OWN + half * CY // 2, OWN + half * CY // 2 + CY // 2)
        for side in range(2):
            layers = slice(CX + 2, CX + 4) if side else slice(0, 2)
            out = along_z(F[c, layers, rows, :].reshape(CY, CZ), CZ)
            changed = CXE[side, c // 4]
            for xi in range(2):
                for b in range(2):
                    turn = CZ - 2 - 32 * (c % 4) - 4 * (BLOCKS * xi + 2 * half + b)
                    row = CY // 2 * xi + 8 * b
                    target = slice(rows.start + 8 * b, rows.start + 8 * b + 8)
                    DZ[c, layers.start + xi, target, :] = out[row : row + 8] + at_ends(changed, turn)

    def x_edge_rows(*tiles):
        x_rows(lambda k: k + (k // 2) * (CX - 4), tiles)

    def outer(b):
        def body(i, _):
            for n in range(2):
                cell((CX - 2) * i + n, b)
            return 0

        lax.fori_loop(0, 2, body, 0)

    x_changes(0)
    for c in range(GEO):
        x_ends(c, 0)
    x_edge_rows(1, 2, 3)
    outer(1)
    x_changes(1)
    for c in range(GEO):
        x_ends(c, 1)
    x_edge_rows(4)
    outer(2)
    all_xy.wait_recv()
    for sx in range(2):
        for sy in range(2):
            for c in range(GEO):
                for k in range(2):
                    layer = (CX + 2 if sx else 0) + k
                    row = OWN + CY if sy else OWN - 2
                    F[c, layer, row : row + 2, :] = XYR[sx, sy, c * 4 + k * 2 : c * 4 + k * 2 + 2, :]
    x_edge_rows(0, 5)
    outer(0)
    outer(3)
    all_terms.wait_recv()

    def finish(k, _):
        side, sub = k // 2, lax.rem(k, 2)
        x = k + side * (CX - 4)
        ham_out[x] = ham_out[x] + CR[side, 0, sub]
        for n in range(3):
            mom_out[n, x] = mom_out[n, x] + CR[side, 1 + n, sub]
        for b in range(BLOCKS):
            tally(x, b)
        return 0

    lax.fori_loop(0, 4, finish, 0)
    halves = [jnp.sum(ACC[n], axis=0, keepdims=True) for n in range(2)]
    halves = [half + pltpu.roll(half, CZ // 2, 1) for half in halves]
    lower = lax.broadcasted_iota(jnp.int32, (1, CZ), 1) < CZ // 2
    MINE[0] = jnp.where(lower, halves[0], halves[1])
    n_chips = n_gz // 2
    n_plane, n_line = n_gy * n_chips, 2 * n_gx
    core = lax.rem(iz, 2)
    rank_a, rank_b = iy * n_chips + iz // 2, 2 * ix + core
    SUM_A[rank_a] = MINE[0]
    pl.semaphore_wait(last_sem, n_gx - 1)
    def is_lead(device):
        return (device[0] == LEAD[0]) & (device[1] == LEAD[1]) & (device[2] == LEAD[2])

    own = rank_b * n_plane + rank_a
    leading = is_lead((ix, iy, iz))
    ALL[own] = MINE[0]
    direct = remote(MINE.at[0], ALL.at[own], S_DIRECT, LEAD)
    pl.when(jnp.logical_not(leading))(direct.start)

    far_first = sorted(
        ((dy, k) for dy in range(n_gy) for k in range(n_chips) if dy or k),
        key=lambda p: -min(p[0], n_gy - p[0]) - min(p[1], n_chips - p[1]),
    )
    for dy, k in far_first:
        remote(MINE.at[0], SUM_A.at[rank_a], S_SUM_A, at(0, dy, 2 * k)).start()
    others = remote(SUM_A.at[pl.ds(0, n_plane - 1)], SUM_A.at[pl.ds(0, n_plane - 1)], S_SUM_A, at(0, 1, 0))
    others.wait_recv()
    total = SUM_A[0]
    for k in range(1, n_plane):
        total = total + SUM_A[k]
    MINE[1] = total
    SUM_B[rank_b] = total
    for dx in sorted(range(n_gx), key=lambda k: -min(k, n_gx - k)):
        for z in [zs[0], twin[2]] if dx else [twin[2]]:
            copy = remote(MINE.at[1], SUM_B.at[rank_b], S_SUM_B, (xs[dx], iy, z))
            pl.when(jnp.logical_not(is_lead((xs[dx], iy, z))))(copy.start)

    def norms(total):
        cells = float(CX * CY * CZ * n_gx * n_gy * n_gz)
        column = lax.broadcasted_iota(jnp.int32, (1, 2), 1)
        ham_sum = jnp.sum(jnp.where(lower, total, 0.0), axis=1, keepdims=True)
        mom_sum = jnp.sum(jnp.where(lower, 0.0, total), axis=1, keepdims=True)
        ham_sum, mom_sum = jnp.broadcast_to(ham_sum, (1, 2)), jnp.broadcast_to(mom_sum, (1, 2))
        norm_out[...] = jnp.sqrt(jnp.where(column == 0, ham_sum / cells, mom_sum / (3.0 * cells)))

    @pl.when(jnp.logical_not(leading))
    def _():
        group(SUM_B.at[0 : n_line - 1], S_SUM_B).wait_recv()
        total = SUM_B[0]
        for j in range(1, n_line):
            total = total + SUM_B[j]
        norms(total)

    @pl.when(leading)
    def _():
        group(ALL.at[0 : n_line * n_plane - 1], S_DIRECT).wait_recv()

        def rows_of(j):
            rows = ALL[n_plane * j]
            for k in range(1, n_plane):
                rows = rows + ALL[n_plane * j + k]
            return rows

        norms(lax.fori_loop(1, n_line, lambda j, total: total + rows_of(j), rows_of(0)))

    group(PT.at[0:15, 0:4], S_GEO_X).wait_send()
    group(PT.at[0:7, 0:2], S_GEO_Y).wait_send()
    others.wait_send()
    pl.when(jnp.logical_not(leading))(direct.wait_send)
    fewer = jnp.logical_not(leading) & (iy == LEAD[1]) & (iz // 2 == LEAD[2] // 2)
    pl.when(fewer)(group(SUM_B.at[0 : n_line - 2], S_SUM_B).wait_send)
    pl.when(jnp.logical_not(fewer))(group(SUM_B.at[0 : n_line - 1], S_SUM_B).wait_send)


def write_out(ham, mom, norm, ham_out, mom_out, norm_out, sems):
    copies = [
        pltpu.make_async_copy(src, dst, sems.at[i])
        for i, (src, dst) in enumerate(((ham, ham_out), (mom, mom_out), (norm, norm_out)))
    ]
    for copy in copies:
        copy.start()
    for copy in copies:
        copy.wait()


def solution(mesh):
    sizes = (mesh.shape["gx"], mesh.shape["gy"], mesh.shape["gz"])
    f32 = jnp.float32

    def step(chi, met, cur, trk, gam):
        vm = lambda *shape: pltpu.VMEM(shape, f32)
        ham, mom, norm = pl.pallas_call(
            functools.partial(kernel, sizes),
            out_shape=(
                pltpu.VMEM((CX, CY, CZ), f32),
                pltpu.VMEM((3, CX, CY, CZ), f32),
                pltpu.VMEM((1, 2), f32),
            ),
            in_specs=[pl.BlockSpec(memory_space=pl.ANY)] * 5,
            out_specs=(
                pl.BlockSpec(memory_space=pltpu.VMEM),
                pl.BlockSpec(memory_space=pltpu.VMEM),
                pl.BlockSpec(memory_space=pltpu.VMEM),
            ),
            scratch_shapes=[
                vm(GEO, LX, ROWS, CZ), vm(REST, LX, ROWS, CZ),
                vm(GEO, LX, ROWS, CZ), vm(GEO, CX, CY, CZ), vm(8, CX, CY, CZ),
                vm(GEO, CX, ROWS, CZ), vm(GEO, CX, ROWS, CZ), vm(2, 8, CZ),
                vm(2, 136, CZ), vm(2, 8, 2 * CX, CZ), vm(2, 136, CZ), vm(2, 8, 2 * CX, CZ),
                vm(2, 128, CZ), vm(2, 2, 8, CZ), vm(2, 2, 32, CZ),
                pltpu.VMEM((3 * CZ, 2 * CZ), jnp.bfloat16),
                vm(15, 8, CZ), vm(2, 15, 8, CZ), vm(15, 8, CZ), vm(GEO, 8, CZ),
                vm(2, 2, 8, CZ), vm(2, 2, 8, CZ), vm(2, 2, 8, CZ),
                vm(2, 4, 2, CY, CZ), vm(2, 4, 2, CY, CZ), vm(18, CX, CY, CZ),
                vm(2, 1, CZ), vm(sizes[1] * sizes[2] // 2, 1, CZ), vm(2 * sizes[0], 1, CZ), vm(sizes[0] * sizes[1] * sizes[2], 1, CZ),
                pltpu.SemaphoreType.DMA((3,)),
                pltpu.SemaphoreType.DMA((5,)),
                pltpu.SemaphoreType.DMA((S_GEO_X + BLOCKS,)),
                pltpu.SemaphoreType.REGULAR,
                pltpu.SemaphoreType.REGULAR,
                pltpu.SemaphoreType.REGULAR,
                pltpu.SemaphoreType.REGULAR,
            ],
            compiler_params=pltpu.CompilerParams(collective_id=0, has_side_effects=True),
        )(chi, met, cur, trk, gam)
        ham, mom, norm = pl.pallas_call(
            write_out,
            out_shape=(
                jax.ShapeDtypeStruct((CX, CY, CZ), f32),
                jax.ShapeDtypeStruct((3, CX, CY, CZ), f32),
                jax.ShapeDtypeStruct((1, 2), f32),
            ),
            in_specs=[pl.BlockSpec(memory_space=pl.ANY)] * 3,
            out_specs=[pl.BlockSpec(memory_space=pl.ANY)] * 3,
            scratch_shapes=[pltpu.SemaphoreType.DMA((3,))],
        )(*[pltpu.with_memory_space_constraint(x, pltpu.VMEM) for x in (ham, mom, norm)])
        return ham, mom, norm.reshape(2)

    return jax.shard_map(
        step,
        mesh=mesh,
        in_specs=(
            P("gx", "gy", "gz"),
            P(None, "gx", "gy", "gz"),
            P(None, "gx", "gy", "gz"),
            P("gx", "gy", "gz"),
            P(None, "gx", "gy", "gz"),
        ),
        out_specs=(P("gx", "gy", "gz"), P(None, "gx", "gy", "gz"), P()),
        check_vma=False,
    )
```

```python
import functools

import jax
import jax.numpy as jnp
from jax import lax
from jax.experimental import pallas as pl
from jax.experimental.pallas import tpu as pltpu
from jax.sharding import PartitionSpec as P

MESH = pl.DeviceIdType.MESH
PAIR = ((0, 1, 2), (1, 3, 4), (2, 4, 5))

CX, CY, CZ = 8, 32, 128
LX, ROWS, OWN = CX + 4, 48, 8
BLOCKS = CY // 8
PAIRS = CX // 2
GEO, REST = 7, 10
Y_REST = (0, 1, 2, 3, 4, 5, 6, 8)
Z_REST = (0, 1, 2, 3, 4, 5, 6, 9)
X_REST = 8

S_GEO_Y, S_GEO_Z, S_REST_Y, S_REST_Z, S_EDGE_XY, S_EDGE_YZ, S_EDGE_XZ, S_TERM = range(8)
S_SUM_A, S_SUM_B, S_DIRECT, S_GEO_X = 8, 9, 10, 11
SENT = {
    S_GEO_X: 0, S_REST_Y: 0, S_REST_Z: 0, S_EDGE_XY: 0, S_TERM: 0,
    S_GEO_Y: 1, S_GEO_Z: 1, S_EDGE_YZ: 1, S_EDGE_XZ: 1, S_SUM_A: 2, S_SUM_B: 3, S_DIRECT: 4,
}
LEAD = (0, 0, 1)


def lane_ids():
    return lax.broadcasted_iota(jnp.int32, (8, CZ), 1)


def inverse_of(g):
    g00, g01, g02, g11, g12, g22 = g
    m00 = g11 * g22 - g12 * g12
    m01 = g02 * g12 - g01 * g22
    m02 = g01 * g12 - g02 * g11
    m11 = g00 * g22 - g02 * g02
    m12 = g01 * g02 - g00 * g12
    m22 = g00 * g11 - g01 * g01
    scale = 1.0 / (g00 * m00 + g01 * m01 + g02 * m02)
    return [m00 * scale, m01 * scale, m02 * scale, m11 * scale, m12 * scale, m22 * scale]


def first(lo2, lo1, hi1, hi2):
    return (lo2 - hi2) + 8.0 * (hi1 - lo1)


def second(lo2, lo1, mid, hi1, hi2):
    return 16.0 * (lo1 + hi1) - (lo2 + hi2) - 30.0 * mid


def kernel(
    sizes,
    chi_in, met_in, cur_in, trk_in, gam_in,
    ham_out, mom_out, norm_out,
    F, R, DZ, DZZ, DZR, DX, DXX, ACC,
    YSG, YSR, YRG, YRR, YDZ, YZR, XYR, TAPS,
    ZP, ZPR, C1, C2, XE, XER, CXE,
    CS, CR, PT, MINE, SUM_A, SUM_B, ALL,
    load_sem, send_sem, recv_sem, two_sem, near_sem, far_sem, last_sem,
):
    n_gx, n_gy, n_gz = sizes
    ix, iy, iz = lax.axis_index("gx"), lax.axis_index("gy"), lax.axis_index("gz")
    xs = {k: lax.rem(ix + k + n_gx, n_gx) for k in range(-2, n_gx)}
    ys = {k: lax.rem(iy + k + n_gy, n_gy) for k in range(-1, n_gy)}
    zs = {k: lax.rem(iz + k + n_gz, n_gz) for k in range(-2, n_gz)}

    def at(dx, dy, dz):
        return xs[dx], ys[dy], zs[dz]

    def remote(src, dst, place, device, part=0):
        return pltpu.make_async_remote_copy(
            src_ref=src, dst_ref=dst, send_sem=send_sem.at[SENT[place]], recv_sem=recv_sem.at[place + part],
            device_id=device, device_id_type=MESH,
        )

    def group(whole, place, part=0):
        return remote(whole, whole, place, at(1, 0, 0), part)

    def block(src, dst, lo, hi):
        if len(src.shape) == 3:
            return src.at[lo:hi], dst.at[2 + lo : 2 + hi, OWN : OWN + CY]
        return src.at[:, lo:hi], dst.at[:, 2 + lo : 2 + hi, OWN : OWN + CY]

    layers = ((0, 2), (CX - 2, CX), (2, CX - 2))
    loads = [block(src, dst, lo, hi) for lo, hi in layers for src, dst in ((chi_in, F.at[0]), (met_in, F.at[1:7]))]
    loads += [
        block(src, dst, 0, CX) for src, dst in ((cur_in, R.at[0:6]), (trk_in, R.at[6]), (gam_in, R.at[7:10]))
    ]
    loads = [pltpu.make_async_copy(s, d, load_sem.at[(i > 3) + (i > 5)]) for i, (s, d) in enumerate(loads)]
    for copy in loads:
        copy.start()

    barrier = pltpu.get_barrier_semaphore()
    faces = [(-1, 0, 0), (1, 0, 0), (0, -1, 0), (0, 1, 0), (0, 0, -1), (0, 0, 1)]
    for step in faces:
        pl.semaphore_signal(barrier, inc=1, device_id=at(*step), device_id_type=MESH)

    lane = lane_ids()
    lane4, place = lane // 4, lax.rem(lane, 4)
    ends = (lane < 2) | (lane >= CZ - 2)
    zero = jnp.zeros((8, CZ), jnp.float32)

    def clear(c, _):
        for layer in (0, 1, LX - 2, LX - 1):
            for b in range(BLOCKS):
                R[c, layer, pl.ds(OWN + 8 * b, 8), :] = zero
        return 0

    lax.fori_loop(0, X_REST, clear, 0)
    ACC[...] = jnp.zeros_like(ACC)

    def packed(tiles):
        out = zero
        for t, tile in enumerate(tiles):
            if tile is None:
                continue
            turn = (4 * t + 2) % CZ
            out = jnp.where(lane4 == t, pltpu.roll(tile, turn, 1) if turn else tile, out)
        return out

    def own_tiles(ref, c):
        return [ref[c, 2 + x, pl.ds(OWN + 8 * b, 8), :] for x in range(CX) for b in range(BLOCKS)]

    def pack_y_geo(p, _):
        for c in range(GEO):
            for xi in range(2):
                rows = pl.ds(32 * p + c * 4 + xi * 2, 2)
                YSG[0, rows, :] = F[c, 2 + 2 * p + xi, OWN : OWN + 2, :]
                YSG[1, rows, :] = F[c, 2 + 2 * p + xi, OWN + CY - 2 : OWN + CY, :]
        return 0

    def pack_y_rest(x, _):
        rows = pl.ds(2 * x, 2)
        for n, c in enumerate(Y_REST):
            YSR[0, n, rows, :] = R[c, 2 + x, OWN : OWN + 2, :]
            YSR[1, n, rows, :] = R[c, 2 + x, OWN + CY - 2 : OWN + CY, :]
        return 0

    def geo_x(d, b):
        rows = pl.ds(OWN + 8 * b, 8)
        src = F.at[0:GEO, pl.ds(CX if d else 2, 2), rows]
        dst = F.at[0:GEO, pl.ds(0 if d else CX + 2, 2), rows]
        return remote(src, dst, S_GEO_X, at(2 * d - 1, 0, 0), b)

    geo_xs = [[geo_x(d, b) for b in range(BLOCKS)] for d in range(2)]
    geo_ys = [remote(YSG.at[d], YRG.at[1 - d], S_GEO_Y, at(0, 2 * d - 1, 0)) for d in range(2)]
    geo_zs = [remote(ZP.at[0:GEO], ZPR.at[1 - d, 0:GEO], S_GEO_Z, at(0, 0, 2 * d - 1)) for d in range(2)]
    rest_ys = [remote(YSR.at[d], YRR.at[1 - d], S_REST_Y, at(0, 2 * d - 1, 0)) for d in range(2)]
    rest_zs = [
        remote(ZP.at[GEO : GEO + 8], ZPR.at[1 - d, GEO : GEO + 8], S_REST_Z, at(0, 0, 2 * d - 1)) for d in range(2)
    ]
    combos = [(a, b) for a in range(2) for b in range(2)]
    edge_xy = [
        remote(
            YSG.at[dy, pl.ds(96 if dx else 0, 32)], XYR.at[1 - dx, 1 - dy], S_EDGE_XY,
            at(2 * dx - 1, 2 * dy - 1, 0),
        )
        for dx, dy in combos
    ]
    edge_yz = [
        remote(
            YSG.at[dy, 128:136], YZR.at[1 - dz, 1 - dy], S_EDGE_YZ, at(0, 2 * dy - 1, 2 * dz - 1)
        )
        for dy, dz in combos
    ]
    edge_xz = [
        remote(XE.at[dx, dz], XER.at[1 - dx, 1 - dz], S_EDGE_XZ, at(2 * dx - 1, 0, 2 * dz - 1))
        for dx, dz in combos
    ]

    column = lax.broadcasted_iota(jnp.int32, (CZ, 2 * CZ), 1)
    step = lax.rem(lax.broadcasted_iota(jnp.int32, (CZ, 2 * CZ), 0) - column + 2 * CZ, CZ)

    def weights(table):
        out = jnp.zeros((CZ, 2 * CZ), jnp.float32)
        for k, w in table:
            out = jnp.where(step == k % CZ, w, out)
        return out

    taps = jnp.where(
        column < CZ,
        weights(((-2, 1.0), (-1, -8.0), (1, 8.0), (2, -1.0))),
        weights(((-2, -1.0), (-1, 16.0), (0, -30.0), (1, 16.0), (2, -1.0))),
    ).astype(jnp.bfloat16)
    for k in range(3):
        TAPS[CZ * k : CZ * k + CZ, :] = taps
    for s in range(2):
        for p in range(PAIRS):
            YSG[s, 32 * p + 24 : 32 * p + 32, :] = zero

    def along_z(cells, width):
        high = cells.astype(jnp.bfloat16)
        rest = cells - high.astype(jnp.float32)
        middle = rest.astype(jnp.bfloat16)
        low = (rest - middle.astype(jnp.float32)).astype(jnp.bfloat16)
        pieces = jnp.concatenate([high, middle, low], axis=1)
        return jnp.dot(pieces, TAPS[:, 0:width], preferred_element_type=jnp.float32)

    all_geo_y, all_rest_y = group(YRG, S_GEO_Y), group(YRR, S_REST_Y)
    all_geo_z, all_rest_z = group(ZPR.at[:, 0:GEO], S_GEO_Z), group(ZPR.at[:, GEO : GEO + 8], S_REST_Z)
    all_xy, all_yz, all_xz = group(XYR, S_EDGE_XY), group(YZR, S_EDGE_YZ), group(XER, S_EDGE_XZ)
    all_terms = group(CR, S_TERM)

    half = F.at[:, 2 : 2 + CX // 2, OWN : OWN + CY]
    pltpu.make_async_copy(half, half, load_sem.at[0]).wait()
    pl.semaphore_wait(barrier, len(faces))
    for step in faces:
        pl.semaphore_signal(two_sem, inc=1, device_id=at(*step), device_id_type=MESH)
    for b in range(BLOCKS - 1):
        for d in range(2):
            geo_xs[d][b].start()
    pltpu.make_async_copy(half, half, load_sem.at[1]).wait()
    for c in range(GEO):
        ZP[c] = packed(own_tiles(F, c))
    for copy in geo_zs:
        copy.start()
    lax.fori_loop(0, PAIRS, pack_y_geo, 0)
    for s in range(2):
        YSG[s, 128:136, :] = packed([YSG[s, 8 * k : 8 * k + 8, :] for k in range(16)])
        parts = []
        for v in range(2):
            out = zero
            for c in range(4 * v, min(4 * v + 4, GEO)):
                turn = (32 * (c % 4) - 96 * s) % CZ
                out = jnp.where(lane // 32 == c % 4, pltpu.roll(ZP[c], turn, 1) if turn else ZP[c], out)
            parts.append(out)
        XE[s, 0] = jnp.where(place < 2, pltpu.roll(parts[0], CZ - 2, 1), parts[1])
        XE[s, 1] = jnp.where(place < 2, parts[0], pltpu.roll(parts[1], 2, 1))
    for copy in geo_ys:
        copy.start()
    whole = R.at[:, 2 : 2 + CX, OWN : OWN + CY]
    pltpu.make_async_copy(whole, whole, load_sem.at[2]).wait()
    for n, c in enumerate(Z_REST):
        ZP[GEO + n] = packed(own_tiles(R, c))
    for copy in rest_zs:
        copy.start()
    lax.fori_loop(0, CX, pack_y_rest, 0)
    for copy in rest_ys:
        copy.start()

    own_rows = (slice(2, 2 + CX), slice(OWN, OWN + CY))

    def z_geo(c):
        out = along_z(F[c, own_rows[0], own_rows[1], :].reshape(CX * CY, CZ), 2 * CZ)
        DZ[c, own_rows[0], own_rows[1], :] = out[:, 0:CZ].reshape(CX, CY, CZ)
        DZZ[c] = out[:, CZ:].reshape(CX, CY, CZ)

    def z_rest(n):
        c = n + (n // 7) * 2
        DZR[n] = along_z(R[c, own_rows[0], own_rows[1], :].reshape(CX * CY, CZ), CZ).reshape(CX, CY, CZ)

    def x_rows(layers, tiles):
        def body(k, _):
            x = layers(k)
            for b in tiles:
                rows = slice(8 * b, 8 * b + 8)
                for c in range(GEO):
                    taps = [F[c, x + k, rows, :] for k in range(5)]
                    DX[c, x, rows, :] = first(taps[0], taps[1], taps[3], taps[4])
                    DXX[c, x, rows, :] = second(*taps)
            return 0

        lax.fori_loop(0, 4, body, 0)

    for c in range(GEO):
        z_geo(c)
    for n in range(8):
        z_rest(n)
    pl.semaphore_wait(two_sem, len(faces))
    for copy in edge_yz + [geo_xs[0][BLOCKS - 1], geo_xs[1][BLOCKS - 1]] + edge_xz + edge_xy:
        copy.start()
    for step in [(-2, 0, 0), (2, 0, 0), (0, 0, -2), (0, 0, 2)]:
        pl.semaphore_signal(near_sem, inc=1, device_id=at(*step), device_id_type=MESH)
    x_rows(lambda k: k + 2, (1, 2, 3, 4))
    def point(i, _):
        x = i // 2
        for n in range(2):
            b = 2 * lax.rem(i, 2) + n
            mid = pl.ds(pl.multiple_of(OWN + 8 * b, 8), 8)
            own = pl.ds(pl.multiple_of(8 * b, 8), 8)
            g00, g01, g02, g11, g12, g22 = [F[1 + k, x + 2, mid, :] for k in range(6)]
            m00 = g11 * g22 - g12 * g12
            m01 = g02 * g12 - g01 * g22
            m02 = g01 * g12 - g02 * g11
            m11 = g00 * g22 - g02 * g02
            m12 = g01 * g02 - g00 * g12
            m22 = g00 * g11 - g01 * g01
            scale = 1.0 / (g00 * m00 + g01 * m01 + g02 * m02)
            gu = [m00 * scale, m01 * scale, m02 * scale, m11 * scale, m12 * scale, m22 * scale]
            d0 = 1.0 / g00
            m_inv = 1.0 / m22
            u01, u12 = -g01 * d0, m12 * m_inv

            def inv(i, j):
                return gu[PAIR[i][j]]

            A = [R[k, x + 2, mid, :] for k in range(6)]
            K = R[6, x + 2, mid, :]
            mixed = [
                [A[PAIR[i][0]] * inv(0, j) + A[PAIR[i][1]] * inv(1, j) + A[PAIR[i][2]] * inv(2, j) for j in range(3)]
                for i in range(3)
            ]
            raised = [
                inv(i, 0) * mixed[0][j] + inv(i, 1) * mixed[1][j] + inv(i, 2) * mixed[2][j]
                for i, j in ((0, 0), (0, 1), (0, 2), (1, 1), (1, 2), (2, 2))
            ]
            a_sq = mixed[0][0] * mixed[0][0] + mixed[1][1] * mixed[1][1] + mixed[2][2] * mixed[2][2]
            a_sq = a_sq + 2.0 * (
                mixed[0][1] * mixed[1][0] + mixed[0][2] * mixed[2][0] + mixed[1][2] * mixed[2][1]
            )
            twice = [0.5 * raised[0], raised[1], raised[2], 0.5 * raised[3], raised[4], 0.5 * raised[5]]
            kept = gu + twice + [(2.0 / 3.0) * (K * K) - a_sq]
            kept += [u01, m02 * m_inv - u12 * u01, u12, d0, g00 * m_inv]
            for k, value in enumerate(kept):
                PT[k, x, own, :] = value
        return 0

    lax.fori_loop(0, 2 * CX, point, 0)
    def term(d, b):
        rows = pl.ds(8 * b, 8)
        return remote(CS.at[d, :, :, rows], CR.at[1 - d, :, :, rows], S_TERM, at(2 * d - 1, 0, 0))

    terms = [[term(d, b) for b in range(BLOCKS)] for d in range(2)]

    def send_terms(b):
        mid = pl.ds(OWN + 8 * b, 8)
        group(F.at[:, 2 : 2 + CX // 2, OWN : OWN + 8], S_GEO_X, b).wait_recv()
        for d in range(2):
            halo = CX + 2 if d else 0
            for k in range(2):
                gu = inverse_of([F[1 + n, halo + k, mid, :] for n in range(6)])
                chi = F[0, halo + k, mid, :]

                def part(n):
                    if d == 0:
                        f0 = R[n, 2, mid, :]
                        return -f0 if k == 0 else 8.0 * f0 - R[n, 3, mid, :]
                    f7 = R[n, CX + 1, mid, :]
                    return R[n, CX, mid, :] - 8.0 * f7 if k == 0 else f7

                a = [part(n) for n in range(8)]
                own = pl.ds(8 * b, 8)
                CS[d, 0, k, own, :] = chi * a[7] * (1.0 / 12.0)
                for i in range(3):
                    value = gu[0] * a[PAIR[0][i]] + gu[1] * a[PAIR[1][i]] + gu[2] * a[PAIR[2][i]]
                    if i == 0:
                        value = value - (2.0 / 3.0) * a[6]
                    CS[d, 1 + i, k, own, :] = value * (1.0 / 12.0)
        for d in range(2):
            terms[d][b].start()

    all_geo_z.wait_recv()

    def change(own, left, right):
        e = jnp.where(place < 2, left, right) - own
        hi2, hi1, lo1, lo2 = (pltpu.roll(e, k, 1) for k in (CZ - 2, CZ - 1, 1, 2))
        hi1 = jnp.where(place == 1, hi1, 0.0)
        lo1 = jnp.where(place == 2, lo1, 0.0)
        return (
            jnp.where(place < 2, 8.0 * hi1 - hi2, lo2 - 8.0 * lo1),
            16.0 * (hi1 + lo1) - jnp.where(place < 2, hi2, lo2),
        )

    def at_ends(change, turn):
        return jnp.where(ends, pltpu.roll(change, turn, 1), 0.0)

    for c in range(GEO):
        C1[c], C2[c] = change(ZP[c], ZPR[0, c], ZPR[1, c])

    def z_ends(half, _):
        for c in range(GEO):
            changed = C1[c]
            for k in range(4):
                x = 4 * half + k
                for b in range(BLOCKS):
                    rows = pl.ds(OWN + 8 * b, 8)
                    DZ[c, x + 2, rows, :] += at_ends(changed, CZ - 2 - 4 * (BLOCKS * x + b))
        return 0

    lax.fori_loop(0, 2, z_ends, 0)
    all_rest_z.wait_recv()
    for n in range(8):
        C1[GEO + n] = change(ZP[GEO + n], ZPR[0, GEO + n], ZPR[1, GEO + n])[0]

    def open_y_rest(x, _):
        rows = pl.ds(2 * x, 2)
        for n, c in enumerate(Y_REST):
            R[c, 2 + x, OWN - 2 : OWN, :] = YRR[0, n, rows, :]
            R[c, 2 + x, OWN + CY : OWN + CY + 2, :] = YRR[1, n, rows, :]
        return 0

    def open_y_geo(p, _):
        for c in range(GEO):
            for xi in range(2):
                rows = pl.ds(32 * p + c * 4 + xi * 2, 2)
                F[c, 2 + 2 * p + xi, OWN - 2 : OWN, :] = YRG[0, rows, :]
                F[c, 2 + 2 * p + xi, OWN + CY : OWN + CY + 2, :] = YRG[1, rows, :]
        return 0

    def y_ends(s):
        changed = change(YRG[s, 128:136, :], YZR[0, s], YZR[1, s])[0]
        out = along_z(YRG[s, 0:128, :], CZ)
        for k in range(16):
            rows = slice(8 * k, 8 * k + 8)
            YDZ[s, rows, :] = out[rows] + at_ends(changed, CZ - 2 - 4 * k)

    def open_y_dz(p, _):
        for c in range(GEO):
            for xi in range(2):
                rows = pl.ds(32 * p + c * 4 + xi * 2, 2)
                DZ[c, 2 + 2 * p + xi, OWN - 2 : OWN, :] = YDZ[0, rows, :]
                DZ[c, 2 + 2 * p + xi, OWN + CY : OWN + CY + 2, :] = YDZ[1, rows, :]
        return 0

    def cell(x, b):
        r0 = OWN + 8 * b
        mid = pl.ds(pl.multiple_of(r0, 8), 8)
        own = pl.ds(pl.multiple_of(8 * b, 8), 8)
        turn = CZ - 2 - 4 * (BLOCKS * x + b)

        def y_of(ref, c, layer):
            return [ref[c, layer, pl.ds(r0 + k, 8), :] for k in (-2, -1, 1, 2)]

        def x_of(ref, c):
            return [ref[c, x + 2 + k, mid, :] for k in (-2, -1, 1, 2)]

        chi = F[0, x + 2, mid, :]
        gu = [PT[n, x, own, :] for n in range(6)]
        wide = [gu[0], 2.0 * gu[1], 2.0 * gu[2], gu[3], 2.0 * gu[4], gu[5]]
        same = [12.0 * gu[0], 12.0 * gu[3], 12.0 * gu[5]]

        grads, bend = [[], [], []], []
        for c in range(GEO):
            f = F[c, x + 2, mid, :]
            ys = y_of(F, c, x + 2)
            grads[0].append(DX[c, x, mid, :])
            grads[1].append(first(*ys))
            grads[2].append(DZ[c, x + 2, mid, :])
            bend.append(
                same[0] * DXX[c, x, mid, :]
                + same[1] * second(ys[0], ys[1], f, ys[2], ys[3])
                + same[2] * (DZZ[c, x, own, :] + at_ends(C2[c], turn))
                + wide[1] * first(*y_of(DX, c, x))
                + wide[2] * first(*x_of(DZ, c))
                + wide[4] * first(*y_of(DZ, c, x + 2))
            )
        dchi = [grads[a][0] for a in range(3)]
        bend_g = sum(wide[n] * bend[1 + n] for n in range(1, 6)) + wide[0] * bend[1]

        def d(a, i, j):
            return grads[a][1 + PAIR[i][j]]

        def inv(i, j):
            return gu[PAIR[i][j]]

        def along(values):
            one = values[1] + u01 * values[0]
            return [values[0], one, values[2] + u12 * one + u02 * values[0]]

        u01, u02, u12, d0, d1 = [PT[n, x, own, :] for n in range(13, 18)]
        d2 = gu[5]
        trace = []
        for a in range(3):
            t = wide[0] * grads[a][1]
            for n in range(1, 6):
                t = t + wide[n] * grads[a][1 + n]
            trace.append(t)
        trace = along(trace)
        dchi = along(dchi)

        cyc = {
            (0, 0, 0): 3.0 * d(0, 0, 0), (1, 1, 1): 3.0 * d(1, 1, 1), (2, 2, 2): 3.0 * d(2, 2, 2),
            (0, 0, 1): 2.0 * d(0, 0, 1) + d(1, 0, 0), (0, 0, 2): 2.0 * d(0, 0, 2) + d(2, 0, 0),
            (0, 1, 1): 2.0 * d(1, 0, 1) + d(0, 1, 1), (1, 1, 2): 2.0 * d(1, 1, 2) + d(2, 1, 1),
            (0, 2, 2): 2.0 * d(2, 0, 2) + d(0, 2, 2), (1, 2, 2): 2.0 * d(2, 1, 2) + d(1, 2, 2),
            (0, 1, 2): d(0, 1, 2) + d(1, 0, 2) + d(2, 0, 1),
        }

        s000 = cyc[0, 0, 0]
        s001 = cyc[0, 0, 1] + u01 * s000
        s011 = cyc[0, 1, 1] + u01 * cyc[0, 0, 1]
        s111 = cyc[1, 1, 1] + u01 * cyc[0, 1, 1] + u01 * s011
        s011 = s011 + u01 * s001
        s111 = s111 + u01 * s011
        a00 = cyc[0, 0, 2]
        a01 = cyc[0, 1, 2] + u01 * a00
        a11 = cyc[1, 1, 2] + u01 * cyc[0, 1, 2] + u01 * a01
        b0 = cyc[0, 2, 2]
        b1 = cyc[1, 2, 2] + u01 * b0
        b2 = cyc[2, 2, 2] + u12 * b1 + u02 * b0
        s002 = a00 + u12 * s001 + u02 * s000
        s012 = a01 + u12 * s011 + u02 * s001
        s112 = a11 + u12 * s111 + u02 * s011
        b0 = b0 + u12 * a01 + u02 * a00
        b1 = b1 + u12 * a11 + u02 * a01
        s022 = b0 + u12 * s012 + u02 * s002
        s122 = b1 + u12 * s112 + u02 * s012
        s222 = b2 + u12 * b1 + u02 * b0 + u12 * s122 + u02 * s022
        low = [
            0.5 * (d0 * s000 + d1 * s011 + d2 * s022) - trace[0],
            0.5 * (d0 * s001 + d1 * s111 + d2 * s122) - trace[1],
            0.5 * (d0 * s002 + d1 * s112 + d2 * s222) - trace[2],
        ]
        three1, three2 = 3.0 * d1, 3.0 * d2
        both2 = three2 * d2
        squares = d0 * (
            d0 * (d0 * (s000 * s000) + three1 * (s001 * s001) + three2 * (s002 * s002))
            + three1 * (d1 * (s011 * s011) + (2.0 * d2) * (s012 * s012))
            + both2 * (s022 * s022)
        )
        squares = squares + d1 * (
            d1 * (d1 * (s111 * s111) + three2 * (s112 * s112)) + both2 * (s122 * s122)
        )
        squares = squares + (d2 * d2) * (d2 * (s222 * s222))

        def z_of(n):
            return DZR[n, x, own, :] + at_ends(C1[GEO + n], turn)

        rest_grad = [[], [], []]
        for n in range(7):
            rest_grad[0].append(first(*x_of(R, n)))
            rest_grad[1].append(first(*y_of(R, n, x + 2)))
            rest_grad[2].append(z_of(n))
        div = first(*x_of(R, 7)) + first(*y_of(R, 8, x + 2)) + z_of(7)
        A = [R[n, x + 2, mid, :] for n in range(6)]
        chi_inv = 1.0 / chi
        gd = [d0 * low[0], d1 * low[1], d2 * low[2]]
        dchi_up = [d0 * dchi[0], d1 * dchi[1], d2 * dchi[2]]
        grad_sq = dchi_up[0] * dchi[0] + dchi_up[1] * dchi[1] + dchi_up[2] * dchi[2]
        gd_trace = gd[0] * trace[0] + gd[1] * trace[1] + gd[2] * trace[2]
        gd_chi = gd[0] * dchi[0] + gd[1] * dchi[1] + gd[2] * dchi[2]
        ricci = 0.5 * (gd_trace - bend_g) + squares * (1.0 / 12.0) + 12.0 * div
        ham = (chi * ricci + 2.0 * (bend[0] - gd_chi) - 2.5 * grad_sq * chi_inv) * (1.0 / 144.0)
        ham = ham + PT[12, x, own, :]
        ham_out[x, own, :] = ham

        weight = 1.5 * chi_inv
        vec = [gd[l] + weight * dchi_up[l] for l in range(3)]
        vec[1] = vec[1] + u12 * vec[2]
        vec[0] = vec[0] + u01 * vec[1] + u02 * vec[2]
        twice = [PT[6 + n, x, own, :] for n in range(6)]
        squared = None
        for i in range(3):
            total = (-2.0 / 3.0) * rest_grad[i][6]
            for j in range(3):
                for k in range(3):
                    total = total + inv(j, k) * rest_grad[j][PAIR[k][i]]
            for l in range(3):
                total = total - vec[l] * A[PAIR[l][i]]
            for n in range(6):
                total = total - twice[n] * grads[i][1 + n]
            total = total * (1.0 / 12.0)
            mom_out[i, x, own, :] = total
            squared = total * total if squared is None else squared + total * total
        return ham * ham, squared

    def tally(x, b):
        own = pl.ds(pl.multiple_of(8 * b, 8), 8)
        ham = ham_out[x, own, :]
        m0, m1, m2 = [mom_out[n, x, own, :] for n in range(3)]
        ACC[0] += ham * ham
        ACC[1] += m0 * m0 + m1 * m1 + m2 * m2

    def inner(lo, hi):
        def body(i, _):
            x, last = 2 + lax.rem(i, 4), i // 4
            one, two = [cell(x, (1 - last) * (1 + n) + last * 3 * n) for n in range(2)]
            ACC[0] += one[0] + two[0]
            ACC[1] += one[1] + two[1]
            return 0

        lax.fori_loop(lo, hi, body, 0)

    inner(0, 4)
    send_terms(0)
    pl.semaphore_wait(near_sem, 4)
    twin = (ix, iy, iz + 1 - 2 * lax.rem(iz, 2))
    for device in [at(0, k, 0) for k in range(1, n_gy)] + [twin]:
        pl.semaphore_signal(far_sem, inc=1, device_id=device, device_id_type=MESH)
    all_geo_y.wait_recv()
    lax.fori_loop(0, PAIRS, open_y_geo, 0)
    x_rows(lambda k: k + 2, (0, 5))
    all_yz.wait_recv()
    for s in range(2):
        y_ends(s)
    lax.fori_loop(0, PAIRS, open_y_dz, 0)
    all_rest_y.wait_recv()
    lax.fori_loop(0, CX, open_y_rest, 0)
    send_terms(1)
    inner(4, 6)
    send_terms(2)
    inner(6, 8)
    pl.semaphore_wait(far_sem, n_gy)
    for k in range(1, n_gx):
        pl.semaphore_signal(last_sem, inc=1, device_id=at(k, 0, 0), device_id_type=MESH)

    send_terms(3)
    all_xz.wait_recv()
    def x_changes(half):
        for sx in range(2):
            left, right = XER[sx, 0], XER[sx, 1]
            lefts = left, pltpu.roll(left, CZ - 2, 1)
            rights = pltpu.roll(right, 2, 1), right
            for v in range(2):
                own = packed([
                    F[c, (CX + 2) * sx + xi, OWN + 8 * b : OWN + 8 * b + 8, :] if b // 2 == half else None
                    for c in range(4 * v, min(4 * v + 4, GEO)) for xi in range(2) for b in range(BLOCKS)
                ])
                CXE[sx, v] = change(own, lefts[v], rights[v])[0]

    def x_ends(c, half):
        rows = slice(OWN + half * CY // 2, OWN + half * CY // 2 + CY // 2)
        for side in range(2):
            layers = slice(CX + 2, CX + 4) if side else slice(0, 2)
            out = along_z(F[c, layers, rows, :].reshape(CY, CZ), CZ)
            changed = CXE[side, c // 4]
            for xi in range(2):
                for b in range(2):
                    turn = CZ - 2 - 32 * (c % 4) - 4 * (BLOCKS * xi + 2 * half + b)
                    row = CY // 2 * xi + 8 * b
                    target = slice(rows.start + 8 * b, rows.start + 8 * b + 8)
                    DZ[c, layers.start + xi, target, :] = out[row : row + 8] + at_ends(changed, turn)

    def x_edge_rows(*tiles):
        x_rows(lambda k: k + (k // 2) * (CX - 4), tiles)

    def outer(b):
        def body(i, _):
            for n in range(2):
                cell((CX - 2) * i + n, b)
            return 0

        lax.fori_loop(0, 2, body, 0)

    x_changes(0)
    for c in range(GEO):
        x_ends(c, 0)
    x_edge_rows(1, 2, 3)
    outer(1)
    x_changes(1)
    for c in range(GEO):
        x_ends(c, 1)
    x_edge_rows(4)
    outer(2)
    all_xy.wait_recv()
    for sx in range(2):
        for sy in range(2):
            for c in range(GEO):
                for k in range(2):
                    layer = (CX + 2 if sx else 0) + k
                    row = OWN + CY if sy else OWN - 2
                    F[c, layer, row : row + 2, :] = XYR[sx, sy, c * 4 + k * 2 : c * 4 + k * 2 + 2, :]
    x_edge_rows(0, 5)
    outer(0)
    outer(3)
    all_terms.wait_recv()

    def finish(k, _):
        side, sub = k // 2, lax.rem(k, 2)
        x = k + side * (CX - 4)
        ham_out[x] = ham_out[x] + CR[side, 0, sub]
        for n in range(3):
            mom_out[n, x] = mom_out[n, x] + CR[side, 1 + n, sub]
        for b in range(BLOCKS):
            tally(x, b)
        return 0

    lax.fori_loop(0, 4, finish, 0)
    halves = [jnp.sum(ACC[n], axis=0, keepdims=True) for n in range(2)]
    halves = [half + pltpu.roll(half, CZ // 2, 1) for half in halves]
    lower = lax.broadcasted_iota(jnp.int32, (1, CZ), 1) < CZ // 2
    MINE[0] = jnp.where(lower, halves[0], halves[1])
    n_chips = n_gz // 2
    n_plane, n_line = n_gy * n_chips, 2 * n_gx
    core = lax.rem(iz, 2)
    rank_a, rank_b = iy * n_chips + iz // 2, 2 * ix + core
    SUM_A[rank_a] = MINE[0]
    pl.semaphore_wait(last_sem, n_gx - 1)
    def is_lead(device):
        return (device[0] == LEAD[0]) & (device[1] == LEAD[1]) & (device[2] == LEAD[2])

    own = rank_b * n_plane + rank_a
    leading = is_lead((ix, iy, iz))
    ALL[own] = MINE[0]
    direct = remote(MINE.at[0], ALL.at[own], S_DIRECT, LEAD)
    pl.when(jnp.logical_not(leading))(direct.start)

    far_first = sorted(
        ((dy, k) for dy in range(n_gy) for k in range(n_chips) if dy or k),
        key=lambda p: -min(p[0], n_gy - p[0]) - min(p[1], n_chips - p[1]),
    )
    for dy, k in far_first:
        remote(MINE.at[0], SUM_A.at[rank_a], S_SUM_A, at(0, dy, 2 * k)).start()
    others = remote(SUM_A.at[pl.ds(0, n_plane - 1)], SUM_A.at[pl.ds(0, n_plane - 1)], S_SUM_A, at(0, 1, 0))
    others.wait_recv()
    total = SUM_A[0]
    for k in range(1, n_plane):
        total = total + SUM_A[k]
    MINE[1] = total
    SUM_B[rank_b] = total
    for dx in sorted(range(n_gx), key=lambda k: -min(k, n_gx - k)):
        for z in [zs[0], twin[2]] if dx else [twin[2]]:
            copy = remote(MINE.at[1], SUM_B.at[rank_b], S_SUM_B, (xs[dx], iy, z))
            pl.when(jnp.logical_not(is_lead((xs[dx], iy, z))))(copy.start)

    def norms(total):
        cells = float(CX * CY * CZ * n_gx * n_gy * n_gz)
        column = lax.broadcasted_iota(jnp.int32, (1, 2), 1)
        ham_sum = jnp.sum(jnp.where(lower, total, 0.0), axis=1, keepdims=True)
        mom_sum = jnp.sum(jnp.where(lower, 0.0, total), axis=1, keepdims=True)
        ham_sum, mom_sum = jnp.broadcast_to(ham_sum, (1, 2)), jnp.broadcast_to(mom_sum, (1, 2))
        norm_out[...] = jnp.sqrt(jnp.where(column == 0, ham_sum / cells, mom_sum / (3.0 * cells)))

    @pl.when(jnp.logical_not(leading))
    def _():
        group(SUM_B.at[0 : n_line - 1], S_SUM_B).wait_recv()
        total = SUM_B[0]
        for j in range(1, n_line):
            total = total + SUM_B[j]
        norms(total)

    @pl.when(leading)
    def _():
        group(ALL.at[0 : n_line * n_plane - 1], S_DIRECT).wait_recv()

        def rows_of(j):
            rows = ALL[n_plane * j]
            for k in range(1, n_plane):
                rows = rows + ALL[n_plane * j + k]
            return rows

        parts = [rows_of(j) for j in range(n_line)]
        total = parts[0]
        for part in parts[1:]:
            total = total + part
        norms(total)

    group(PT.at[0:15, 0:4], S_GEO_X).wait_send()
    group(PT.at[0:7, 0:2], S_GEO_Y).wait_send()
    others.wait_send()
    pl.when(jnp.logical_not(leading))(direct.wait_send)
    fewer = jnp.logical_not(leading) & (iy == LEAD[1]) & (iz // 2 == LEAD[2] // 2)
    pl.when(fewer)(group(SUM_B.at[0 : n_line - 2], S_SUM_B).wait_send)
    pl.when(jnp.logical_not(fewer))(group(SUM_B.at[0 : n_line - 1], S_SUM_B).wait_send)


def write_out(ham, mom, norm, ham_out, mom_out, norm_out, sems):
    copies = [
        pltpu.make_async_copy(src, dst, sems.at[i])
        for i, (src, dst) in enumerate(((ham, ham_out), (mom, mom_out), (norm, norm_out)))
    ]
    for copy in copies:
        copy.start()
    for copy in copies:
        copy.wait()


def solution(mesh):
    sizes = (mesh.shape["gx"], mesh.shape["gy"], mesh.shape["gz"])
    f32 = jnp.float32

    def step(chi, met, cur, trk, gam):
        vm = lambda *shape: pltpu.VMEM(shape, f32)
        ham, mom, norm = pl.pallas_call(
            functools.partial(kernel, sizes),
            out_shape=(
                pltpu.VMEM((CX, CY, CZ), f32),
                pltpu.VMEM((3, CX, CY, CZ), f32),
                pltpu.VMEM((1, 2), f32),
            ),
            in_specs=[pl.BlockSpec(memory_space=pl.ANY)] * 5,
            out_specs=(
                pl.BlockSpec(memory_space=pltpu.VMEM),
                pl.BlockSpec(memory_space=pltpu.VMEM),
                pl.BlockSpec(memory_space=pltpu.VMEM),
            ),
            scratch_shapes=[
                vm(GEO, LX, ROWS, CZ), vm(REST, LX, ROWS, CZ),
                vm(GEO, LX, ROWS, CZ), vm(GEO, CX, CY, CZ), vm(8, CX, CY, CZ),
                vm(GEO, CX, ROWS, CZ), vm(GEO, CX, ROWS, CZ), vm(2, 8, CZ),
                vm(2, 136, CZ), vm(2, 8, 2 * CX, CZ), vm(2, 136, CZ), vm(2, 8, 2 * CX, CZ),
                vm(2, 128, CZ), vm(2, 2, 8, CZ), vm(2, 2, 32, CZ),
                pltpu.VMEM((3 * CZ, 2 * CZ), jnp.bfloat16),
                vm(15, 8, CZ), vm(2, 15, 8, CZ), vm(15, 8, CZ), vm(GEO, 8, CZ),
                vm(2, 2, 8, CZ), vm(2, 2, 8, CZ), vm(2, 2, 8, CZ),
                vm(2, 4, 2, CY, CZ), vm(2, 4, 2, CY, CZ), vm(18, CX, CY, CZ),
                vm(2, 1, CZ), vm(sizes[1] * sizes[2] // 2, 1, CZ), vm(2 * sizes[0], 1, CZ), vm(sizes[0] * sizes[1] * sizes[2], 1, CZ),
                pltpu.SemaphoreType.DMA((3,)),
                pltpu.SemaphoreType.DMA((5,)),
                pltpu.SemaphoreType.DMA((S_GEO_X + BLOCKS,)),
                pltpu.SemaphoreType.REGULAR,
                pltpu.SemaphoreType.REGULAR,
                pltpu.SemaphoreType.REGULAR,
                pltpu.SemaphoreType.REGULAR,
            ],
            compiler_params=pltpu.CompilerParams(collective_id=0, has_side_effects=True),
        )(chi, met, cur, trk, gam)
        ham, mom, norm = pl.pallas_call(
            write_out,
            out_shape=(
                jax.ShapeDtypeStruct((CX, CY, CZ), f32),
                jax.ShapeDtypeStruct((3, CX, CY, CZ), f32),
                jax.ShapeDtypeStruct((1, 2), f32),
            ),
            in_specs=[pl.BlockSpec(memory_space=pl.ANY)] * 3,
            out_specs=[pl.BlockSpec(memory_space=pl.ANY)] * 3,
            scratch_shapes=[pltpu.SemaphoreType.DMA((3,))],
        )(*[pltpu.with_memory_space_constraint(x, pltpu.VMEM) for x in (ham, mom, norm)])
        return ham, mom, norm.reshape(2)

    return jax.shard_map(
        step,
        mesh=mesh,
        in_specs=(
            P("gx", "gy", "gz"),
            P(None, "gx", "gy", "gz"),
            P(None, "gx", "gy", "gz"),
            P("gx", "gy", "gz"),
            P(None, "gx", "gy", "gz"),
        ),
        out_specs=(P("gx", "gy", "gz"), P(None, "gx", "gy", "gz"), P()),
        check_vma=False,
    )
```
